8 devices in a mesh: sys: 1 (over z), gx: 2 (over y), gy: 2 (over x), gz: 2 (over core).
Axes of the slice: x: 2, y: 2, z: 1, core: 2. Of those that a mesh axis runs over, the one named last changes fastest.
Arguments:
- source: float32 [96, 128, 128], P(('sys', 'gx'), 'gy', 'gz')
- initial: float32 [96, 128, 128], P(('sys', 'gx'), 'gy', 'gz')
- velocity: float32 [3, 96, 128, 128], P(None, ('sys', 'gx'), 'gy', 'gz')
- damping: float32 [2, 10], P('sys')
Outputs:
- output 1: float32 [96, 128, 128], P(('sys', 'gx'), 'gy', 'gz')
- output 2: float32 [2, 11], P('sys')
All inputs are finite; a program needn't handle non-finite values.
Results may differ from the reference program's by a relative error of at most 0.001.
Values sent between devices are 32-bit elements.
A program may use at most 1 GiB of HBM per device.

```python
import math
import jax
import jax.numpy as jnp
from jax import lax

TILES_X = 2
TILES_Y = 2
TILES_Z = 2
BLOCK_X = 48
BLOCK_Y = 64
BLOCK_Z = 64
RESTART = 10
CYCLES = 2
SWEEPS = 3
GRID_X = TILES_X * BLOCK_X
GRID_Y = TILES_Y * BLOCK_Y
GRID_Z = TILES_Z * BLOCK_Z


def smooth_modes(extent):
    positions = jnp.arange(1, extent + 1).astype(jnp.float32) / (extent + 1)
    orders = jnp.arange(1, 4).astype(jnp.float32)
    return jnp.sin(math.pi * orders[:, None] * positions[None, :])


def setup_inputs(seed: int = 0, part: int = 0) -> dict:
    base_key = jax.random.fold_in(jax.random.key(seed), part)
    subkeys = jax.random.split(base_key, 9)
    grid_shape = (GRID_X, GRID_Y, GRID_Z)
    src_scale = jax.random.uniform(subkeys[6], (), jnp.float32, 0.5, 1.5)
    source = src_scale * jax.random.normal(subkeys[0], grid_shape, jnp.float32)
    init_scale = jax.random.uniform(subkeys[7], (), jnp.float32, 0.1, 0.6)
    mode_coef = 0.5 * jax.random.normal(subkeys[8], (3, 3, 3), jnp.float32)
    smooth_part = jnp.einsum('pqr,pi,qj,rk->ijk', mode_coef, smooth_modes(GRID_X), smooth_modes(GRID_Y), smooth_modes(GRID_Z))
    initial = init_scale * jax.random.normal(subkeys[1], grid_shape, jnp.float32) + smooth_part
    flow_size = jax.random.uniform(subkeys[2], (3, 1, 1, 1), jnp.float32, 0.3, 0.8)
    flow_sign = 2.0 * jax.random.bernoulli(subkeys[3], 0.5, (3, 1, 1, 1)).astype(jnp.float32) - 1.0
    velocity = flow_size * flow_sign + 0.5 * jax.random.normal(subkeys[4], (3,) + grid_shape, jnp.float32)
    damping = jax.random.uniform(subkeys[5], (CYCLES, RESTART), jnp.float32, 0.3, 1.3)
    return {'source': source, 'initial': initial, 'velocity': velocity, 'damping': damping}


def block_masks():
    mask_pairs = []
    for axis_pos, extent, block_len in ((0, GRID_X, BLOCK_X), (1, GRID_Y, BLOCK_Y), (2, GRID_Z, BLOCK_Z)):
        positions = jnp.arange(extent) % block_len
        view_shape = [1, 1, 1]
        view_shape[axis_pos] = extent
        ahead_keep = (positions != block_len - 1).astype(jnp.float32).reshape(tuple(view_shape))
        behind_keep = (positions != 0).astype(jnp.float32).reshape(tuple(view_shape))
        mask_pairs.append((ahead_keep, behind_keep))
    return mask_pairs


def stencil(field, velocity, masks):
    padded = jnp.pad(field, 1)
    ahead_all = (padded[2:, 1:-1, 1:-1], padded[1:-1, 2:, 1:-1], padded[1:-1, 1:-1, 2:])
    behind_all = (padded[:-2, 1:-1, 1:-1], padded[1:-1, :-2, 1:-1], padded[1:-1, 1:-1, :-2])
    result = 6.0 * field
    for axis_pos in range(3):
        ahead_val = ahead_all[axis_pos] * masks[axis_pos][0]
        behind_val = behind_all[axis_pos] * masks[axis_pos][1]
        result = result - ahead_val - behind_val + 0.5 * velocity[axis_pos] * (ahead_val - behind_val)
    return result


def precondition(vector, velocity, relax_w, masks):
    step_scale = relax_w / 6.0
    approx = step_scale * vector
    for sweep_id in range(SWEEPS - 1):
        approx = approx + step_scale * (vector - stencil(approx, velocity, masks))
    return approx


def givens_solve(hessen, beta_zero):
    col_count = hessen.shape[1]
    rot_rows = hessen
    rhs_vec = jnp.zeros((col_count + 1,), jnp.float32).at[0].set(beta_zero)
    sine_list = []
    for col_id in range(col_count):
        diag_val = rot_rows[col_id, col_id]
        below_val = rot_rows[col_id + 1, col_id]
        radius = jnp.sqrt(diag_val * diag_val + below_val * below_val)
        cosine = diag_val / radius
        sine_val = below_val / radius
        upper_row = cosine * rot_rows[col_id] + sine_val * rot_rows[col_id + 1]
        lower_row = cosine * rot_rows[col_id + 1] - sine_val * rot_rows[col_id]
        rot_rows = rot_rows.at[col_id].set(upper_row).at[col_id + 1].set(lower_row)
        lead_val = rhs_vec[col_id]
        rhs_vec = rhs_vec.at[col_id].set(cosine * lead_val).at[col_id + 1].set(-sine_val * lead_val)
        sine_list.append(jnp.abs(sine_val))
    coeffs = jnp.zeros((col_count,), jnp.float32)
    for row_id in reversed(range(col_count)):
        remainder = rhs_vec[row_id] - jnp.sum(rot_rows[row_id] * coeffs)
        coeffs = coeffs.at[row_id].set(remainder / rot_rows[row_id, row_id])
    factors = jnp.concatenate([jnp.ones((1,), jnp.float32), jnp.stack(sine_list)])
    return coeffs, beta_zero * jnp.cumprod(factors)


def reference(source, initial, velocity, damping):
    cell_count = GRID_X * GRID_Y * GRID_Z
    grid_shape = (GRID_X, GRID_Y, GRID_Z)
    no_masks = ((1.0, 1.0), (1.0, 1.0), (1.0, 1.0))
    block_keep = block_masks()

    def run_cycle(current, omegas):
        residual = source - stencil(current, velocity, no_masks)
        beta_zero = jnp.sqrt(jnp.sum(residual * residual))
        basis = jnp.zeros((RESTART + 1, cell_count), jnp.float32).at[0].set((residual / beta_zero).reshape(cell_count))
        search = jnp.zeros((RESTART, cell_count), jnp.float32)
        hessen = jnp.zeros((RESTART + 1, RESTART), jnp.float32)

        def arnoldi_step(col_id, loop_state):
            basis_now, search_now, hessen_now = loop_state
            precond_vec = precondition(basis_now[col_id].reshape(grid_shape), velocity, omegas[col_id], block_keep)
            work_vec = stencil(precond_vec, velocity, no_masks).reshape(cell_count)
            proj_one = jnp.dot(basis_now, work_vec, preferred_element_type=jnp.float32)
            work_vec = work_vec - jnp.dot(proj_one, basis_now, preferred_element_type=jnp.float32)
            proj_two = jnp.dot(basis_now, work_vec, preferred_element_type=jnp.float32)
            work_vec = work_vec - jnp.dot(proj_two, basis_now, preferred_element_type=jnp.float32)
            norm_w = jnp.sqrt(jnp.sum(work_vec * work_vec))
            column = (proj_one + proj_two).at[col_id + 1].set(norm_w)
            return (basis_now.at[col_id + 1].set(work_vec / norm_w),
                    search_now.at[col_id].set(precond_vec.reshape(cell_count)),
                    hessen_now.at[:, col_id].set(column))

        basis, search, hessen = lax.fori_loop(0, RESTART, arnoldi_step, (basis, search, hessen))
        coeffs, estimates = givens_solve(hessen, beta_zero)
        update = jnp.dot(coeffs, search, preferred_element_type=jnp.float32).reshape(grid_shape)
        return current + update, estimates / math.sqrt(cell_count)

    solution, residuals = lax.scan(run_cycle, initial, damping)
    return solution, residuals
```

```python
import math
import jax
import jax.numpy as jnp
from jax import lax
from jax.experimental import pallas as pl
from jax.experimental.pallas import tpu as pltpu
from jax.sharding import PartitionSpec as P

MESH = pl.DeviceIdType.MESH
RESTART = 10
CYCLES = 2
NP = 24
LO, HI, ROWS = 8, 72, 80
XG, YG, ZG = slice(0, 32), slice(32, 56), slice(56, 120)
GROWS = 120
UA, UB, UD, UI, UP, UR, UG = 2, 2, 2, 2, 2, 2, 1


def planes(unroll, body, carry=()):
    if unroll == NP:
        for p in range(1, NP + 1):
            carry = body(p, carry)
        return carry

    def trip(t, carry):
        for i in range(unroll):
            carry = body(t * unroll + (i + 1), carry)
        return carry
    return lax.fori_loop(0, NP // unroll, trip, carry)


def groups(fn):
    def trip(t, carry):
        for i in range(UG):
            fn(pl.ds(pl.multiple_of((t * UG + i) * 8, 8), 8))
        return carry
    lax.fori_loop(0, GROWS // 8 // UG, trip, 0)


def kernel(src_ref, ini_ref, vel_ref, damp_ref, out_ref, res_ref,
           U, Z, UC, ZC, T1, T2, W, X, SRC, CPZ, CMZ, HVX, HVY, CGZ,
           GU, RB, SB, GZ, GX, SS, ACC, GM, RM, SIG, EC, CS, SN, GV, YY, RES, MISC,
           s_send, s_recv, h_send, h_recv, x_recv):
    f32 = jnp.float32
    gx, gy, gz = lax.axis_index('gx'), lax.axis_index('gy'), lax.axis_index('gz')
    peers = {}
    for p in range(1, 8):
        a, b, c = p // 4, (p // 2) % 2, p % 2
        peers[p] = {'gx': 1 - gx if a else gx, 'gy': 1 - gy if b else gy, 'gz': 1 - gz if c else gz}
    side = {0: 4, 1: 2, 2: 1}

    bar = pltpu.get_barrier_semaphore()
    for p in range(1, 8):
        pl.semaphore_signal(bar, inc=1, device_id=peers[p], device_id_type=MESH)

    lane = lax.broadcasted_iota(jnp.int32, (64, 128), 1)
    lane8 = lane[0:8]
    left = lane < 64
    zlane = jnp.where(left, lane, lane - 64)
    zero64 = jnp.zeros((64, 128), f32)
    zero8 = jnp.zeros((8, 128), f32)
    hi_x = (1 - gx).astype(f32)
    hi_y = (1 - gy).astype(f32)
    l0 = 63 * (1 - gz)
    sx_lo, sx_hi = 64 * (1 - gx), 64 * gx
    y_send = HI - 1 - 63 * gy
    y_pad = HI - 65 * gy

    def seams(V, ghost=None):
        a = pltpu.roll(V[NP, LO:HI, :], 64, 1)
        b = pltpu.roll(V[1, LO:HI, :], 64, 1)
        if ghost is None:
            V[0, LO:HI, :] = jnp.where(left, 0.0, a)
            V[NP + 1, LO:HI, :] = jnp.where(left, b, 0.0)
        else:
            V[0, LO:HI, :] = jnp.where(left, ghost * (1.0 - hi_x), a)
            V[NP + 1, LO:HI, :] = jnp.where(left, b, ghost * hi_x)

    def stencil(V, p):
        u = V[p, LO:HI, :]
        yp, ym = V[p, LO + 1:HI + 1, :], V[p, LO - 1:HI - 1, :]
        xp, xm = V[p + 1, LO:HI, :], V[p - 1, LO:HI, :]
        n = CPZ[p - 1] * pltpu.roll(u, 127, 1) + CMZ[p - 1] * pltpu.roll(u, 1, 1)
        n = n + (xp + xm) - HVX[p - 1] * (xp - xm)
        n = n + (yp + ym) - HVY[p - 1] * (yp - ym)
        return u, 6.0 * u - n

    def ghost_z(cz, p):
        shift = (l0 - (p - 1) + 128) % 128
        return CGZ[p - 1] * pltpu.roll(cz, shift, 1)

    def fill_ghosts(V, rec):
        g = rec[XG, :]
        gfull = jnp.concatenate([pltpu.roll(g, sx_lo, 1), pltpu.roll(g, sx_hi, 1)], axis=0)
        seams(V, gfull)

        def row(p, c):
            V[p, pl.ds(y_pad, 1), :] = rec[pl.ds(p + 31, 1), :]
            return c
        planes(UP, row)

    def pack(V, q):
        pd = NP - 23 * gx
        plane = V[pd, LO:HI, :]
        a = pltpu.roll(plane[0:32], sx_lo, 1)
        b = pltpu.roll(plane[32:64], sx_hi, 1)
        SB[q, XG, :] = jnp.where(left[0:32], a, b)

        def row(p, acc):
            SB[q, pl.ds(p + 31, 1), :] = V[p, pl.ds(y_send, 1), :]
            shift = (p - 1 - l0 + 128) % 128
            return jnp.where(zlane == p - 1, pltpu.roll(V[p, LO:HI, :], shift, 1), acc)
        SB[q, ZG, :] = planes(UP, row, zero64)

    def halo(q, dst, sem):
        out = []
        for ax, rows in ((0, XG), (1, YG), (2, ZG)):
            out.append(pltpu.make_async_remote_copy(
                src_ref=SB.at[q, rows, :], dst_ref=dst.at[rows, :],
                send_sem=h_send.at[q, ax], recv_sem=sem.at[ax],
                device_id=peers[side[ax]], device_id_type=MESH))
        return out

    def sync_copies(par):
        return [pltpu.make_async_remote_copy(
            src_ref=SS.at[par, pl.ds(0, 1), :], dst_ref=SS.at[par, pl.ds(p, 1), :],
            send_sem=s_send.at[p], recv_sem=s_recv.at[par, p],
            device_id=peers[p], device_id_type=MESH) for p in range(1, 8)]

    def sync_start(par, items):
        row = zero8
        for idx, acc in items:
            row = jnp.where(lane8 == idx, jnp.sum(acc, axis=1, keepdims=True), row)
        row = row + pltpu.roll(row, 4, 0)
        row = row + pltpu.roll(row, 2, 0)
        row = row + pltpu.roll(row, 1, 0)
        SS[par, 0:1, :] = row[0:1]
        for cp in sync_copies(par):
            cp.start()

    def sync_wait(par):
        for cp in sync_copies(par):
            cp.wait_recv()
        for cp in sync_copies(par):
            cp.wait_send()
        tot = SS[par]
        tot = tot + pltpu.roll(tot, 4, 0)
        tot = tot + pltpu.roll(tot, 2, 0)
        return tot + pltpu.roll(tot, 1, 0)

    def bc(tot, k):
        return jnp.broadcast_to(tot[:, k:k + 1], (8, 128))

    def fold(x):
        return jnp.sum(x.reshape(8, 8, 128), axis=0)

    def wide(e):
        return jnp.concatenate([e] * 8, axis=0)

    def packed(lo, hi):
        return jnp.concatenate([lo, hi], axis=1)

    @pl.loop(0, NP + 2)
    def _(p):
        for V in (UC, ZC, T1, W, X):
            V[p, 0:LO, :] = zero8
            V[p, HI:ROWS, :] = zero8

    @pl.loop(0, NP)
    def _(i):
        X[i + 1, LO:HI, :] = packed(ini_ref[i], ini_ref[i + NP])
        SRC[i] = packed(src_ref[i], src_ref[i + NP])
        HVX[i] = 0.5 * packed(vel_ref[0, i], vel_ref[0, i + NP])
        HVY[i] = 0.5 * packed(vel_ref[1, i], vel_ref[1, i + NP])
        hz = 0.5 * packed(vel_ref[2, i], vel_ref[2, i + NP])
        first, last = zlane == 0, zlane == 63
        CPZ[i] = jnp.where(last, 0.0, 1.0 - hz)
        CMZ[i] = jnp.where(first, 0.0, 1.0 + hz)
        hi_z = (1 - gz).astype(f32)
        CGZ[i] = jnp.where(last, hi_z * (1.0 - hz), jnp.where(first, (1.0 - hi_z) * (1.0 + hz), 0.0))

    pack(X, 0)
    pl.semaphore_wait(bar, 7)
    cps = halo(0, GX, x_recv)
    for cp in cps:
        cp.start()
    for cp in cps:
        cp.wait()

    def residual(scale):
        fill_ghosts(X, GX)
        cz = GX[ZG, :]

        def one(p, acc):
            _, ax = stencil(X, p)
            r = SRC[p - 1] - (ax - ghost_z(cz, p))
            if scale is not None:
                r = r * wide(scale)
                U[0, p - 1] = r
            UC[p, LO:HI, :] = r
            return acc + fold(r * r)
        acc = planes(UR, one, zero8)
        seams(UC)
        return acc

    def block_apply(V, O, unroll):
        def one(p, c):
            _, t = stencil(V, p)
            O[p, LO:HI, :] = t
            return c
        planes(unroll, one)

    acc0 = residual(None)
    sync_start(0, [(16, acc0)])
    started = []
    pack(UC, 0)
    started += halo(0, GU.at[0, 0], h_recv.at[1, 0])
    for cp in started[0:3]:
        cp.start()
    block_apply(UC, T1, UR)
    seams(T1)
    pack(T1, 1)
    started += halo(1, GU.at[0, 1], h_recv.at[1, 1])
    for cp in started[3:6]:
        cp.start()
    block_apply(T1, T2, UR)
    pack(T2, 2)
    started += halo(2, GU.at[0, 2], h_recv.at[1, 2])
    for cp in started[6:9]:
        cp.start()
    tot = sync_wait(0)
    beta0 = jnp.sqrt(bc(tot, 16))
    inv0 = 1.0 / beta0
    MISC[0] = beta0
    MISC[1] = inv0
    ACC[0] = acc0 * inv0 * inv0

    def rescale(p, c):
        r = UC[p, LO:HI, :] * wide(inv0)
        UC[p, LO:HI, :] = r
        U[0, p - 1] = r
        return c
    planes(UP, rescale)
    seams(UC)
    for cp in started:
        cp.wait()

    def rescale_ghost(rows):
        for q in range(3):
            GU[0, q, rows, :] = GU[0, q, rows, :] * inv0
    groups(rescale_ghost)

    def givens(m, sub):
        h = [RM[i, m] for i in range(m + 1)]
        for i in range(m):
            cs, sn = CS[i], SN[i]
            h[i], h[i + 1] = cs * h[i] + sn * h[i + 1], cs * h[i + 1] - sn * h[i]
        d = h[m]
        rad = jnp.sqrt(d * d + sub * sub)
        cs, sn = d / rad, sub / rad
        CS[m] = cs
        SN[m] = sn
        h[m] = cs * d + sn * sub
        for i in range(m + 1):
            RM[i, m] = h[i]
        g = GV[m]
        GV[m] = cs * g
        GV[m + 1] = -sn * g
        est = MISC[4] * jnp.abs(sn)
        MISC[4] = est
        return est

    out_scale = 1.0 / math.sqrt(1572864.0)

    @pl.loop(0, CYCLES)
    def _(c):
        @pl.loop(0, RESTART)
        def _(j):
            step = c * RESTART + j
            par = (step + 1) % 2
            hpar = step % 2
            s = damp_ref[c, j] / 6.0
            a0, a1, a2 = 3.0 * s, 3.0 * s * s, s * s * s

            block_apply(UC, T1, UA)
            seams(T1)

            def precond(p, cy):
                t1, t2 = stencil(T1, p)
                z = a0 * UC[p, LO:HI, :] - a1 * t1 + a2 * t2
                ZC[p, LO:HI, :] = z
                Z[j, p - 1] = z
                return cy
            planes(UB, precond)

            for k in range(1, RESTART):
                @pl.when(j == k)
                def _():
                    for cp in [x for q in range(3) for x in halo(q, RB.at[c, k - 1, q], h_recv.at[1 - hpar, q])]:
                        cp.wait_recv()
                    ec = [EC[i] for i in range(k + 1)]

                    def ghost_u(rows):
                        for q in range(3):
                            g = ec[k] * RB[c, k - 1, q, rows, :]
                            for i in range(k):
                                g = g - ec[i] * GU[i, q, rows, :]
                            GU[k, q, rows, :] = g
                    groups(ghost_u)

            def ghost_of_z(rows):
                GZ[j, rows, :] = a0 * GU[j, 0, rows, :] - a1 * GU[j, 1, rows, :] + a2 * GU[j, 2, rows, :]
            groups(ghost_of_z)
            fill_ghosts(ZC, GZ.at[j])

            for k in range(RESTART):
                @pl.when(j == k)
                def _():
                    cz = GZ[k, ZG, :]

                    def one(p, accs):
                        accs = list(accs)
                        _, az = stencil(ZC, p)
                        w = az - ghost_z(cz, p)
                        W[p, LO:HI, :] = w
                        for i in range(k + 1):
                            accs[i] = accs[i] + fold(U[i, p - 1] * w)
                        if k == 0 or k == RESTART - 1:
                            accs[k + 1] = accs[k + 1] + fold(w * w)
                        return tuple(accs)
                    accs = planes(UD, one, (zero8,) * (k + 2))
                    accw = accs[k + 1]
                    items = [(i, accs[i]) for i in range(k + 1)] + [(16 + i, ACC[i]) for i in range(k + 1)]
                    if k == 0 or k == RESTART - 1:
                        items.append((32, accw))
                    sync_start(par, items)

            @pl.when(step < CYCLES * RESTART - 1)
            def _():
                seams(W)
                pack(W, 0)
                for cp in halo(0, RB.at[c, j, 0], h_recv.at[hpar, 0]):
                    cp.start()
                block_apply(W, T1, UI)
                seams(T1)
                pack(T1, 1)
                for cp in halo(1, RB.at[c, j, 1], h_recv.at[hpar, 1]):
                    cp.start()
                block_apply(T1, T2, UI)
                pack(T2, 2)
                for cp in halo(2, RB.at[c, j, 2], h_recv.at[hpar, 2]):
                    cp.start()

            tot = sync_wait(par)

            @pl.when(step < CYCLES * RESTART - 1)
            def _():
                for cp in [x for q in range(3) for x in halo(q, RB.at[c, j, q], h_recv.at[hpar, q])]:
                    cp.wait_send()

            for k in range(RESTART):
                @pl.when(j == k)
                def _():
                    nn = bc(tot, 16 + k)
                    nrm = jnp.sqrt(nn)
                    sg = 1.0 / nrm
                    SIG[k] = sg
                    sig = [SIG[i] for i in range(k)] + [sg]
                    h = [bc(tot, i) * sig[i] * sg for i in range(k + 1)]
                    gcol = [bc(tot, 16 + i) * sig[i] * sg for i in range(k)] + [nn * sg * sg]
                    for i in range(k + 1):
                        GM[i, k] = gcol[i]
                        if i < k:
                            GM[k, i] = gcol[i]
                    if k == 0:
                        beta = MISC[0] * nrm
                        MISC[4] = beta
                        GV[0] = beta
                        RES[c] = jnp.where(lane8 == 0, beta, 0.0)
                    else:
                        est = givens(k - 1, nrm * MISC[3])
                        RES[c] = jnp.where(lane8 == k, est, RES[c])
                    cf = []
                    for i in range(k + 1):
                        gh = gcol[i] * h[k]
                        for m in range(k):
                            gh = gh + GM[i, m] * h[m]
                        cf.append(2.0 * h[i] - gh)
                        RM[i, k] = cf[i]
                    if k == 0:
                        wn = jnp.sqrt(bc(tot, 32)) * sg
                        MISC[3] = wn
                        MISC[2] = 1.0 / wn
                    rho = MISC[2]
                    if k < RESTART - 1:
                        es = [rho * cf[i] * sig[i] for i in range(k + 1)]
                        ew = rho * sg
                        for i in range(k + 1):
                            EC[i] = es[i]
                        EC[k + 1] = ew

                        def body(i, accs):
                            accs = list(accs)
                            for r in range(0, 64, 16):
                                v = [U[m, i, r:r + 16, :].reshape(2, 8, 128) for m in range(k + 1)]
                                u = ew * W[i + 1, LO + r:LO + r + 16, :].reshape(2, 8, 128)
                                for m in range(k + 1):
                                    u = u - es[m] * v[m]
                                for m in range(k + 1):
                                    t = u * v[m]
                                    accs[m] = accs[m] + (t[0] + t[1])
                                t = u * u
                                accs[k + 1] = accs[k + 1] + (t[0] + t[1])
                                u = u.reshape(16, 128)
                                UC[i + 1, LO + r:LO + r + 16, :] = u
                                U[k + 1, i, r:r + 16, :] = u
                            return tuple(accs)

                        accs = lax.fori_loop(0, NP, body, (zero8,) * (k + 2))
                        for i in range(k + 2):
                            ACC[i] = accs[i]
                        seams(UC)
                    else:
                        wn2 = bc(tot, 32) * sg * sg
                        drop = zero8
                        for i in range(k + 1):
                            q = gcol[i] * cf[k]
                            for m in range(k):
                                q = q + GM[i, m] * cf[m]
                            drop = drop + cf[i] * (2.0 * h[i] - q)
                        sub = jnp.sqrt(jnp.maximum(wn2 - drop, 0.0))
                        est = givens(k, sub)
                        RES[c] = jnp.where(lane8 == k + 1, est, RES[c])
                        g = [GV[i] for i in range(RESTART)]
                        for i in reversed(range(RESTART)):
                            y = g[i] / RM[i, i]
                            YY[i] = y * sig[i]
                            for m in range(i):
                                g[m] = g[m] - RM[m, i] * y

        yy = [YY[i] for i in range(RESTART)]

        @pl.when(c == 0)
        def _():
            @pl.loop(0, NP)
            def _(i):
                for r in range(0, 64, 8):
                    x = X[i + 1, LO + r:LO + r + 8, :]
                    for m in range(RESTART):
                        x = x + yy[m] * Z[m, i, r:r + 8, :]
                    X[i + 1, LO + r:LO + r + 8, :] = x

            def ghost_x(rows):
                g = GX[rows, :]
                for m in range(RESTART):
                    g = g + yy[m] * GZ[m, rows, :]
                GX[rows, :] = g
            groups(ghost_x)
            inv = MISC[1]
            ACC[0] = residual(inv)
            for cp in [x for q in range(3) for x in halo(q, RB.at[0, RESTART - 1, q], h_recv.at[1, q])]:
                cp.wait_recv()

            def ghost_r(rows):
                for q in range(3):
                    g = zero8
                    for m in range(RESTART):
                        g = g + yy[m] * RB[0, m, q, rows, :]
                    GU[0, q, rows, :] = GU[0, q, rows, :] - inv * g
            groups(ghost_r)

        @pl.when(c == CYCLES - 1)
        def _():
            @pl.loop(0, NP)
            def _(i):
                x = X[i + 1, LO:HI, :].reshape(8, 8, 128)
                for m in range(RESTART):
                    x = x + yy[m] * Z[m, i].reshape(8, 8, 128)
                x = x.reshape(64, 128)
                out_ref[i] = x[:, 0:64]
                out_ref[i + NP] = x[:, 64:128]

    rows = jnp.where(lax.broadcasted_iota(jnp.int32, (8, 128), 0) == 0, RES[0], RES[1]) * out_scale
    res_ref[...] = rows[0:2, 0:RESTART + 1]


def solution(mesh):
    grid_spec = P(('sys', 'gx'), 'gy', 'gz')
    vel_spec = P(None, ('sys', 'gx'), 'gy', 'gz')
    table_spec = P('sys', None)
    f32 = jnp.float32

    def local_solve(source, initial, velocity, damping):
        big = (NP + 2, ROWS, 128)
        vol = (NP, 64, 128)
        v = lambda *s: pltpu.VMEM(s, f32)
        scratch = [
            v(RESTART, *vol), v(RESTART, *vol),
            v(*big), v(*big), v(*big), v(*big), v(*big), v(*big),
            v(*vol), v(*vol), v(*vol), v(*vol), v(*vol), v(*vol),
            v(RESTART, 3, GROWS, 128), v(CYCLES, RESTART, 3, GROWS, 128), v(3, GROWS, 128),
            v(RESTART, GROWS, 128), v(GROWS, 128),
            v(2, 8, 128), v(RESTART + 1, 8, 128),
            v(RESTART, RESTART, 8, 128), v(RESTART, RESTART, 8, 128),
            v(RESTART, 8, 128), v(RESTART + 1, 8, 128), v(RESTART, 8, 128), v(RESTART, 8, 128),
            v(RESTART + 1, 8, 128), v(RESTART, 8, 128), v(CYCLES, 8, 128), v(8, 8, 128),
            pltpu.SemaphoreType.DMA((8,)), pltpu.SemaphoreType.DMA((2, 8)),
            pltpu.SemaphoreType.DMA((3, 3)), pltpu.SemaphoreType.DMA((2, 3, 3)), pltpu.SemaphoreType.DMA((3,)),
        ]
        vm = pl.BlockSpec(memory_space=pltpu.VMEM)
        return pl.pallas_call(
            kernel,
            out_shape=(jax.ShapeDtypeStruct(source.shape, f32), jax.ShapeDtypeStruct((CYCLES, RESTART + 1), f32)),
            in_specs=[vm, vm, vm, pl.BlockSpec(memory_space=pltpu.SMEM)],
            out_specs=(vm, vm),
            scratch_shapes=scratch,
            compiler_params=pltpu.CompilerParams(
                collective_id=0, has_side_effects=True, vmem_limit_bytes=67043328),
            name='fgmres',
        )(source, initial, velocity, damping)

    return jax.shard_map(local_solve, mesh=mesh, in_specs=(grid_spec, grid_spec, vel_spec, table_spec),
                         out_specs=(grid_spec, table_spec), check_vma=False)
```

```python
import math
import jax
import jax.numpy as jnp
from jax import lax
from jax.experimental import pallas as pl
from jax.experimental.pallas import tpu as pltpu
from jax.sharding import PartitionSpec as P

MESH = pl.DeviceIdType.MESH
RESTART = 10
CYCLES = 2
NP = 24
LO, HI, ROWS = 8, 72, 80
XG, YG, ZG = slice(0, 32), slice(32, 56), slice(56, 120)
GROWS = 120
UA, UB, UD, UI, UP, UR, UG = 24, 24, 24, 24, 24, 4, 5


def planes(unroll, body, carry=()):
    if unroll == NP:
        for p in range(1, NP + 1):
            carry = body(p, carry)
        return carry

    def trip(t, carry):
        for i in range(unroll):
            carry = body(t * unroll + (i + 1), carry)
        return carry
    return lax.fori_loop(0, NP // unroll, trip, carry)


def groups(fn):
    def trip(t, carry):
        for i in range(UG):
            fn(pl.ds(pl.multiple_of((t * UG + i) * 8, 8), 8))
        return carry
    lax.fori_loop(0, GROWS // 8 // UG, trip, 0)


def kernel(src_ref, ini_ref, vel_ref, damp_ref, out_ref, res_ref,
           U, Z, UC, ZC, T1, T2, W, X, SRC, CPZ, CMZ, HVX, HVY, CGZ,
           GU, RB, SB, GZ, GX, SS, ACC, GM, RM, SIG, EC, CS, SN, GV, YY, NRM, RES, MISC,
           s_send, s_recv, h_send, h_recv, x_recv):
    f32 = jnp.float32
    gx, gy, gz = lax.axis_index('gx'), lax.axis_index('gy'), lax.axis_index('gz')
    peers = {}
    for p in range(1, 8):
        a, b, c = p // 4, (p // 2) % 2, p % 2
        peers[p] = {'gx': 1 - gx if a else gx, 'gy': 1 - gy if b else gy, 'gz': 1 - gz if c else gz}
    side = {0: 4, 1: 2, 2: 1}

    bar = pltpu.get_barrier_semaphore()
    for p in range(1, 8):
        pl.semaphore_signal(bar, inc=1, device_id=peers[p], device_id_type=MESH)

    lane = lax.broadcasted_iota(jnp.int32, (64, 128), 1)
    lane8 = lane[0:8]
    left = lane < 64
    zlane = jnp.where(left, lane, lane - 64)
    zero64 = jnp.zeros((64, 128), f32)
    zero8 = jnp.zeros((8, 128), f32)
    hi_x = (1 - gx).astype(f32)
    hi_y = (1 - gy).astype(f32)
    l0 = 63 * (1 - gz)
    sx_lo, sx_hi = 64 * (1 - gx), 64 * gx
    y_send = HI - 1 - 63 * gy
    y_pad = HI - 65 * gy

    def seams(V, ghost=None):
        a = pltpu.roll(V[NP, LO:HI, :], 64, 1)
        b = pltpu.roll(V[1, LO:HI, :], 64, 1)
        if ghost is None:
            V[0, LO:HI, :] = jnp.where(left, 0.0, a)
            V[NP + 1, LO:HI, :] = jnp.where(left, b, 0.0)
        else:
            V[0, LO:HI, :] = jnp.where(left, ghost * (1.0 - hi_x), a)
            V[NP + 1, LO:HI, :] = jnp.where(left, b, ghost * hi_x)

    def stencil(V, p):
        u = V[p, LO:HI, :]
        yp, ym = V[p, LO + 1:HI + 1, :], V[p, LO - 1:HI - 1, :]
        xp, xm = V[p + 1, LO:HI, :], V[p - 1, LO:HI, :]
        n = CPZ[p - 1] * pltpu.roll(u, 127, 1) + CMZ[p - 1] * pltpu.roll(u, 1, 1)
        n = n + (xp + xm) - HVX[p - 1] * (xp - xm)
        n = n + (yp + ym) - HVY[p - 1] * (yp - ym)
        return u, 6.0 * u - n

    def ghost_z(cz, p):
        shift = (l0 - (p - 1) + 128) % 128
        return CGZ[p - 1] * pltpu.roll(cz, shift, 1)

    def fill_ghosts(V, rec):
        g = rec[XG, :]
        gfull = jnp.concatenate([pltpu.roll(g, sx_lo, 1), pltpu.roll(g, sx_hi, 1)], axis=0)
        seams(V, gfull)

        def row(p, c):
            V[p, pl.ds(y_pad, 1), :] = rec[pl.ds(p + 31, 1), :]
            return c
        planes(UP, row)

    def pack(V, q):
        pd = NP - 23 * gx
        plane = V[pd, LO:HI, :]
        a = pltpu.roll(plane[0:32], sx_lo, 1)
        b = pltpu.roll(plane[32:64], sx_hi, 1)
        SB[q, XG, :] = jnp.where(left[0:32], a, b)

        def row(p, acc):
            SB[q, pl.ds(p + 31, 1), :] = V[p, pl.ds(y_send, 1), :]
            shift = (p - 1 - l0 + 128) % 128
            return jnp.where(zlane == p - 1, pltpu.roll(V[p, LO:HI, :], shift, 1), acc)
        SB[q, ZG, :] = planes(UP, row, zero64)

    def halo(q, dst, sem):
        out = []
        for ax, rows in ((0, XG), (1, YG), (2, ZG)):
            out.append(pltpu.make_async_remote_copy(
                src_ref=SB.at[q, rows, :], dst_ref=dst.at[rows, :],
                send_sem=h_send.at[q, ax], recv_sem=sem.at[ax],
                device_id=peers[side[ax]], device_id_type=MESH))
        return out

    def sync_copies(par):
        return [pltpu.make_async_remote_copy(
            src_ref=SS.at[par, pl.ds(0, 1), :], dst_ref=SS.at[par, pl.ds(p, 1), :],
            send_sem=s_send.at[p], recv_sem=s_recv.at[par, p],
            device_id=peers[p], device_id_type=MESH) for p in range(1, 8)]

    def sync_start(par, items):
        row = zero8
        for idx, acc in items:
            row = jnp.where(lane8 == idx, jnp.sum(acc, axis=1, keepdims=True), row)
        row = row + pltpu.roll(row, 4, 0)
        row = row + pltpu.roll(row, 2, 0)
        row = row + pltpu.roll(row, 1, 0)
        SS[par, 0:1, :] = row[0:1]
        for cp in sync_copies(par):
            cp.start()

    def sync_wait(par):
        for cp in sync_copies(par):
            cp.wait_recv()
        for cp in sync_copies(par):
            cp.wait_send()
        tot = SS[par]
        tot = tot + pltpu.roll(tot, 4, 0)
        tot = tot + pltpu.roll(tot, 2, 0)
        return tot + pltpu.roll(tot, 1, 0)

    def bc(tot, k):
        return jnp.broadcast_to(tot[:, k:k + 1], (8, 128))

    def fold(x):
        return jnp.sum(x.reshape(8, 8, 128), axis=0)

    def wide(e):
        return jnp.concatenate([e] * 8, axis=0)

    def packed(lo, hi):
        return jnp.concatenate([lo, hi], axis=1)

    @pl.loop(0, NP + 2)
    def _(p):
        for V in (UC, ZC, T1, W, X):
            V[p, 0:LO, :] = zero8
            V[p, HI:ROWS, :] = zero8

    @pl.loop(0, NP)
    def _(i):
        X[i + 1, LO:HI, :] = packed(ini_ref[i], ini_ref[i + NP])
        SRC[i] = packed(src_ref[i], src_ref[i + NP])
        HVX[i] = 0.5 * packed(vel_ref[0, i], vel_ref[0, i + NP])
        HVY[i] = 0.5 * packed(vel_ref[1, i], vel_ref[1, i + NP])
        hz = 0.5 * packed(vel_ref[2, i], vel_ref[2, i + NP])
        first, last = zlane == 0, zlane == 63
        CPZ[i] = jnp.where(last, 0.0, 1.0 - hz)
        CMZ[i] = jnp.where(first, 0.0, 1.0 + hz)
        hi_z = (1 - gz).astype(f32)
        CGZ[i] = jnp.where(last, hi_z * (1.0 - hz), jnp.where(first, (1.0 - hi_z) * (1.0 + hz), 0.0))

    pack(X, 0)
    pl.semaphore_wait(bar, 7)
    cps = halo(0, GX, x_recv)
    for cp in cps:
        cp.start()
    for cp in cps:
        cp.wait()

    def residual(scale):
        fill_ghosts(X, GX)
        cz = GX[ZG, :]

        def one(p, acc):
            _, ax = stencil(X, p)
            r = SRC[p - 1] - (ax - ghost_z(cz, p))
            if scale is not None:
                r = r * wide(scale)
                U[0, p - 1] = r
            UC[p, LO:HI, :] = r
            return acc + fold(r * r)
        acc = planes(UR, one, zero8)
        seams(UC)
        return acc

    def block_apply(V, O, unroll):
        def one(p, c):
            _, t = stencil(V, p)
            O[p, LO:HI, :] = t
            return c
        planes(unroll, one)

    acc0 = residual(None)
    sync_start(0, [(16, acc0)])
    started = []
    pack(UC, 0)
    started += halo(0, GU.at[0, 0], h_recv.at[1, 0])
    for cp in started[0:3]:
        cp.start()
    block_apply(UC, T1, UR)
    seams(T1)
    pack(T1, 1)
    started += halo(1, GU.at[0, 1], h_recv.at[1, 1])
    for cp in started[3:6]:
        cp.start()
    block_apply(T1, T2, UR)
    pack(T2, 2)
    started += halo(2, GU.at[0, 2], h_recv.at[1, 2])
    for cp in started[6:9]:
        cp.start()
    tot = sync_wait(0)
    beta0 = jnp.sqrt(bc(tot, 16))
    inv0 = 1.0 / beta0
    MISC[0] = beta0
    MISC[1] = inv0
    ACC[0] = acc0 * inv0 * inv0

    def rescale(p, c):
        r = UC[p, LO:HI, :] * wide(inv0)
        UC[p, LO:HI, :] = r
        U[0, p - 1] = r
        return c
    planes(UP, rescale)
    seams(UC)
    for cp in started:
        cp.wait()

    def rescale_ghost(rows):
        for q in range(3):
            GU[0, q, rows, :] = GU[0, q, rows, :] * inv0
    groups(rescale_ghost)

    def givens(m, sub):
        h = [RM[i, m] for i in range(m + 1)]
        for i in range(m):
            cs, sn = CS[i], SN[i]
            h[i], h[i + 1] = cs * h[i] + sn * h[i + 1], cs * h[i + 1] - sn * h[i]
        d = h[m]
        rad = jnp.sqrt(d * d + sub * sub)
        cs, sn = d / rad, sub / rad
        CS[m] = cs
        SN[m] = sn
        h[m] = cs * d + sn * sub
        for i in range(m + 1):
            RM[i, m] = h[i]
        g = GV[m]
        GV[m] = cs * g
        GV[m + 1] = -sn * g
        est = MISC[4] * jnp.abs(sn)
        MISC[4] = est
        return est

    out_scale = 1.0 / math.sqrt(1572864.0)

    @pl.loop(0, CYCLES)
    def _(c):
        @pl.loop(0, RESTART)
        def _(j):
            step = c * RESTART + j
            par = (step + 1) % 2
            hpar = step % 2
            s = damp_ref[c, j] / 6.0
            a0, a1, a2 = 3.0 * s, 3.0 * s * s, s * s * s

            block_apply(UC, T1, UA)
            seams(T1)

            def precond(p, cy):
                t1, t2 = stencil(T1, p)
                z = a0 * UC[p, LO:HI, :] - a1 * t1 + a2 * t2
                ZC[p, LO:HI, :] = z
                Z[j, p - 1] = z
                return cy
            planes(UB, precond)

            for k in range(1, RESTART):
                @pl.when(j == k)
                def _():
                    for cp in [x for q in range(3) for x in halo(q, RB.at[c, k - 1, q], h_recv.at[1 - hpar, q])]:
                        cp.wait_recv()
                    ec = [EC[i] for i in range(k + 1)]

                    def ghost_u(rows):
                        for q in range(3):
                            g = ec[k] * RB[c, k - 1, q, rows, :]
                            for i in range(k):
                                g = g - ec[i] * GU[i, q, rows, :]
                            GU[k, q, rows, :] = g
                    groups(ghost_u)

            def ghost_of_z(rows):
                GZ[j, rows, :] = a0 * GU[j, 0, rows, :] - a1 * GU[j, 1, rows, :] + a2 * GU[j, 2, rows, :]
            groups(ghost_of_z)
            fill_ghosts(ZC, GZ.at[j])

            cz = GZ[j, ZG, :]

            def apply_a(p, cy):
                _, az = stencil(ZC, p)
                W[p, LO:HI, :] = az - ghost_z(cz, p)
                return cy
            planes(UD, apply_a)

            for k in range(RESTART):
                @pl.when(j == k)
                def _():
                    last = k == 0 or k == RESTART - 1

                    def dots(t, accs):
                        accs = list(accs)
                        w = W[pl.ds(t * 2 + 1, 2), LO:HI, :].reshape(16, 8, 128)
                        for i in range(k + 1):
                            v = U[i, pl.ds(t * 2, 2)].reshape(16, 8, 128)
                            accs[i] = accs[i] + jnp.sum(v * w, axis=0)
                        if last:
                            accs[k + 1] = accs[k + 1] + jnp.sum(w * w, axis=0)
                        return tuple(accs)
                    accs = lax.fori_loop(0, NP // 2, dots, (zero8,) * (k + 2 if last else k + 1))
                    items = [(i, accs[i]) for i in range(k + 1)] + [(16 + i, ACC[i]) for i in range(k + 1)]
                    if last:
                        items.append((32, accs[k + 1]))
                    sync_start(par, items)

            @pl.when(step < CYCLES * RESTART - 1)
            def _():
                seams(W)
                pack(W, 0)
                for cp in halo(0, RB.at[c, j, 0], h_recv.at[hpar, 0]):
                    cp.start()
                block_apply(W, T1, UI)
                seams(T1)
                pack(T1, 1)
                for cp in halo(1, RB.at[c, j, 1], h_recv.at[hpar, 1]):
                    cp.start()
                block_apply(T1, T2, UI)
                pack(T2, 2)
                for cp in halo(2, RB.at[c, j, 2], h_recv.at[hpar, 2]):
                    cp.start()

            for k in range(2, RESTART):
                @pl.when(j == k)
                def _():
                    est = givens(k - 2, NRM[k - 1] * MISC[3])
                    RES[c] = jnp.where(lane8 == k - 1, est, RES[c])

            tot = sync_wait(par)

            @pl.when(step < CYCLES * RESTART - 1)
            def _():
                for cp in [x for q in range(3) for x in halo(q, RB.at[c, j, q], h_recv.at[hpar, q])]:
                    cp.wait_send()

            for k in range(RESTART):
                @pl.when(j == k)
                def _():
                    nn = bc(tot, 16 + k)
                    nrm = jnp.sqrt(nn)
                    sg = 1.0 / nrm
                    SIG[k] = sg
                    NRM[k] = nrm
                    sig = SIG[0:k + 1] * sg
                    h = jnp.stack([bc(tot, i) for i in range(k + 1)]) * sig
                    gcol = jnp.stack([bc(tot, 16 + i) for i in range(k + 1)]) * sig
                    GM[k, 0:k + 1] = gcol
                    if k > 0:
                        GM[0:k, k] = gcol[0:k]

                    def gram_times(x):
                        out = gcol * x[k]
                        for m in range(k):
                            out = out + GM[m, 0:k + 1] * x[m]
                        return out
                    cf = 2.0 * h - gram_times(h)
                    RM[0:k + 1, k] = cf
                    if k == 0:
                        beta = MISC[0] * nrm
                        MISC[4] = beta
                        GV[0] = beta
                        RES[c] = jnp.where(lane8 == 0, beta, 0.0)
                        wn = jnp.sqrt(bc(tot, 32)) * sg
                        MISC[3] = wn
                        MISC[2] = 1.0 / wn
                        rho = 1.0 / wn
                    else:
                        rho = MISC[2]
                    if k < RESTART - 1:
                        es = rho * cf * SIG[0:k + 1]
                        ew = rho * sg
                        EC[0:k + 1] = es
                        EC[k + 1] = ew

                        def body(i, accs):
                            accs = list(accs)
                            for r in range(0, 64, 8):
                                v = [U[m, i, r:r + 8, :] for m in range(k + 1)]
                                u = ew * W[i + 1, LO + r:LO + r + 8, :]
                                for m in range(k + 1):
                                    u = u - es[m] * v[m]
                                UC[i + 1, LO + r:LO + r + 8, :] = u
                                U[k + 1, i, r:r + 8, :] = u
                                for m in range(k + 1):
                                    accs[m] = accs[m] + u * v[m]
                                accs[k + 1] = accs[k + 1] + u * u
                            return tuple(accs)

                        accs = lax.fori_loop(0, NP, body, (zero8,) * (k + 2))
                        ACC[0:k + 2] = jnp.stack(accs)
                        seams(UC)
                    else:
                        wn2 = bc(tot, 32) * sg * sg
                        drop = jnp.sum(cf * (2.0 * h - gram_times(cf)), axis=0)
                        sub = jnp.sqrt(jnp.maximum(wn2 - drop, 0.0))
                        est = givens(k - 1, nrm * MISC[3])
                        RES[c] = jnp.where(lane8 == k, est, RES[c])
                        est = givens(k, sub)
                        RES[c] = jnp.where(lane8 == k + 1, est, RES[c])
                        g = [GV[i] for i in range(RESTART)]
                        for i in reversed(range(RESTART)):
                            y = g[i] / RM[i, i]
                            YY[i] = y * SIG[i]
                            for m in range(i):
                                g[m] = g[m] - RM[m, i] * y

        yy = [YY[i] for i in range(RESTART)]

        @pl.when(c == 0)
        def _():
            @pl.loop(0, NP)
            def _(i):
                for r in range(0, 64, 8):
                    x = X[i + 1, LO + r:LO + r + 8, :]
                    for m in range(RESTART):
                        x = x + yy[m] * Z[m, i, r:r + 8, :]
                    X[i + 1, LO + r:LO + r + 8, :] = x

            def ghost_x(rows):
                g = GX[rows, :]
                for m in range(RESTART):
                    g = g + yy[m] * GZ[m, rows, :]
                GX[rows, :] = g
            groups(ghost_x)
            inv = MISC[1]
            ACC[0] = residual(inv)
            for cp in [x for q in range(3) for x in halo(q, RB.at[0, RESTART - 1, q], h_recv.at[1, q])]:
                cp.wait_recv()

            def ghost_r(rows):
                for q in range(3):
                    g = zero8
                    for m in range(RESTART):
                        g = g + yy[m] * RB[0, m, q, rows, :]
                    GU[0, q, rows, :] = GU[0, q, rows, :] - inv * g
            groups(ghost_r)

        @pl.when(c == CYCLES - 1)
        def _():
            @pl.loop(0, NP)
            def _(i):
                x = X[i + 1, LO:HI, :].reshape(8, 8, 128)
                for m in range(RESTART):
                    x = x + yy[m] * Z[m, i].reshape(8, 8, 128)
                x = x.reshape(64, 128)
                out_ref[i] = x[:, 0:64]
                out_ref[i + NP] = x[:, 64:128]

    rows = jnp.where(lax.broadcasted_iota(jnp.int32, (8, 128), 0) == 0, RES[0], RES[1]) * out_scale
    res_ref[...] = rows[0:2, 0:RESTART + 1]


def solution(mesh):
    grid_spec = P(('sys', 'gx'), 'gy', 'gz')
    vel_spec = P(None, ('sys', 'gx'), 'gy', 'gz')
    table_spec = P('sys', None)
    f32 = jnp.float32

    def local_solve(source, initial, velocity, damping):
        big = (NP + 2, ROWS, 128)
        vol = (NP, 64, 128)
        v = lambda *s: pltpu.VMEM(s, f32)
        scratch = [
            v(RESTART, *vol), v(RESTART, *vol),
            v(*big), v(*big), v(*big), v(*big), v(*big), v(*big),
            v(*vol), v(*vol), v(*vol), v(*vol), v(*vol), v(*vol),
            v(RESTART, 3, GROWS, 128), v(CYCLES, RESTART, 3, GROWS, 128), v(3, GROWS, 128),
            v(RESTART, GROWS, 128), v(GROWS, 128),
            v(2, 8, 128), v(RESTART + 1, 8, 128),
            v(RESTART, RESTART, 8, 128), v(RESTART, RESTART, 8, 128),
            v(RESTART, 8, 128), v(RESTART + 1, 8, 128), v(RESTART, 8, 128), v(RESTART, 8, 128),
            v(RESTART + 1, 8, 128), v(RESTART, 8, 128), v(RESTART, 8, 128), v(CYCLES, 8, 128), v(8, 8, 128),
            pltpu.SemaphoreType.DMA((8,)), pltpu.SemaphoreType.DMA((2, 8)),
            pltpu.SemaphoreType.DMA((3, 3)), pltpu.SemaphoreType.DMA((2, 3, 3)), pltpu.SemaphoreType.DMA((3,)),
        ]
        vm = pl.BlockSpec(memory_space=pltpu.VMEM)
        return pl.pallas_call(
            kernel,
            out_shape=(jax.ShapeDtypeStruct(source.shape, f32), jax.ShapeDtypeStruct((CYCLES, RESTART + 1), f32)),
            in_specs=[vm, vm, vm, pl.BlockSpec(memory_space=pltpu.SMEM)],
            out_specs=(vm, vm),
            scratch_shapes=scratch,
            compiler_params=pltpu.CompilerParams(
                collective_id=0, has_side_effects=True, vmem_limit_bytes=67043328),
            name='fgmres',
        )(source, initial, velocity, damping)

    return jax.shard_map(local_solve, mesh=mesh, in_specs=(grid_spec, grid_spec, vel_spec, table_spec),
                         out_specs=(grid_spec, table_spec), check_vma=False)
```

```python
import math
import jax
import jax.numpy as jnp
from jax import lax
from jax.experimental import pallas as pl
from jax.experimental.pallas import tpu as pltpu
from jax.sharding import PartitionSpec as P

MESH = pl.DeviceIdType.MESH
RESTART = 10
CYCLES = 2
XL = 12
NP = 2 * XL
PZ = XL + 2
LO, HI, ROWS = 8, 72, 80
XG, YG, ZG = slice(0, 32), slice(32, 56), slice(56, 120)
GROWS = 120
UN, UR, UC_ = 12, 2, 2


def pairs(unroll, body, carry=()):
    if unroll == XL:
        for i in range(XL):
            carry = body(i, carry)
        return carry

    def trip(t, carry):
        for i in range(unroll):
            carry = body(t * unroll + i, carry)
        return carry
    return lax.fori_loop(0, XL // unroll, trip, carry)


def groups(fn):
    def trip(t, carry):
        for i in range(5):
            fn(pl.ds(pl.multiple_of((t * 5 + i) * 8, 8), 8))
        return carry
    lax.fori_loop(0, GROWS // 40, trip, 0)


def v8(x):
    return x.reshape(-1, 8, 128)


def kernel(src_hbm, ini_hbm, vel_hbm, damp_ref, out_hbm, res_ref,
           U, NU, N2U, MU, Z, ZC, W, X, T1, T2, MW, SRC, CZP, CZM, HVX, HVY, CZA,
           GU, RB, SB, GZ, GX, SS, ACC, GM, RM, SIG, EC, CS, SN, GV, YY, NRM, RES, MISC, STG,
           s_send, s_recv, h_send, h_recv, x_recv, l_sem):
    f32 = jnp.float32
    gx, gy, gz = lax.axis_index('gx'), lax.axis_index('gy'), lax.axis_index('gz')
    peers = {}
    for p in range(1, 8):
        a, b, c = p // 4, (p // 2) % 2, p % 2
        peers[p] = {'gx': 1 - gx if a else gx, 'gy': 1 - gy if b else gy, 'gz': 1 - gz if c else gz}
    side = {0: 4, 1: 2, 2: 1}

    loads = [pltpu.make_async_copy(s, STG.at[i], l_sem.at[i]) for i, s in enumerate(
        (ini_hbm, vel_hbm.at[0], vel_hbm.at[1], vel_hbm.at[2], src_hbm))]
    for cp in loads:
        cp.start()
    bar = pltpu.get_barrier_semaphore()
    for p in range(1, 8):
        pl.semaphore_signal(bar, inc=1, device_id=peers[p], device_id_type=MESH)

    lane = lax.broadcasted_iota(jnp.int32, (64, 128), 1)
    lane8 = lane[0:8]
    left = lane < 64
    zh = jnp.where(left, jnp.where(lane < 32, lane, lane - 32), jnp.where(lane < 96, lane - 64, lane - 96))
    first_q, last_q = lane < 32, lane >= 96
    zero64 = jnp.zeros((64, 128), f32)
    zero8 = jnp.zeros((8, 128), f32)
    hi_x = (1 - gx).astype(f32)
    l0 = 31 * (1 - gz)
    o_x = 96 * (1 - gx)
    y_send = HI - 1 - 63 * gy
    y_pad = HI - 65 * gy
    edge_lo = zh == 32 * (1 - gz)
    edge_hi = zh == 31 + 32 * gz

    def seams(V, ghost=None):
        for zl in range(2):
            b = zl * PZ
            a = pltpu.roll(V[b + XL, LO:HI, :], 32, 1)
            d = pltpu.roll(V[b + 1, LO:HI, :], 96, 1)
            lo = 0.0 if ghost is None else ghost[zl] * (1.0 - hi_x)
            hi = 0.0 if ghost is None else ghost[zl] * hi_x
            V[b, LO:HI, :] = jnp.where(first_q, lo, a)
            V[b + XL + 1, LO:HI, :] = jnp.where(last_q, hi, d)

    def neighbours(V, i, ghost=None):
        u0, u1 = V[i + 1, LO:HI, :], V[i + (PZ + 1), LO:HI, :]
        below, above = pltpu.roll(u1, 1, 1), pltpu.roll(u0, 127, 1)
        if ghost is None:
            cm0, cp1 = CZM[i], CZP[i + XL]
        else:
            g = pltpu.roll(ghost, (l0 - i + 128) % 128, 1)
            below = jnp.where(edge_lo, g, below)
            above = jnp.where(edge_hi, g, above)
            cm0, cp1 = CZA[i], CZA[i + XL]
        out = []
        for zl, u, n in ((0, u0, CZP[i] * u1 + cm0 * below), (1, u1, CZM[i + XL] * u0 + cp1 * above)):
            q = i + (zl * PZ + 1)
            yp, ym = V[q, LO + 1:HI + 1, :], V[q, LO - 1:HI - 1, :]
            xp, xm = V[q + 1, LO:HI, :], V[q - 1, LO:HI, :]
            n = n + (xp + xm) - HVX[i + zl * XL] * (xp - xm)
            n = n + (yp + ym) - HVY[i + zl * XL] * (yp - ym)
            out.append((u, n))
        return out

    def fill_ghosts(V, rec):
        g = rec[XG, :]
        full = [jnp.concatenate([pltpu.roll(g, (o_x - 64 * zl - 32 * yh + 128) % 128, 1) for yh in range(2)], axis=0)
                for zl in range(2)]
        seams(V, full)

        def row(i, c):
            for zl in range(2):
                V[i + (zl * PZ + 1), pl.ds(y_pad, 1), :] = rec[pl.ds(i + (32 + zl * XL), 1), :]
            return c
        pairs(XL, row)

    def pack(plane, q):
        pd = (XL - 1) * (1 - gx)
        acc = zero64[0:32]
        for zl in range(2):
            v = plane(zl, pd)
            for yh in range(2):
                slot = 2 * zl + yh
                r = pltpu.roll(v[32 * yh:32 * yh + 32, :], (32 * slot - o_x + 128) % 128, 1)
                here = jnp.logical_and(lane[0:32] >= 32 * slot, lane[0:32] < 32 * slot + 32)
                acc = jnp.where(here, r, acc)
        SB[q, XG, :] = acc

        def row(i, acc):
            for zl in range(2):
                SB[q, pl.ds(i + (32 + zl * XL), 1), :] = plane(zl, i)[pl.ds(y_send - LO, 1), :]
            r = pltpu.roll(plane(1 - gz, i)[...], (i - l0 + 128) % 128, 1)
            return jnp.where(zh == i, r, acc)
        SB[q, ZG, :] = pairs(XL, row, zero64)

    def padded(V):
        return lambda zl, i: V.at[zl * PZ + i + 1, pl.ds(LO, 64), :]

    def dense(V):
        return lambda zl, i: V.at[zl * XL + i]

    def halo(q, dst, recv):
        return [pltpu.make_async_remote_copy(
            src_ref=SB.at[q, rows, :], dst_ref=dst.at[rows, :], send_sem=h_send, recv_sem=recv,
            device_id=peers[side[ax]], device_id_type=MESH) for ax, rows in ((0, XG), (1, YG), (2, ZG))]

    def halo_start(q, dst, recv):
        for cp in halo(q, dst, recv):
            cp.start()

    def halo_all(dst, recv):
        return pltpu.make_async_remote_copy(src_ref=SB, dst_ref=dst, send_sem=h_send, recv_sem=recv,
                                            device_id=peers[1], device_id_type=MESH)

    def sync_all(par):
        return pltpu.make_async_remote_copy(
            src_ref=SS.at[par, pl.ds(1, 7), :], dst_ref=SS.at[par, pl.ds(1, 7), :],
            send_sem=s_send.at[par], recv_sem=s_recv.at[par], device_id=peers[1], device_id_type=MESH)

    def sync_start(par, items):
        row = zero8
        for idx, acc in items:
            row = jnp.where(lane8 == idx, jnp.sum(acc, axis=1, keepdims=True), row)
        row = row + pltpu.roll(row, 4, 0)
        row = row + pltpu.roll(row, 2, 0)
        row = row + pltpu.roll(row, 1, 0)
        SS[par, 0:1, :] = row[0:1]
        for p in range(1, 8):
            pltpu.make_async_remote_copy(
                src_ref=SS.at[par, pl.ds(0, 1), :], dst_ref=SS.at[par, pl.ds(p, 1), :],
                send_sem=s_send.at[par], recv_sem=s_recv.at[par],
                device_id=peers[p], device_id_type=MESH).start()

    def sync_wait(par):
        sync_all(par).wait_recv()
        tot = SS[par]
        tot = tot + pltpu.roll(tot, 4, 0)
        tot = tot + pltpu.roll(tot, 2, 0)
        return tot + pltpu.roll(tot, 1, 0)

    def bc(tot, k):
        return jnp.broadcast_to(tot[:, k:k + 1], (8, 128))

    def fold(x):
        return jnp.sum(v8(x), axis=0)

    def poly(c, j):
        s = damp_ref[c, j] / 6.0
        a0, a1, a2 = 3.0 * s, 3.0 * s * s, s * s * s
        return a0 - 6.0 * a1 + 36.0 * a2, a1 - 12.0 * a2, a2

    @pl.loop(0, 2 * PZ)
    def _(p):
        for V in (ZC, W, X, T1.at[0], T1.at[1]):
            V[p, 0:LO, :] = zero8
            V[p, HI:ROWS, :] = zero8

    odd = jnp.where(left, 0, 1)
    pos = jnp.where(left, lane, lane - 64)
    deal = jnp.where(pos < 32, 2 * pos, 2 * pos) + odd

    def convert(ref, i):
        both = []
        for h in (0, 2):
            a = jnp.concatenate([ref[h * XL + i], ref[(h + 1) * XL + i]], axis=1)
            both.append(jnp.take_along_axis(a, deal, axis=1))
        p01, p23 = both
        return (jnp.where(left, p01, pltpu.roll(p23, 64, 1)), jnp.where(left, pltpu.roll(p01, 64, 1), p23))

    loads[0].wait()

    def load_x(i, c):
        for zl, v in enumerate(convert(STG.at[0], i)):
            X[i + (zl * PZ + 1), LO:HI, :] = v
        return c
    pairs(UC_, load_x)
    pack(padded(X), 0)
    pl.semaphore_wait(bar, 7)
    halo_start(0, GX, x_recv)
    for cp in loads[1:]:
        cp.wait()

    def load_rest(i, c):
        hx, hy, hz, sv = (convert(STG.at[q], i) for q in range(1, 5))
        for zl in range(2):
            r = i + zl * XL
            HVX[r] = 0.5 * hx[zl]
            HVY[r] = 0.5 * hy[zl]
            SRC[r] = sv[zl]
        cm0, cp1 = 1.0 + 0.5 * hz[0], 1.0 - 0.5 * hz[1]
        CZP[i] = 1.0 - 0.5 * hz[0]
        CZM[i] = jnp.where(zh == 0, 0.0, cm0)
        CZA[i] = jnp.where(zh == 32 * gz, 0.0, cm0)
        CZM[i + XL] = 1.0 + 0.5 * hz[1]
        CZP[i + XL] = jnp.where(zh == 31, 0.0, cp1)
        CZA[i + XL] = jnp.where(zh == 63 - 32 * gz, 0.0, cp1)
        return c
    pairs(UC_, load_rest)
    for cp in halo(0, GX, x_recv):
        cp.wait_send()
    pltpu.make_async_remote_copy(src_ref=SB.at[0], dst_ref=GX, send_sem=h_send, recv_sem=x_recv,
                                 device_id=peers[1], device_id_type=MESH).wait_recv()

    def residual(scale):
        fill_ghosts(X, GX)
        cz = GX[ZG, :]

        def one(i, acc):
            for zl, (u, n) in enumerate(neighbours(X, i, cz)):
                r = SRC[i + zl * XL] - (6.0 * u - n)
                if scale is not None:
                    r = (v8(r) * scale).reshape(64, 128)
                    U[0, i + zl * XL] = r
                W[i + (zl * PZ + 1), LO:HI, :] = r
                acc = acc + fold(r * r)
            return acc
        acc = pairs(UR, one, zero8)
        seams(W)
        return acc

    def apply_n(V, store, unroll):
        def one(i, c):
            for zl, (u, n) in enumerate(neighbours(V, i)):
                store(zl, i, u, n)
            return c
        pairs(unroll, one)

    def to_t1(b):
        def store(zl, i, u, n):
            T1[b, i + (zl * PZ + 1), LO:HI, :] = n
        return store

    def ghosts_of_z(k, q):
        def one(rows):
            GZ[k, rows, :] = q[0] * GU[k, 0, rows, :] + q[1] * GU[k, 1, rows, :] + q[2] * GU[k, 2, rows, :]
        groups(one)
        fill_ghosts(ZC, GZ.at[k])

    acc0 = residual(None)
    sync_start(0, [(16, acc0)])
    pack(padded(W), 0)
    halo_start(0, GU.at[0, 0], h_recv.at[1])
    apply_n(W, to_t1(0), UR)
    seams(T1.at[0])
    pack(padded(T1.at[0]), 1)
    halo_start(1, GU.at[0, 1], h_recv.at[1])

    def to_t2(zl, i, u, n):
        T2[0, i + zl * XL] = n
    apply_n(T1.at[0], to_t2, UR)
    pack(dense(T2.at[0]), 2)
    halo_start(2, GU.at[0, 2], h_recv.at[1])
    tot = sync_wait(0)
    sync_all(0).wait_send()
    beta0 = jnp.sqrt(bc(tot, 16))
    inv0 = 1.0 / beta0
    MISC[0] = beta0
    MISC[1] = inv0
    ACC[0] = acc0 * inv0 * inv0
    q0 = poly(0, 0)

    def scale_start(i, c):
        for zl in range(2):
            r = i + zl * XL
            u = (v8(W[i + (zl * PZ + 1), LO:HI, :]) * inv0).reshape(64, 128)
            n = (v8(T1[0, i + (zl * PZ + 1), LO:HI, :]) * inv0).reshape(64, 128)
            n2 = (v8(T2[0, r]) * inv0).reshape(64, 128)
            U[0, r] = u
            NU[0, r] = n
            N2U[0, r] = n2
            z = q0[0] * u + q0[1] * n + q0[2] * n2
            Z[0, r] = z
            ZC[i + (zl * PZ + 1), LO:HI, :] = z
        return c
    pairs(UR, scale_start)
    halo_all(GU.at[0], h_recv.at[1]).wait_recv()
    halo_all(GU.at[0], h_recv.at[1]).wait_send()

    def rescale_ghost(rows):
        for q in range(3):
            GU[0, q, rows, :] = GU[0, q, rows, :] * inv0
    groups(rescale_ghost)
    ghosts_of_z(0, q0)

    def givens(m, sub):
        h = [RM[i, m] for i in range(m + 1)]
        for i in range(m):
            cs, sn = CS[i], SN[i]
            h[i], h[i + 1] = cs * h[i] + sn * h[i + 1], cs * h[i + 1] - sn * h[i]
        d = h[m]
        rad = jnp.sqrt(d * d + sub * sub)
        cs, sn = d / rad, sub / rad
        CS[m] = cs
        SN[m] = sn
        h[m] = cs * d + sn * sub
        RM[0:m + 1, m] = jnp.stack(h)
        g = GV[m]
        GV[m] = cs * g
        GV[m + 1] = -sn * g
        est = MISC[4] * jnp.abs(sn)
        MISC[4] = est
        return est

    out_scale = 1.0 / math.sqrt(1572864.0)

    @pl.loop(0, CYCLES)
    def _(c):
        @pl.loop(0, RESTART)
        def _(j):
            step = c * RESTART + j
            par = (step + 1) % 2
            b = step % 2
            nxt = (j + 1) % RESTART
            slot = c * RESTART + (1 - c) * j + c * (j % 2)

            cz = GZ[j, ZG, :]

            def apply_a(i, cy):
                for zl, (u, n) in enumerate(neighbours(ZC, i, cz)):
                    W[i + (zl * PZ + 1), LO:HI, :] = 6.0 * u - n
                return cy
            pairs(UN, apply_a)

            for k in range(RESTART):
                @pl.when(j == k)
                def _():
                    ends = k == 0 or k == RESTART - 1
                    accs = (zero8,) * (k + 2 if ends else k + 1)

                    def dots(t, accs):
                        accs = list(accs)
                        w = W[pl.ds(t * 2 + 2 * (t // (XL // 2)) + 1, 2), LO:HI, :].reshape(16, 8, 128)
                        for i in range(k + 1):
                            v = U[i, pl.ds(t * 2, 2)].reshape(16, 8, 128)
                            accs[i] = accs[i] + jnp.sum(v * w, axis=0)
                        if ends:
                            accs[k + 1] = accs[k + 1] + jnp.sum(w * w, axis=0)
                        return tuple(accs)
                    accs = lax.fori_loop(0, XL, dots, accs)
                    items = [(i, accs[i]) for i in range(k + 1)] + [(16 + i, ACC[i]) for i in range(k + 1)]
                    if ends:
                        items.append((32, accs[k + 1]))
                    sync_start(par, items)

            @pl.when(step < CYCLES * RESTART - 1)
            def _():
                seams(W)
                pack(padded(W), 0)
                halo_start(0, RB.at[slot, 0], h_recv.at[b])
                apply_n(W, to_t1(b), UN)
                seams(T1.at[b])
                pack(padded(T1.at[b]), 1)
                halo_start(1, RB.at[slot, 1], h_recv.at[b])
                q0, q1, q2 = poly(c, nxt)

                def store(zl, i, u, n):
                    r = i + zl * XL
                    T2[b, r] = n
                    MW[r] = q0 * W[i + (zl * PZ + 1), LO:HI, :] + q1 * u + q2 * n
                apply_n(T1.at[b], store, UN)
                pack(dense(T2.at[b]), 2)
                halo_start(2, RB.at[slot, 2], h_recv.at[b])

            for k in range(RESTART):
                @pl.when(j == k)
                def _():
                    if k < RESTART - 1:
                        q0, q1, q2 = poly(c, k + 1)
                        e = [EC[i] for i in range(k + 1)] if k else None

                        def body(r, cy):
                            if k:
                                n = e[k] * v8(T1[1 - b, r + 2 * (r // XL) + 1, LO:HI, :])
                                n2 = e[k] * v8(T2[1 - b, r])
                                for m in range(k):
                                    nm, n2m = v8(NU[m, r]), v8(N2U[m, r])
                                    n = n - e[m] * nm
                                    n2 = n2 - e[m] * n2m
                                    MU[m, r] = (q0 * v8(U[m, r]) + q1 * nm + q2 * n2m).reshape(64, 128)
                                NU[k, r] = n.reshape(64, 128)
                                N2U[k, r] = n2.reshape(64, 128)
                            else:
                                n, n2 = v8(NU[0, r]), v8(N2U[0, r])
                            MU[k, r] = (q0 * v8(U[k, r]) + q1 * n + q2 * n2).reshape(64, 128)
                            return cy
                        lax.fori_loop(0, NP, body, 0)
                    if k >= 2:
                        est = givens(k - 2, NRM[k - 1] * MISC[3])
                        RES[c] = jnp.where(lane8 == k - 1, est, RES[c])

            tot = sync_wait(par)

            for k in range(RESTART):
                @pl.when(j == k)
                def _():
                    nn = bc(tot, 16 + k)
                    nrm = jnp.sqrt(nn)
                    sg = 1.0 / nrm
                    SIG[k] = sg
                    NRM[k] = nrm
                    sig = SIG[0:k + 1] * sg
                    h = jnp.stack([bc(tot, i) for i in range(k + 1)]) * sig
                    gcol = jnp.stack([bc(tot, 16 + i) for i in range(k + 1)]) * sig
                    GM[k, 0:k + 1] = gcol
                    if k > 0:
                        GM[0:k, k] = gcol[0:k]

                    def gram_times(x):
                        out = gcol * x[k]
                        for m in range(k):
                            out = out + GM[m, 0:k + 1] * x[m]
                        return out
                    cf = 2.0 * h - gram_times(h)
                    RM[0:k + 1, k] = cf
                    if k == 0:
                        beta = MISC[0] * nrm
                        MISC[4] = beta
                        GV[0] = beta
                        RES[c] = jnp.where(lane8 == 0, beta, 0.0)
                        wn = jnp.sqrt(bc(tot, 32)) * sg
                        MISC[3] = wn
                        rho = 1.0 / wn
                        MISC[2] = rho
                    else:
                        rho = MISC[2]
                    if k < RESTART - 1:
                        es = rho * cf * SIG[0:k + 1]
                        ew = rho * sg
                        EC[0:k + 1] = es
                        EC[k + 1] = ew

                        def body(r, accs):
                            accs = list(accs)
                            q = r + 2 * (r // XL) + 1
                            for y in range(0, 64, 16):
                                v = [v8(U[m, r, y:y + 16, :]) for m in range(k + 1)]
                                u = ew * v8(W[q, LO + y:LO + y + 16, :])
                                z = ew * v8(MW[r, y:y + 16, :])
                                for m in range(k + 1):
                                    u = u - es[m] * v[m]
                                    z = z - es[m] * v8(MU[m, r, y:y + 16, :])
                                U[k + 1, r, y:y + 16, :] = u.reshape(16, 128)
                                z = z.reshape(16, 128)
                                Z[k + 1, r, y:y + 16, :] = z
                                ZC[q, LO + y:LO + y + 16, :] = z
                                for m in range(k + 1):
                                    accs[m] = accs[m] + jnp.sum(u * v[m], axis=0)
                                accs[k + 1] = accs[k + 1] + jnp.sum(u * u, axis=0)
                            return tuple(accs)
                        accs = lax.fori_loop(0, NP, body, (zero8,) * (k + 2))
                        ACC[0:k + 2] = jnp.stack(accs)

                        halo_all(RB.at[slot], h_recv.at[b]).wait_recv()

                        def ghost_u(rows):
                            for q in range(3):
                                g = ew * RB[slot, q, rows, :]
                                for i in range(k + 1):
                                    g = g - es[i] * GU[i, q, rows, :]
                                GU[k + 1, q, rows, :] = g
                        groups(ghost_u)
                    else:
                        wn2 = bc(tot, 32) * sg * sg
                        drop = jnp.sum(cf * (2.0 * h - gram_times(cf)), axis=0)
                        sub = jnp.sqrt(jnp.maximum(wn2 - drop, 0.0))
                        est = givens(k - 1, nrm * MISC[3])
                        RES[c] = jnp.where(lane8 == k, est, RES[c])
                        est = givens(k, sub)
                        RES[c] = jnp.where(lane8 == k + 1, est, RES[c])
                        g = [GV[i] for i in range(RESTART)]
                        for i in reversed(range(RESTART)):
                            y = g[i] / RM[i, i]
                            YY[i] = y * SIG[i]
                            for m in range(i):
                                g[m] = g[m] - RM[m, i] * y

            @pl.when(j < RESTART - 1)
            def _():
                ghosts_of_z(nxt, poly(c, nxt))
            sync_all(par).wait_send()

            @pl.when(step < CYCLES * RESTART - 1)
            def _():
                halo_all(RB.at[slot], h_recv.at[b]).wait_send()

        yy = [YY[i] for i in range(RESTART)]

        @pl.when(c == 0)
        def _():
            def update(i, cy):
                for zl in range(2):
                    q, r = i + (zl * PZ + 1), i + zl * XL
                    x = v8(X[q, LO:HI, :])
                    for m in range(RESTART):
                        x = x + yy[m] * v8(Z[m, r])
                    X[q, LO:HI, :] = x.reshape(64, 128)
                return cy
            pairs(1, update)

            def ghost_x(rows):
                g = GX[rows, :]
                for m in range(RESTART):
                    g = g + yy[m] * GZ[m, rows, :]
                GX[rows, :] = g
            groups(ghost_x)
            inv = MISC[1]
            ACC[0] = residual(inv)
            halo_all(RB.at[RESTART - 1], h_recv.at[1]).wait_recv()

            def ghost_r(rows):
                for q in range(3):
                    g = zero8
                    for m in range(RESTART):
                        g = g + yy[m] * RB[m, q, rows, :]
                    GU[0, q, rows, :] = GU[0, q, rows, :] - inv * g
            groups(ghost_r)

            apply_n(W, to_t1(0), UR)
            seams(T1.at[0])
            q0, q1, q2 = poly(1, 0)

            def first_z(zl, i, u, n):
                r = i + zl * XL
                NU[0, r] = u
                N2U[0, r] = n
                z = q0 * U[0, r] + q1 * u + q2 * n
                Z[0, r] = z
                ZC[i + (zl * PZ + 1), LO:HI, :] = z
            apply_n(T1.at[0], first_z, UR)
            ghosts_of_z(0, (q0, q1, q2))

        @pl.when(c == CYCLES - 1)
        def _():
            def update(i, cy):
                for zl in range(2):
                    q, r = i + (zl * PZ + 1), i + zl * XL
                    x = v8(X[q, LO:HI, :])
                    for m in range(RESTART):
                        x = x + yy[m] * v8(Z[m, r])
                    SRC[r] = x.reshape(64, 128)
                return cy
            pairs(1, update)

    cp = pltpu.make_async_copy(SRC, out_hbm, l_sem.at[0])
    cp.start()
    rows = jnp.where(lax.broadcasted_iota(jnp.int32, (8, 128), 0) == 0, RES[0], RES[1]) * out_scale
    res_ref[...] = rows
    cp.wait()


def unpack(x_ref, r_ref, out_ref, res_ref):
    lane = lax.broadcasted_iota(jnp.int32, (64, 128), 1)
    left = lane < 64
    z = jnp.where(left, lane, lane - 64)
    half = lax.shift_right_logical(z, 1)
    deal = half + 64 * (z - 2 * half) + jnp.where(left, 0, 32)
    for i in range(x_ref.shape[1]):
        e, o = x_ref[0, i], x_ref[1, i]
        for h, p in ((0, jnp.where(left, e, pltpu.roll(o, 64, 1))), (2, jnp.where(left, pltpu.roll(e, 64, 1), o))):
            a = jnp.take_along_axis(p, deal, axis=1)
            out_ref[h, i] = a[:, 0:64]
            out_ref[h + 1, i] = a[:, 64:128]
    res_ref[...] = r_ref[0:CYCLES, 0:RESTART + 1]


def solution(mesh):
    grid_spec = P(('sys', 'gx'), 'gy', 'gz')
    vel_spec = P(None, ('sys', 'gx'), 'gy', 'gz')
    table_spec = P('sys', None)
    f32 = jnp.float32

    def local_solve(source, initial, velocity, damping):
        big = (2 * PZ, ROWS, 128)
        vol = (NP, 64, 128)
        v = lambda *s: pltpu.VMEM(s, f32)
        n = RESTART
        scratch = [
            v(n, *vol), v(n - 1, *vol), v(n - 1, *vol), v(n - 1, *vol), v(n, *vol),
            v(*big), v(*big), v(*big), v(2, *big), v(2, *vol), v(*vol),
            v(*vol), v(*vol), v(*vol), v(*vol), v(*vol), v(*vol),
            v(n, 3, GROWS, 128), v(n + 2, 3, GROWS, 128), v(3, GROWS, 128), v(n, GROWS, 128), v(GROWS, 128),
            v(2, 8, 128), v(n + 1, 8, 128), v(n, n, 8, 128), v(n, n, 8, 128),
            v(n, 8, 128), v(n + 1, 8, 128), v(n, 8, 128), v(n, 8, 128), v(n + 1, 8, 128), v(n, 8, 128), v(n, 8, 128),
            v(CYCLES, 8, 128), v(8, 8, 128), v(5, 48, 64, 64),
            pltpu.SemaphoreType.DMA((2,)), pltpu.SemaphoreType.DMA((2,)), pltpu.SemaphoreType.DMA,
            pltpu.SemaphoreType.DMA((2,)), pltpu.SemaphoreType.DMA, pltpu.SemaphoreType.DMA((5,)),
        ]
        hbm = pl.BlockSpec(memory_space=pl.ANY)
        packed, rows = pl.pallas_call(
            kernel,
            out_shape=(jax.ShapeDtypeStruct(vol, f32), jax.ShapeDtypeStruct((8, 128), f32)),
            in_specs=[hbm, hbm, hbm, pl.BlockSpec(memory_space=pltpu.SMEM)],
            out_specs=(hbm, pl.BlockSpec(memory_space=pltpu.VMEM)),
            scratch_shapes=scratch,
            compiler_params=pltpu.CompilerParams(
                collective_id=0, has_side_effects=True, vmem_limit_bytes=67043328),
            name='fgmres',
        )(source, initial, velocity, damping)
        step = 3
        out, res = pl.pallas_call(
            unpack,
            grid=(XL // step,),
            out_shape=(jax.ShapeDtypeStruct((4, XL, 64, 64), f32), jax.ShapeDtypeStruct((CYCLES, n + 1), f32)),
            in_specs=[pl.BlockSpec((2, step, 64, 128), lambda i: (0, i, 0, 0)), pl.BlockSpec((8, 128), lambda i: (0, 0))],
            out_specs=(pl.BlockSpec((4, step, 64, 64), lambda i: (0, i, 0, 0)),
                       pl.BlockSpec((CYCLES, n + 1), lambda i: (0, 0))),
            name='unpack',
        )(packed.reshape(2, XL, 64, 128), rows)
        return out.reshape(source.shape), res

    return jax.shard_map(local_solve, mesh=mesh, in_specs=(grid_spec, grid_spec, vel_spec, table_spec),
                         out_specs=(grid_spec, table_spec), check_vma=False)
```

```python
import math
import jax
import jax.numpy as jnp
from jax import lax
from jax.experimental import pallas as pl
from jax.experimental.pallas import tpu as pltpu
from jax.sharding import PartitionSpec as P

MESH = pl.DeviceIdType.MESH
RESTART = 10
CYCLES = 2
XL = 12
NP = 2 * XL
PZ = XL + 2
LO, HI, ROWS = 8, 72, 80
SETR = 2 * PZ * ROWS
LATE = 8
XG, YG, ZG = slice(0, 32), slice(32, 56), slice(56, 120)
GROWS = 120
UX = 2


def pairs(unroll, body, carry=()):
    if unroll == XL:
        for i in range(XL):
            carry = body(i, carry)
        return carry

    def trip(t, carry):
        for i in range(unroll):
            carry = body(t * unroll + i, carry)
        return carry
    return lax.fori_loop(0, XL // unroll, trip, carry)


def v8(x):
    return x.reshape(-1, 8, 128)


class Set:
    def __init__(self, ref, t=None):
        self.ref, self.t = ref, t

    def index(self, start, size):
        rows = pl.ds(start, size) if not isinstance(start, int) else slice(start, start + size)
        return (rows, slice(None)) if self.t is None else (self.t, rows, slice(None))

    def get(self, start, size):
        return self.ref[self.index(start, size)]

    def put(self, start, size, v):
        self.ref[self.index(start, size)] = v

    def view(self, start, size):
        return self.ref.at[self.index(start, size)]


def row0(p):
    r = p * ROWS + LO
    return r if isinstance(r, int) else pl.multiple_of(r, 8)


def one_plane(body, carry):
    def outer(zl, carry):
        return lax.fori_loop(0, XL, lambda x, cy: body(zl * XL + x, row0(zl * PZ + x + 1), cy), carry)
    return lax.fori_loop(0, 2, outer, carry)


def all_planes(body, carry, step=1):
    def trip(t, carry):
        for zl in range(2):
            for i in range(step):
                x = t * step + i
                carry = body(x + zl * XL, row0(x + (zl * PZ + 1)), carry)
        return carry
    return lax.fori_loop(0, XL // step, trip, carry)


def kernel(src_hbm, ini_hbm, vel_hbm, damp_ref, out_hbm, res_ref,
           U, NU, N2U, MU, Z, ZC, X, VV, MW, SRC, CZP, CZM, HVX, HVY, CZA, CGX, CGY, YB,
           GU, GMU, RB, RU, SB, SU, GZ, GX, GX2, SS, ACC, GM, RM, SIG, EC, CS, SN, GV, YY, NRM, RES, MISC, STG,
           s_send, s_recv, h_send, h_recv, u_send, u_recv, z_send, z_recv, x_recv, l_sem):
    f32 = jnp.float32
    gx, gy, gz = lax.axis_index('gx'), lax.axis_index('gy'), lax.axis_index('gz')
    peers = {}
    for p in range(1, 8):
        a, b, c = p // 4, (p // 2) % 2, p % 2
        peers[p] = {'gx': 1 - gx if a else gx, 'gy': 1 - gy if b else gy, 'gz': 1 - gz if c else gz}
    side = {0: 4, 1: 2, 2: 1}

    load_x = pltpu.make_async_copy(ini_hbm, STG.at[0], l_sem.at[0])
    load_x.start()
    load_v = [pltpu.make_async_copy(vel_hbm.at[d], STG.at[1 + d], l_sem.at[1 + d]) for d in range(3)]
    load_s = pltpu.make_async_copy(src_hbm, STG.at[0], l_sem.at[0])
    bar = pltpu.get_barrier_semaphore()
    for p in range(1, 8):
        pl.semaphore_signal(bar, inc=1, device_id=peers[p], device_id_type=MESH)

    lane = lax.broadcasted_iota(jnp.int32, (64, 128), 1)
    lane8 = lane[0:8]
    left = lane < 64
    zh = jnp.where(left, jnp.where(lane < 32, lane, lane - 32), jnp.where(lane < 96, lane - 64, lane - 96))
    zh32 = zh[0:32]
    first_q, last_q = lane < 32, lane >= 96
    zero64 = jnp.zeros((64, 128), f32)
    zero8 = jnp.zeros((8, 128), f32)
    hi_x = (1 - gx).astype(f32)
    l0 = 31 * (1 - gz)
    o_x = 96 * (1 - gx)
    y_send = 63 * (1 - gy)
    y_pad = HI - 65 * gy
    edge_lo = zh32 == 32 * (1 - gz)
    edge_hi = zh32 == 31 + 32 * gz
    WS, ZS, XS = Set(VV, 0), Set(ZC), Set(X)

    def seams(V, ghost=None):
        for zl in range(2):
            b = zl * PZ
            a = pltpu.roll(V.get(row0(b + XL), 64), 32, 1)
            d = pltpu.roll(V.get(row0(b + 1), 64), 96, 1)
            lo = 0.0 if ghost is None else ghost[zl] * (1.0 - hi_x)
            hi = 0.0 if ghost is None else ghost[zl] * hi_x
            V.put(row0(b), 64, jnp.where(first_q, lo, a))
            V.put(row0(b + XL + 1), 64, jnp.where(last_q, hi, d))

    def neighbours(V, i, put, ghost=None):
        size = 64 if ghost is None else 32
        for y in range(0, 64, size):
            co = lambda C, r: C[r * 64 + y:r * 64 + y + size, :]
            at = lambda q, d: V.get(row0(q) + y + d, size)
            u0, u1 = at(i + 1, 0), at(i + (PZ + 1), 0)
            below, above = pltpu.roll(u1, 1, 1), pltpu.roll(u0, 127, 1)
            if ghost is None:
                cm0, cp1 = co(CZM, i), co(CZP, i + XL)
            else:
                g = pltpu.roll(ghost[y:y + size, :], (l0 - i + 128) % 128, 1)
                below = jnp.where(edge_lo, g, below)
                above = jnp.where(edge_hi, g, above)
                cm0, cp1 = co(CZA, i), co(CZA, i + XL)
            for zl, u, n in ((0, u0, co(CZP, i) * u1 + cm0 * below), (1, u1, co(CZM, i + XL) * u0 + cp1 * above)):
                q, r = i + (zl * PZ + 1), i + zl * XL
                yp, ym = at(q, 1), at(q, -1)
                xp, xm = at(q + 1, 0), at(q - 1, 0)
                n = n + (xp + xm) - co(HVX, r) * (xp - xm)
                n = n + (yp + ym) - co(HVY, r) * (yp - ym)
                put(r * 8 + y // 8, row0(q) + y, size, u, n)

    def spread_x(rec):
        g = rec[XG, :]
        return [jnp.concatenate([pltpu.roll(g, (o_x - 64 * zl - 32 * yh + 128) % 128, 1) for yh in range(2)], axis=0)
                for zl in range(2)]

    def fill_ghosts(V, rec):
        seams(V, spread_x(rec))

        @pl.loop(0, 2)
        def _(zl):
            for i in range(XL):
                V.put((zl * PZ + (i + 1)) * ROWS + y_pad, 1, rec[pl.ds(zl * XL + (i + 32), 1), :])

    def add_ghosts_xy(rec):
        pd = (XL - 1) * (1 - gx)
        for zl, g in enumerate(spread_x(rec)):
            row = (pd + (zl * PZ + 1)) * ROWS + LO
            WS.put(row, 64, WS.get(row, 64) - CGX[64 * zl:64 * zl + 64, :] * g)
        YB[...] = CGY[...] * rec[YG, :]
        for r in range(NP):
            row = row0(r % XL + r // XL * PZ + 1) + y_send
            WS.put(row, 1, WS.get(row, 1) - YB[r:r + 1, :])

    def pack_xy(get, out):
        pd = (XL - 1) * (1 - gx)
        acc = zero64[0:32]
        for zl in range(2):
            for yh in range(2):
                slot = 2 * zl + yh
                r = pltpu.roll(get(zl, pd, 32 * yh, 32), (32 * slot - o_x + 128) % 128, 1)
                here = jnp.logical_and(lane[0:32] >= 32 * slot, lane[0:32] < 32 * slot + 32)
                acc = jnp.where(here, r, acc)
        out[XG, :] = acc

        @pl.loop(0, 2)
        def _(zl):
            for i in range(XL):
                out[pl.ds(zl * XL + (i + 32), 1), :] = get(zl, i, y_send, 1)

    def pack_z(get, out):
        acc = zero64
        for i in range(XL):
            r = pltpu.roll(get(1 - gz, i, 0, 64), (i - l0 + 128) % 128, 1)
            acc = jnp.where(zh == i, r, acc)
        out[ZG, :] = acc

    def pack(get, out):
        pack_xy(get, out)
        pack_z(get, out)

    def of_set(V):
        return lambda zl, i, y, n: V.get((zl * PZ + i + 1) * ROWS + LO + y, n)

    def of_mw(zl, i, y, n):
        return MW[pl.ds((zl * XL + i) * 64 + y, n), :]

    def halo_start(src, dst, send, recv, axes=(0, 1, 2)):
        for ax in axes:
            rows = (XG, YG, ZG)[ax]
            pltpu.make_async_remote_copy(
                src_ref=src.at[rows, :], dst_ref=dst.at[rows, :], send_sem=send, recv_sem=recv,
                device_id=peers[side[ax]], device_id_type=MESH).start()

    def whole(src, dst, send, recv):
        return pltpu.make_async_remote_copy(src_ref=src, dst_ref=dst, send_sem=send, recv_sem=recv,
                                            device_id=peers[1], device_id_type=MESH)

    def three(b, dst, recv):
        @pl.loop(0, 3)
        def _(q):
            pack(of_set(Set(VV, 2 * q + (b - 1) * ((q + 1) // 2))), SB.at[q])
            halo_start(SB.at[q], dst.at[q], h_send, recv)

    def sync_all(par):
        return pltpu.make_async_remote_copy(
            src_ref=SS.at[par, pl.ds(1, 7), :], dst_ref=SS.at[par, pl.ds(1, 7), :],
            send_sem=s_send.at[par], recv_sem=s_recv.at[par], device_id=peers[1], device_id_type=MESH)

    def sync_start(par, items):
        row = zero8
        for idx, acc in items:
            row = jnp.where(lane8 == idx, jnp.sum(acc, axis=1, keepdims=True), row)
        row = row + pltpu.roll(row, 4, 0)
        row = row + pltpu.roll(row, 2, 0)
        row = row + pltpu.roll(row, 1, 0)
        SS[par, 0:1, :] = row[0:1]
        for p in range(1, 8):
            pltpu.make_async_remote_copy(
                src_ref=SS.at[par, pl.ds(0, 1), :], dst_ref=SS.at[par, pl.ds(p, 1), :],
                send_sem=s_send.at[par], recv_sem=s_recv.at[par],
                device_id=peers[p], device_id_type=MESH).start()

    def sync_wait(par):
        sync_all(par).wait_recv()
        tot = SS[par]
        tot = tot + pltpu.roll(tot, 4, 0)
        tot = tot + pltpu.roll(tot, 2, 0)
        return tot + pltpu.roll(tot, 1, 0)

    def bc(tot, k):
        return jnp.broadcast_to(tot[:, k:k + 1], (8, 128))

    def fold(x):
        return jnp.sum(v8(x), axis=0)

    def poly(c, j):
        s = damp_ref[c, j] / 6.0
        a0, a1, a2 = 3.0 * s, 3.0 * s * s, s * s * s
        q = jnp.full((8, 128), a0 - 6.0 * a1 + 36.0 * a2, f32)
        return q, (a1 - 12.0 * a2) / q, a2 / q

    @pl.loop(0, 2 * PZ)
    def _(p):
        for V in (ZS, XS, WS, Set(VV, 1), Set(VV, 2)):
            V.put(pl.multiple_of(p * ROWS, 8), 8, zero8)
            V.put(pl.multiple_of(p * ROWS + HI, 8), 8, zero8)

    pos = jnp.where(left, lane, lane - 64)
    deal = 2 * pos + jnp.where(left, 0, 1)

    def convert(ref, i):
        both = []
        for h in (0, 2):
            a = jnp.concatenate([ref[h * XL + i], ref[(h + 1) * XL + i]], axis=1)
            both.append(jnp.take_along_axis(a, deal, axis=1))
        p01, p23 = both
        return (jnp.where(left, p01, pltpu.roll(p23, 64, 1)), jnp.where(left, pltpu.roll(p01, 64, 1), p23))

    load_x.wait()
    for cp in load_v:
        cp.start()

    def take_x(i, c):
        for zl, v in enumerate(convert(STG.at[0], i)):
            XS.put(row0(i + (zl * PZ + 1)), 64, v)
        return c
    pairs(UX, take_x)
    load_s.start()
    pack(of_set(XS), SU)
    pl.semaphore_wait(bar, 7)
    halo_start(SU, GX, u_send, x_recv)

    for d, store in ((0, HVX), (1, HVY)):
        load_v[d].wait()

        def take_h(i, c):
            for zl, v in enumerate(convert(STG.at[1 + d], i)):
                store[pl.ds(pl.multiple_of((i + zl * XL) * 64, 8), 64), :] = 0.5 * v
            return c
        pairs(UX, take_h)
    load_v[2].wait()

    def take_z(i, c):
        h0, h1 = convert(STG.at[3], i)
        cm0, cp1 = 1.0 + 0.5 * h0, 1.0 - 0.5 * h1
        low = pl.ds(pl.multiple_of(i * 64, 8), 64)
        high = pl.ds(pl.multiple_of((i + XL) * 64, 8), 64)
        CZP[low, :] = 1.0 - 0.5 * h0
        CZM[low, :] = jnp.where(zh == 0, 0.0, cm0)
        CZA[low, :] = jnp.where(zh == 32 * gz, 0.0, cm0)
        CZM[high, :] = 1.0 + 0.5 * h1
        CZP[high, :] = jnp.where(zh == 31, 0.0, cp1)
        CZA[high, :] = jnp.where(zh == 63 - 32 * gz, 0.0, cp1)
        return c
    pairs(UX, take_z)
    pd = (XL - 1) * (1 - gx)
    at_x = jnp.logical_and(lane >= o_x, lane < o_x + 32)
    sign_x, sign_y = (2 * gx - 1).astype(f32), (2 * gy - 1).astype(f32)
    for zl in range(2):
        hv = HVX[pl.ds(pl.multiple_of((zl * XL + pd) * 64, 8), 64), :]
        CGX[64 * zl:64 * zl + 64, :] = jnp.where(at_x, 1.0 + sign_x * hv, 0.0)

    @pl.loop(0, NP)
    def _(r):
        CGY[pl.ds(r, 1), :] = 1.0 + sign_y * HVY[pl.ds(r * 64 + y_send, 1), :]
    load_s.wait()

    def take_s(i, c):
        for zl, v in enumerate(convert(STG.at[0], i)):
            SRC[pl.ds(pl.multiple_of((i + zl * XL) * 64, 8), 64), :] = v
        return c
    pairs(UX, take_s)
    whole(SU, GX, u_send, x_recv).wait()

    def halo_xy(dst, recv):
        return whole(SU.at[pl.ds(0, 56), :], dst.at[pl.ds(0, 56), :], u_send, recv)

    def halo_z(dst, recv):
        return whole(SU.at[pl.ds(56, 64), :], dst.at[pl.ds(56, 64), :], z_send, recv)

    def ghost_of_z(k, e, ew, b, q, rows):
        g = ew * v8(RU[b, rows, :])
        for i in range(k):
            g = g - e[i] * v8(GMU[i, rows, :])
        GZ[k, rows, :] = (q * g).reshape(-1, 128)

    def sweep(V, unroll, put, ghost=None):
        def one(i, c):
            neighbours(V, i, put, ghost)
            return c
        pairs(unroll, one)

    def to_n(V):
        def put(r8, row, size, u, n):
            V.put(row, size, n)
        return put

    def givens(m, sub):
        h = [RM[i, m] for i in range(m + 1)]
        for i in range(m):
            cs, sn = CS[i], SN[i]
            h[i], h[i + 1] = cs * h[i] + sn * h[i + 1], cs * h[i + 1] - sn * h[i]
        d = h[m]
        rad = jnp.sqrt(d * d + sub * sub)
        cs, sn = d / rad, sub / rad
        CS[m] = cs
        SN[m] = sn
        h[m] = cs * d + sn * sub
        RM[0:m + 1, m] = jnp.stack(h)
        g = GV[m]
        GV[m] = cs * g
        GV[m + 1] = -sn * g
        est = MISC[4] * jnp.abs(sn)
        MISC[4] = est
        return est

    out_scale = 1.0 / math.sqrt(1572864.0)
    last_halo = CYCLES * RESTART - 3

    @pl.loop(0, CYCLES)
    def _(c):
        fill_ghosts(XS, GX)

        def put_r(r8, row, size, u, n):
            WS.put(row, size, SRC[r8 * 8:r8 * 8 + size, :] - (6.0 * u - n))
        sweep(XS, XL, put_r, GX.at[ZG, :])

        @pl.when(c == 0)
        def _():
            def one(r, row, acc):
                t = v8(WS.get(row, 64)).reshape(2, 4, 8, 128)
                return acc + jnp.sum(t * t, axis=0)
            acc = all_planes(one, jnp.zeros((4, 8, 128), f32), 2)
            sync_start(0, [(16, jnp.sum(acc, axis=0))])

        @pl.loop(0, RESTART)
        def _(j):
            step = c * RESTART + j
            par = (step + 1) % 2
            b = step % 2
            nxt = (j + 1) % RESTART
            slot = c * RESTART + (1 - c) * j + c * (j % 3)

            @pl.when(j * (j - LATE) >= 0)
            def _():
                seams(WS)
                sweep(WS, XL, to_n(Set(VV, 1)))
                seams(Set(VV, 1))

            @pl.when(j >= LATE)
            def _():
                q, r1, r2 = (jnp.concatenate([t] * 8, axis=0) for t in poly(c, j))

                def put_z(r8, row, size, u, n):
                    z = q * (WS.get(row, size) + r1 * u + r2 * n)
                    ZS.put(row, size, z)
                    Z[j, r8:r8 + size // 8] = v8(z)
                sweep(Set(VV, 1), XL, put_z)

            @pl.when(j == 0)
            def _():
                sweep(Set(VV, 1), XL, to_n(Set(VV, 3)))

                @pl.when(c == 0)
                def _():
                    three(0, GU.at[0], h_recv.at[1])
                    tot = sync_wait(0)
                    sync_all(0).wait_send()
                    beta0 = jnp.sqrt(bc(tot, 16))
                    MISC[0] = beta0
                    MISC[1] = 1.0 / beta0

                inv0 = MISC[1]
                q, r1, r2 = poly(c, 0)

                def start(r, row, acc):
                    u, n, n2 = (v8(Set(VV, t).get(row, 64)) * inv0 for t in (0, 1, 3))
                    z = q * (u + r1 * n + r2 * n2)
                    acc = acc + jnp.sum((u * u).reshape(2, 4, 8, 128), axis=0)
                    at = pl.ds(r * 8, 8)
                    U[0, at] = u
                    NU[0, at] = n
                    N2U[0, at] = n2
                    Z[0, at] = z
                    ZS.put(row, 64, z.reshape(64, 128))
                    return acc
                ACC[0] = jnp.sum(all_planes(start, jnp.zeros((4, 8, 128), f32)), axis=0)

                @pl.when(c == 0)
                def _():
                    whole(SB, GU.at[0], h_send, h_recv.at[1]).wait()

                    for t in range(3):
                        GU[0, t] = (v8(GU[0, t]) * inv0).reshape(GROWS, 128)

                GZ[0] = (q * (v8(GU[0, 0]) + r1 * v8(GU[0, 1]) + r2 * v8(GU[0, 2]))).reshape(GROWS, 128)

            seams(ZS)
            GX2[...] = GZ[j, ZG, :]

            def put_w(r8, row, size, u, n):
                WS.put(row, size, 6.0 * u - n)
            sweep(ZS, XL, put_w, GX2)

            for k in range(1, RESTART):
                @pl.when(j == k)
                def _():
                    halo_xy(RU.at[1 - b], u_recv.at[1 - b]).wait_recv()
                    ghost_of_z(k, [EC[i] for i in range(k)], EC[k], 1 - b, poly(c, k)[0], slice(0, 56))
            add_ghosts_xy(GZ.at[j])

            for k in range(RESTART):
                @pl.when(j == k)
                def _():
                    ends = k == 0 or k == RESTART - 1
                    wd = 4 if k < 4 else 2 if k < 8 else 1
                    count = k + 2 if ends else k + 1

                    def dots(t, accs):
                        accs = list(accs)
                        for zl in range(2):
                            x = t * 2 + zl * XL
                            w = jnp.concatenate([v8(WS.get(row0(t * 2 + (zl * PZ + 1 + i)), 64)) for i in range(2)])
                            w = w.reshape(16 // wd, wd, 8, 128)
                            for i in range(k + 1):
                                v = U[i, pl.ds(x * 8, 16)].reshape(16 // wd, wd, 8, 128)
                                accs[i] = accs[i] + jnp.sum(v * w, axis=0)
                            if ends:
                                accs[k + 1] = accs[k + 1] + jnp.sum(w * w, axis=0)
                        return tuple(accs)
                    accs = lax.fori_loop(0, XL // 2, dots, (jnp.zeros((wd, 8, 128), f32),) * count)
                    accs = [jnp.sum(a, axis=0) for a in accs]
                    items = [(i, accs[i]) for i in range(k + 1)] + [(16 + i, ACC[i]) for i in range(k + 1)]
                    if ends:
                        items.append((32, accs[k + 1]))
                    sync_start(par, items)

            @pl.when(step > 0)
            def _():
                sync_all(1 - par).wait_send()

            @pl.when(step < CYCLES * RESTART - 1)
            def _():
                seams(WS)
                sweep(WS, XL, to_n(Set(VV, 1 + b)))
                seams(Set(VV, 1 + b))
                r1, r2 = (jnp.concatenate([t] * 8, axis=0) for t in poly(c, nxt)[1:])

                def put(r8, row, size, u, n):
                    Set(VV, 3 + b).put(row, size, n)
                    MW[r8 * 8:r8 * 8 + size, :] = WS.get(row, size) + r1 * u + r2 * n
                sweep(Set(VV, 1 + b), XL, put)

            @pl.when(j > 0)
            def _():
                halo_xy(RU.at[b], u_recv.at[b]).wait_send()
                halo_z(RU.at[b], z_recv.at[b]).wait_send()

            @pl.when(j < RESTART - 1)
            def _():
                pack_xy(of_mw, SU)
                halo_start(SU, RU.at[b], u_send, u_recv.at[b], (0, 1))
                pack_z(of_mw, SU)
                halo_start(SU, RU.at[b], z_send, z_recv.at[b], (2,))

            @pl.when(step <= last_halo + 1)
            def _():
                @pl.when(step > 0)
                def _():
                    whole(SB, RB.at[slot], h_send, h_recv.at[0]).wait_send()

                @pl.when(step <= last_halo)
                def _():
                    three(b, RB.at[slot], h_recv.at[step % 3])

                @pl.when(j > 0)
                def _():
                    whole(SB, RB.at[slot], h_send, h_recv.at[(step + 2) % 3]).wait_recv()

            prev = c * RESTART + (1 - c) * (j - 1) + c * ((j + 2) % 3)
            for k in range(RESTART):
                @pl.when(j == k)
                def _():
                    if k < RESTART - 1:
                        q, r1, r2 = poly(c, k + 1)
                        e = [EC[i] for i in range(k + 1)] if k else None

                        size = 8 if k < 4 else 4

                        def body(r, row, cy):
                            for y in range(0, 8, size):
                                at = pl.ds(r * 8 + y, size)
                                if k:
                                    n = e[k] * v8(Set(VV, 2 - b).get(row + 8 * y, 8 * size))
                                    n2 = e[k] * v8(Set(VV, 4 - b).get(row + 8 * y, 8 * size))
                                    for m in range(k):
                                        nm, n2m = NU[m, at], N2U[m, at]
                                        n = n - e[m] * nm
                                        n2 = n2 - e[m] * n2m
                                        MU[m, at] = U[m, at] + r1 * nm + r2 * n2m
                                    NU[k, at] = n
                                    N2U[k, at] = n2
                                else:
                                    n, n2 = NU[0, at], N2U[0, at]
                                MU[k, at] = U[k, at] + r1 * n + r2 * n2
                            return cy
                        if k < LATE - 1:
                            (all_planes if k < 4 else one_plane)(body, 0)

                        if k:
                            for t in range(3):
                                g = e[k] * v8(RB[prev, t])
                                for i in range(k):
                                    g = g - e[i] * v8(GU[i, t])
                                GU[k, t] = g.reshape(GROWS, 128)

                        @pl.loop(0, k + 1)
                        def _(i):
                            g = v8(GU[i, 0]) + r1 * v8(GU[i, 1]) + r2 * v8(GU[i, 2])
                            GMU[i] = g.reshape(GROWS, 128)
                    if k >= 2:
                        est = givens(k - 2, NRM[k - 1] * MISC[3])
                        RES[c] = jnp.where(lane8 == k - 1, est, RES[c])

            tot = sync_wait(par)

            for k in range(RESTART):
                @pl.when(j == k)
                def _():
                    nn = bc(tot, 16 + k)
                    nrm = jnp.sqrt(nn)
                    sg = 1.0 / nrm
                    SIG[k] = sg
                    NRM[k] = nrm
                    sig = SIG[0:k + 1] * sg
                    h = jnp.stack([bc(tot, i) for i in range(k + 1)]) * sig
                    gcol = jnp.stack([bc(tot, 16 + i) for i in range(k + 1)]) * sig
                    GM[k, 0:k + 1] = gcol
                    if k > 0:
                        GM[0:k, k] = gcol[0:k]

                    def gram_times(x):
                        out = gcol * x[k]
                        for m in range(k):
                            out = out + GM[m, 0:k + 1] * x[m]
                        return out
                    cf = 2.0 * h - gram_times(h)
                    RM[0:k + 1, k] = cf
                    if k == 0:
                        beta = MISC[0] * nrm
                        MISC[4] = beta
                        GV[0] = beta
                        RES[c] = jnp.where(lane8 == 0, beta, 0.0)
                        wn = jnp.sqrt(bc(tot, 32)) * sg
                        MISC[3] = wn
                        rho = 1.0 / wn
                        MISC[2] = rho
                    else:
                        rho = MISC[2]
                    if k < RESTART - 1:
                        es = rho * cf * SIG[0:k + 1]
                        ew = rho * sg
                        EC[0:k + 1] = es
                        EC[k + 1] = ew
                        q = poly(c, k + 1)[0]

                        size = 8 if k < 2 else 4 if k < 5 else 2

                        def body(r, row, accs):
                            accs = list(accs)
                            for y in range(0, 8, size):
                                at = pl.ds(r * 8 + y, size)
                                v = [U[m, at] for m in range(k + 1)]
                                u = ew * v8(WS.get(row + 8 * y, 8 * size))
                                if k < LATE - 1:
                                    z = ew * v8(MW[pl.ds(pl.multiple_of(r * 64 + 8 * y, 8), 8 * size), :])
                                for m in range(k + 1):
                                    u = u - es[m] * v[m]
                                    if k < LATE - 1:
                                        z = z - es[m] * MU[m, at]
                                U[k + 1, at] = u
                                if k < LATE - 1:
                                    z = q * z
                                    Z[k + 1, at] = z
                                    ZS.put(row + 8 * y, 8 * size, z.reshape(8 * size, 128))
                                else:
                                    WS.put(row + 8 * y, 8 * size, u.reshape(8 * size, 128))
                                for m in range(k + 1):
                                    accs[m] = accs[m] + jnp.sum(u * v[m], axis=0)
                                accs[k + 1] = accs[k + 1] + jnp.sum(u * u, axis=0)
                            return tuple(accs)
                        accs = (all_planes if k < 5 else one_plane)(body, (zero8,) * (k + 2))
                        ACC[0:k + 2] = jnp.stack(accs)
                        halo_z(RU.at[b], z_recv.at[b]).wait_recv()
                        ghost_of_z(k + 1, es, ew, b, q, slice(56, 120))
                    else:
                        wn2 = bc(tot, 32) * sg * sg
                        drop = jnp.sum(cf * (2.0 * h - gram_times(cf)), axis=0)
                        sub = jnp.sqrt(jnp.maximum(wn2 - drop, 0.0))
                        est = givens(k - 1, nrm * MISC[3])
                        RES[c] = jnp.where(lane8 == k, est, RES[c])
                        est = givens(k, sub)
                        RES[c] = jnp.where(lane8 == k + 1, est, RES[c])
                        g = [GV[i] for i in range(RESTART)]
                        for i in reversed(range(RESTART)):
                            y = g[i] / RM[i, i]
                            YY[i] = y * SIG[i]
                            for m in range(i):
                                g[m] = g[m] - RM[m, i] * y

        yy = [YY[i] for i in range(RESTART)]

        def update(r, row, cy):
            x = v8(XS.get(row, 64))
            for m in range(RESTART):
                x = x + yy[m] * Z[m, pl.ds(r * 8, 8)]
            x = x.reshape(64, 128)
            XS.put(row, 64, x)
            MW[pl.ds(pl.multiple_of(r * 64, 8), 64), :] = x
            return cy
        all_planes(update, 0)

        @pl.when(c == 0)
        def _():
            inv = MISC[1]
            whole(SB, RB.at[RESTART - 1], h_send, h_recv.at[(RESTART - 1) % 3]).wait_recv()

            g = v8(GX[...])
            for m in range(RESTART):
                g = g + yy[m] * v8(GZ[m])
            GX[...] = g.reshape(GROWS, 128)
            for t in range(3):
                g = yy[0] * v8(RB[0, t])
                for m in range(1, RESTART):
                    g = g + yy[m] * v8(RB[m, t])
                GU[0, t] = (v8(GU[0, t]) - inv * g).reshape(GROWS, 128)

    cp = pltpu.make_async_copy(MW, out_hbm, l_sem.at[0])
    cp.start()
    sync_all((CYCLES * RESTART) % 2).wait_send()
    rows = jnp.where(lax.broadcasted_iota(jnp.int32, (8, 128), 0) == 0, RES[0], RES[1]) * out_scale
    res_ref[...] = rows
    cp.wait()


def unpack(x_ref, r_ref, out_ref, res_ref):
    lane = lax.broadcasted_iota(jnp.int32, (64, 128), 1)
    left = lane < 64
    z = jnp.where(left, lane, lane - 64)
    half = lax.shift_right_logical(z, 1)
    deal = half + 64 * (z - 2 * half) + jnp.where(left, 0, 32)
    for i in range(x_ref.shape[1]):
        e, o = x_ref[0, i], x_ref[1, i]
        for h, p in ((0, jnp.where(left, e, pltpu.roll(o, 64, 1))), (2, jnp.where(left, pltpu.roll(e, 64, 1), o))):
            a = jnp.take_along_axis(p, deal, axis=1)
            out_ref[h, i] = a[:, 0:64]
            out_ref[h + 1, i] = a[:, 64:128]
    res_ref[...] = r_ref[0:CYCLES, 0:RESTART + 1]


def solution(mesh):
    grid_spec = P(('sys', 'gx'), 'gy', 'gz')
    vel_spec = P(None, ('sys', 'gx'), 'gy', 'gz')
    table_spec = P('sys', None)
    f32 = jnp.float32

    def local_solve(source, initial, velocity, damping):
        big = (SETR, 128)
        vol, flat = (NP * 8, 8, 128), (NP * 64, 128)
        v = lambda *s: pltpu.VMEM(s, f32)
        n = RESTART
        scratch = [
            v(n, *vol), v(LATE - 1, *vol), v(LATE - 1, *vol), v(LATE - 1, *vol), v(n, *vol),
            v(*big), v(*big), v(5, *big), v(*flat),
            v(*flat), v(*flat), v(*flat), v(*flat), v(*flat), v(*flat), v(128, 128), v(NP, 128), v(NP, 128),
            v(n - 1, 3, GROWS, 128), v(n - 1, GROWS, 128), v(n + 3, 3, GROWS, 128), v(2, GROWS, 128),
            v(3, GROWS, 128), v(GROWS, 128), v(n, GROWS, 128), v(GROWS, 128), v(64, 128),
            v(2, 8, 128), v(n + 1, 8, 128), v(n, n, 8, 128), v(n, n, 8, 128),
            v(n, 8, 128), v(n + 1, 8, 128), v(n, 8, 128), v(n, 8, 128), v(n + 1, 8, 128), v(n, 8, 128), v(n, 8, 128),
            v(CYCLES, 8, 128), v(8, 8, 128), v(4, 48, 64, 64),
            pltpu.SemaphoreType.DMA((2,)), pltpu.SemaphoreType.DMA((2,)), pltpu.SemaphoreType.DMA,
            pltpu.SemaphoreType.DMA((3,)), pltpu.SemaphoreType.DMA, pltpu.SemaphoreType.DMA((2,)),
            pltpu.SemaphoreType.DMA, pltpu.SemaphoreType.DMA((2,)), pltpu.SemaphoreType.DMA, pltpu.SemaphoreType.DMA((4,)),
        ]
        hbm = pl.BlockSpec(memory_space=pl.ANY)
        packed, rows = pl.pallas_call(
            kernel,
            out_shape=(jax.ShapeDtypeStruct(flat, f32), jax.ShapeDtypeStruct((8, 128), f32)),
            in_specs=[hbm, hbm, hbm, pl.BlockSpec(memory_space=pltpu.SMEM)],
            out_specs=(hbm, pl.BlockSpec(memory_space=pltpu.VMEM)),
            scratch_shapes=scratch,
            compiler_params=pltpu.CompilerParams(
                collective_id=0, has_side_effects=True, vmem_limit_bytes=67043328),
            name='fgmres',
        )(source, initial, velocity, damping)
        step = 3
        out, res = pl.pallas_call(
            unpack,
            grid=(XL // step,),
            out_shape=(jax.ShapeDtypeStruct((4, XL, 64, 64), f32), jax.ShapeDtypeStruct((CYCLES, n + 1), f32)),
            in_specs=[pl.BlockSpec((2, step, 64, 128), lambda i: (0, i, 0, 0)), pl.BlockSpec((8, 128), lambda i: (0, 0))],
            out_specs=(pl.BlockSpec((4, step, 64, 64), lambda i: (0, i, 0, 0)),
                       pl.BlockSpec((CYCLES, n + 1), lambda i: (0, 0))),
            name='unpack',
        )(packed.reshape(2, XL, 64, 128), rows)
        return out.reshape(source.shape), res

    return jax.shard_map(local_solve, mesh=mesh, in_specs=(grid_spec, grid_spec, vel_spec, table_spec),
                         out_specs=(grid_spec, table_spec), check_vma=False)
```

```python
import math
import jax
import jax.numpy as jnp
from jax import lax
from jax.experimental import pallas as pl
from jax.experimental.pallas import tpu as pltpu
from jax.sharding import PartitionSpec as P

MESH = pl.DeviceIdType.MESH
RESTART = 10
CYCLES = 2
XL = 12
NP = 2 * XL
PZ = XL + 2
LO, HI, ROWS = 8, 72, 80
SETR = 2 * PZ * ROWS
LATE = 8
XG, YG, ZG = slice(0, 32), slice(32, 56), slice(56, 120)
GROWS = 120
UX = 2


def pairs(unroll, body, carry=()):
    if unroll == XL:
        for i in range(XL):
            carry = body(i, carry)
        return carry

    def trip(t, carry):
        for i in range(unroll):
            carry = body(t * unroll + i, carry)
        return carry
    return lax.fori_loop(0, XL // unroll, trip, carry)


def v8(x):
    return x.reshape(-1, 8, 128)


class Set:
    def __init__(self, ref, t=None):
        self.ref, self.t = ref, t

    def index(self, start, size):
        rows = pl.ds(start, size) if not isinstance(start, int) else slice(start, start + size)
        return (rows, slice(None)) if self.t is None else (self.t, rows, slice(None))

    def get(self, start, size):
        return self.ref[self.index(start, size)]

    def put(self, start, size, v):
        self.ref[self.index(start, size)] = v

    def view(self, start, size):
        return self.ref.at[self.index(start, size)]


def row0(p):
    r = p * ROWS + LO
    return r if isinstance(r, int) else pl.multiple_of(r, 8)


def all_planes(body, carry, step=1):
    def trip(t, carry):
        for zl in range(2):
            for i in range(step):
                x = t * step + i
                carry = body(x + zl * XL, row0(x + (zl * PZ + 1)), carry)
        return carry
    return lax.fori_loop(0, XL // step, trip, carry)


def kernel(src_hbm, ini_hbm, vel_hbm, damp_ref, out_hbm, res_ref,
           U, NU, N2U, MU, Z, ZC, X, VV, MW, SRC, CZP, CZM, HVX, HVY, CZA, CGX, CGY, YB,
           GU, GMU, RB, RU, SB, SU, GZ, GX, GX2, SS, ACC, GM, RM, SIG, EC, CS, SN, GV, YY, NRM, RES, MISC, STG, DEAL,
           s_send, s_recv, h_send, h_recv, u_send, u_recv, z_send, z_recv, x_recv, l_sem):
    f32 = jnp.float32
    gx, gy, gz = lax.axis_index('gx'), lax.axis_index('gy'), lax.axis_index('gz')
    peers = {}
    for p in range(1, 8):
        a, b, c = p // 4, (p // 2) % 2, p % 2
        peers[p] = {'gx': 1 - gx if a else gx, 'gy': 1 - gy if b else gy, 'gz': 1 - gz if c else gz}
    side = {0: 4, 1: 2, 2: 1}

    load_x = pltpu.make_async_copy(ini_hbm, STG.at[0], l_sem.at[0])
    load_x.start()
    load_v = [pltpu.make_async_copy(vel_hbm.at[d], STG.at[1 + d], l_sem.at[1 + d]) for d in range(3)]
    load_s = pltpu.make_async_copy(src_hbm, STG.at[0], l_sem.at[0])
    bar = pltpu.get_barrier_semaphore()
    for p in range(1, 8):
        pl.semaphore_signal(bar, inc=1, device_id=peers[p], device_id_type=MESH)

    lane = lax.broadcasted_iota(jnp.int32, (64, 128), 1)
    lane8 = lane[0:8]
    left = lane < 64
    zh = jnp.where(left, jnp.where(lane < 32, lane, lane - 32), jnp.where(lane < 96, lane - 64, lane - 96))
    zh32 = zh[0:32]
    first_q, last_q = lane < 32, lane >= 96
    zero64 = jnp.zeros((64, 128), f32)
    zero8 = jnp.zeros((8, 128), f32)
    hi_x = (1 - gx).astype(f32)
    l0 = 31 * (1 - gz)
    o_x = 96 * (1 - gx)
    y_send = 63 * (1 - gy)
    y_pad = HI - 65 * gy
    edge_lo = zh32 == 32 * (1 - gz)
    edge_hi = zh32 == 31 + 32 * gz
    WS, ZS, XS = Set(VV, 0), Set(ZC), Set(X)

    def seams(V, ghost=None):
        for zl in range(2):
            b = zl * PZ
            a = pltpu.roll(V.get(row0(b + XL), 64), 32, 1)
            d = pltpu.roll(V.get(row0(b + 1), 64), 96, 1)
            lo = 0.0 if ghost is None else ghost[zl] * (1.0 - hi_x)
            hi = 0.0 if ghost is None else ghost[zl] * hi_x
            V.put(row0(b), 64, jnp.where(first_q, lo, a))
            V.put(row0(b + XL + 1), 64, jnp.where(last_q, hi, d))

    def neighbours(V, i, put, ghost=None):
        size = 64 if ghost is None else 32
        for y in range(0, 64, size):
            co = lambda C, r: C[r * 64 + y:r * 64 + y + size, :]
            at = lambda q, d: V.get(row0(q) + y + d, size)
            u0, u1 = at(i + 1, 0), at(i + (PZ + 1), 0)
            below, above = pltpu.roll(u1, 1, 1), pltpu.roll(u0, 127, 1)
            if ghost is None:
                cm0, cp1 = co(CZM, i), co(CZP, i + XL)
            else:
                g = pltpu.roll(ghost[y:y + size, :], (l0 - i + 128) % 128, 1)
                below = jnp.where(edge_lo, g, below)
                above = jnp.where(edge_hi, g, above)
                cm0, cp1 = co(CZA, i), co(CZA, i + XL)
            for zl, u, n in ((0, u0, co(CZP, i) * u1 + cm0 * below), (1, u1, co(CZM, i + XL) * u0 + cp1 * above)):
                q, r = i + (zl * PZ + 1), i + zl * XL
                yp, ym = at(q, 1), at(q, -1)
                xp, xm = at(q + 1, 0), at(q - 1, 0)
                n = n + (xp + xm) - co(HVX, r) * (xp - xm)
                n = n + (yp + ym) - co(HVY, r) * (yp - ym)
                put(r * 8 + y // 8, row0(q) + y, size, u, n)

    def spread_x(rec):
        g = rec[XG, :]
        return [jnp.concatenate([pltpu.roll(g, (o_x - 64 * zl - 32 * yh + 128) % 128, 1) for yh in range(2)], axis=0)
                for zl in range(2)]

    def fill_ghosts(V, rec):
        seams(V, spread_x(rec))

        @pl.loop(0, 2)
        def _(zl):
            for i in range(XL):
                V.put((zl * PZ + (i + 1)) * ROWS + y_pad, 1, rec[pl.ds(zl * XL + (i + 32), 1), :])

    def add_ghosts_xy(rec):
        pd = (XL - 1) * (1 - gx)
        for zl, g in enumerate(spread_x(rec)):
            row = (pd + (zl * PZ + 1)) * ROWS + LO
            WS.put(row, 64, WS.get(row, 64) - CGX[64 * zl:64 * zl + 64, :] * g)
        YB[...] = CGY[...] * rec[YG, :]
        for r in range(NP):
            row = row0(r % XL + r // XL * PZ + 1) + y_send
            WS.put(row, 1, WS.get(row, 1) - YB[r:r + 1, :])

    def pack_xy(get, out):
        pd = (XL - 1) * (1 - gx)
        acc = zero64[0:32]
        for zl in range(2):
            for yh in range(2):
                slot = 2 * zl + yh
                r = pltpu.roll(get(zl, pd, 32 * yh, 32), (32 * slot - o_x + 128) % 128, 1)
                here = jnp.logical_and(lane[0:32] >= 32 * slot, lane[0:32] < 32 * slot + 32)
                acc = jnp.where(here, r, acc)
        out[XG, :] = acc

        for zl in range(2):
            for i in range(XL):
                r = 32 + zl * XL + i
                out[r:r + 1, :] = get(zl, i, y_send, 1)

    def pack_z(get, out):
        acc = zero64
        for i in range(XL):
            r = pltpu.roll(get(1 - gz, i, 0, 64), (i - l0 + 128) % 128, 1)
            acc = jnp.where(zh == i, r, acc)
        out[ZG, :] = acc

    def pack(get, out):
        pack_xy(get, out)
        pack_z(get, out)

    def of_set(V):
        return lambda zl, i, y, n: V.get((zl * PZ + i + 1) * ROWS + LO + y, n)

    def of_mw(zl, i, y, n):
        return MW[pl.ds((zl * XL + i) * 64 + y, n), :]

    def halo_start(src, dst, send, recv, axes=(0, 1, 2)):
        for ax in axes:
            rows = (XG, YG, ZG)[ax]
            pltpu.make_async_remote_copy(
                src_ref=src.at[rows, :], dst_ref=dst.at[rows, :], send_sem=send, recv_sem=recv,
                device_id=peers[side[ax]], device_id_type=MESH).start()

    def whole(src, dst, send, recv):
        return pltpu.make_async_remote_copy(src_ref=src, dst_ref=dst, send_sem=send, recv_sem=recv,
                                            device_id=peers[1], device_id_type=MESH)

    def three_at_once(b, dst, recv):
        for q, t in enumerate((0, 1 + b, 3 + b)):
            pack_xy(of_set(Set(VV, t)), SB.at[q])
        for q, t in enumerate((0, 1 + b, 3 + b)):
            pack_z(of_set(Set(VV, t)), SB.at[q])
        for q in range(3):
            halo_start(SB.at[q], dst.at[q], h_send, recv)

    def three(b, dst, recv):
        @pl.loop(0, 3)
        def _(q):
            pack(of_set(Set(VV, 2 * q + (b - 1) * ((q + 1) // 2))), SB.at[q])
            halo_start(SB.at[q], dst.at[q], h_send, recv)

    def sync_all(par):
        return pltpu.make_async_remote_copy(
            src_ref=SS.at[par, pl.ds(1, 7), :], dst_ref=SS.at[par, pl.ds(1, 7), :],
            send_sem=s_send.at[par], recv_sem=s_recv.at[par], device_id=peers[1], device_id_type=MESH)

    def sync_start(par, items):
        row = zero8
        for idx, acc in items:
            row = jnp.where(lane8 == idx, jnp.sum(acc, axis=1, keepdims=True), row)
        row = row + pltpu.roll(row, 4, 0)
        row = row + pltpu.roll(row, 2, 0)
        row = row + pltpu.roll(row, 1, 0)
        SS[par, 0:1, :] = row[0:1]
        for p in range(1, 8):
            pltpu.make_async_remote_copy(
                src_ref=SS.at[par, pl.ds(0, 1), :], dst_ref=SS.at[par, pl.ds(p, 1), :],
                send_sem=s_send.at[par], recv_sem=s_recv.at[par],
                device_id=peers[p], device_id_type=MESH).start()

    def sync_wait(par):
        sync_all(par).wait_recv()
        tot = SS[par]
        tot = tot + pltpu.roll(tot, 4, 0)
        tot = tot + pltpu.roll(tot, 2, 0)
        return tot + pltpu.roll(tot, 1, 0)

    def bc(tot, k):
        return jnp.broadcast_to(tot[:, k:k + 1], (8, 128))

    def fold(x):
        return jnp.sum(v8(x), axis=0)

    def poly(c, j):
        s = damp_ref[c, j] / 6.0
        a0, a1, a2 = 3.0 * s, 3.0 * s * s, s * s * s
        q = jnp.full((8, 128), a0 - 6.0 * a1 + 36.0 * a2, f32)
        return q, (a1 - 12.0 * a2) / q, a2 / q

    @pl.loop(0, 2 * PZ)
    def _(p):
        for V in (ZS, XS, WS, Set(VV, 1), Set(VV, 2)):
            V.put(pl.multiple_of(p * ROWS, 8), 8, zero8)
            V.put(pl.multiple_of(p * ROWS + HI, 8), 8, zero8)

    a = lax.broadcasted_iota(jnp.int32, (256, 256), 0)
    d = lax.broadcasted_iota(jnp.int32, (256, 256), 1)
    d0 = d - jnp.where(d >= 128, 128, 0)
    h = jnp.where(d0 >= 96, 3, jnp.where(d0 >= 64, 2, jnp.where(d0 >= 32, 1, 0)))
    target = 64 * h + 2 * (d0 - 32 * h) + jnp.where(d >= 128, 1, 0)
    DEAL[...] = jnp.where(a == target, 1.0, 0.0).astype(jnp.bfloat16)

    def convert(ref, i):
        v = jnp.concatenate([ref[h * XL + i] for h in range(4)], axis=1)
        a1 = v.astype(jnp.bfloat16)
        v = v - a1.astype(f32)
        a2 = v.astype(jnp.bfloat16)
        a3 = (v - a2.astype(f32)).astype(jnp.bfloat16)
        m = DEAL[...]
        out = [jnp.dot(p, m, preferred_element_type=f32) for p in (a1, a2, a3)]
        out = (out[2] + out[1]) + out[0]
        return out[:, 0:128], out[:, 128:256]

    load_x.wait()
    for cp in load_v:
        cp.start()

    def take_x(i, c):
        for zl, v in enumerate(convert(STG.at[0], i)):
            XS.put(row0(i + (zl * PZ + 1)), 64, v)
        return c
    pairs(UX, take_x)
    load_s.start()
    pack(of_set(XS), SU)
    pl.semaphore_wait(bar, 7)
    halo_start(SU, GX, u_send, x_recv)

    for d, store in ((0, HVX), (1, HVY)):
        load_v[d].wait()

        def take_h(i, c):
            for zl, v in enumerate(convert(STG.at[1 + d], i)):
                store[pl.ds(pl.multiple_of((i + zl * XL) * 64, 8), 64), :] = 0.5 * v
            return c
        pairs(UX, take_h)
    load_v[2].wait()

    def take_z(i, c):
        h0, h1 = convert(STG.at[3], i)
        cm0, cp1 = 1.0 + 0.5 * h0, 1.0 - 0.5 * h1
        low = pl.ds(pl.multiple_of(i * 64, 8), 64)
        high = pl.ds(pl.multiple_of((i + XL) * 64, 8), 64)
        CZP[low, :] = 1.0 - 0.5 * h0
        CZM[low, :] = jnp.where(zh == 0, 0.0, cm0)
        CZA[low, :] = jnp.where(zh == 32 * gz, 0.0, cm0)
        CZM[high, :] = 1.0 + 0.5 * h1
        CZP[high, :] = jnp.where(zh == 31, 0.0, cp1)
        CZA[high, :] = jnp.where(zh == 63 - 32 * gz, 0.0, cp1)
        return c
    pairs(UX, take_z)
    pd = (XL - 1) * (1 - gx)
    at_x = jnp.logical_and(lane >= o_x, lane < o_x + 32)
    sign_x, sign_y = (2 * gx - 1).astype(f32), (2 * gy - 1).astype(f32)
    for zl in range(2):
        hv = HVX[pl.ds(pl.multiple_of((zl * XL + pd) * 64, 8), 64), :]
        CGX[64 * zl:64 * zl + 64, :] = jnp.where(at_x, 1.0 + sign_x * hv, 0.0)

    @pl.loop(0, NP)
    def _(r):
        CGY[pl.ds(r, 1), :] = 1.0 + sign_y * HVY[pl.ds(r * 64 + y_send, 1), :]
    load_s.wait()

    def take_s(i, c):
        for zl, v in enumerate(convert(STG.at[0], i)):
            SRC[pl.ds(pl.multiple_of((i + zl * XL) * 64, 8), 64), :] = v
        return c
    pairs(UX, take_s)
    whole(SU, GX, u_send, x_recv).wait()

    def halo_xy(dst, recv):
        return whole(SU.at[pl.ds(0, 56), :], dst.at[pl.ds(0, 56), :], u_send, recv)

    def halo_z(dst, recv):
        return whole(SU.at[pl.ds(56, 64), :], dst.at[pl.ds(56, 64), :], z_send, recv)

    def ghost_of_z(k, e, ew, b, q, rows):
        g = ew * v8(RU[b, rows, :])
        for i in range(k):
            g = g - e[i] * v8(GMU[i, rows, :])
        GZ[k, rows, :] = (q * g).reshape(-1, 128)

    def sweep(V, unroll, put, ghost=None):
        def one(i, c):
            neighbours(V, i, put, ghost)
            return c
        pairs(unroll, one)

    def to_n(V):
        def put(r8, row, size, u, n):
            V.put(row, size, n)
        return put

    def givens(m, sub):
        h = [RM[i, m] for i in range(m + 1)]
        for i in range(m):
            cs, sn = CS[i], SN[i]
            h[i], h[i + 1] = cs * h[i] + sn * h[i + 1], cs * h[i + 1] - sn * h[i]
        d = h[m]
        rad = jnp.sqrt(d * d + sub * sub)
        cs, sn = d / rad, sub / rad
        CS[m] = cs
        SN[m] = sn
        h[m] = cs * d + sn * sub
        RM[0:m + 1, m] = jnp.stack(h)
        g = GV[m]
        GV[m] = cs * g
        GV[m + 1] = -sn * g
        est = MISC[4] * jnp.abs(sn)
        MISC[4] = est
        return est

    out_scale = 1.0 / math.sqrt(1572864.0)
    last_halo = CYCLES * RESTART - 3

    @pl.loop(0, CYCLES)
    def _(c):
        fill_ghosts(XS, GX)

        def put_r(r8, row, size, u, n):
            WS.put(row, size, SRC[r8 * 8:r8 * 8 + size, :] - (6.0 * u - n))
        sweep(XS, XL, put_r, GX.at[ZG, :])

        @pl.when(c == 0)
        def _():
            def one(r, row, acc):
                t = v8(WS.get(row, 64)).reshape(2, 4, 8, 128)
                return acc + jnp.sum(t * t, axis=0)
            acc = all_planes(one, jnp.zeros((4, 8, 128), f32), 2)
            sync_start(0, [(16, jnp.sum(acc, axis=0))])

        @pl.loop(0, RESTART)
        def _(j):
            step = c * RESTART + j
            par = (step + 1) % 2
            b = step % 2
            nxt = (j + 1) % RESTART
            slot = c * RESTART + (1 - c) * j + c * (j % 3)

            @pl.when(j * (j - LATE) >= 0)
            def _():
                seams(WS)
                sweep(WS, XL, to_n(Set(VV, 1)))
                seams(Set(VV, 1))

            @pl.when(j >= LATE)
            def _():
                q, r1, r2 = (jnp.concatenate([t] * 8, axis=0) for t in poly(c, j))

                def put_z(r8, row, size, u, n):
                    z = q * (WS.get(row, size) + r1 * u + r2 * n)
                    ZS.put(row, size, z)
                    Z[j, r8:r8 + size // 8] = v8(z)
                sweep(Set(VV, 1), XL, put_z)

            @pl.when(j == 0)
            def _():
                sweep(Set(VV, 1), XL, to_n(Set(VV, 3)))

                @pl.when(c == 0)
                def _():
                    three(0, GU.at[0], h_recv.at[1])
                    tot = sync_wait(0)
                    sync_all(0).wait_send()
                    beta0 = jnp.sqrt(bc(tot, 16))
                    MISC[0] = beta0
                    MISC[1] = 1.0 / beta0

                inv0 = MISC[1]
                q, r1, r2 = poly(c, 0)

                def start(r, row, acc):
                    u, n, n2 = (v8(Set(VV, t).get(row, 64)) * inv0 for t in (0, 1, 3))
                    z = q * (u + r1 * n + r2 * n2)
                    acc = acc + jnp.sum((u * u).reshape(2, 4, 8, 128), axis=0)
                    at = pl.ds(r * 8, 8)
                    U[0, at] = u
                    NU[0, at] = n
                    N2U[0, at] = n2
                    Z[0, at] = z
                    ZS.put(row, 64, z.reshape(64, 128))
                    return acc
                ACC[0] = jnp.sum(all_planes(start, jnp.zeros((4, 8, 128), f32)), axis=0)

                @pl.when(c == 0)
                def _():
                    whole(SB, GU.at[0], h_send, h_recv.at[1]).wait()

                    for t in range(3):
                        GU[0, t] = (v8(GU[0, t]) * inv0).reshape(GROWS, 128)

                GZ[0] = (q * (v8(GU[0, 0]) + r1 * v8(GU[0, 1]) + r2 * v8(GU[0, 2]))).reshape(GROWS, 128)

            seams(ZS)
            GX2[...] = GZ[j, ZG, :]

            def put_w(r8, row, size, u, n):
                WS.put(row, size, 6.0 * u - n)
            sweep(ZS, XL, put_w, GX2)

            for k in range(1, RESTART):
                @pl.when(j == k)
                def _():
                    halo_xy(RU.at[1 - b], u_recv.at[1 - b]).wait_recv()
                    ghost_of_z(k, [EC[i] for i in range(k)], EC[k], 1 - b, poly(c, k)[0], slice(0, 56))
            add_ghosts_xy(GZ.at[j])

            for k in range(RESTART):
                @pl.when(j == k)
                def _():
                    ends = k == 0 or k == RESTART - 1
                    wd = 4 if k < 4 else 2 if k < 8 else 1
                    count = k + 2 if ends else k + 1

                    def dots(t, accs):
                        accs = list(accs)
                        for zl in range(2):
                            x = t * 2 + zl * XL
                            w = jnp.concatenate([v8(WS.get(row0(t * 2 + (zl * PZ + 1 + i)), 64)) for i in range(2)])
                            w = w.reshape(16 // wd, wd, 8, 128)
                            for i in range(k + 1):
                                v = U[i, pl.ds(x * 8, 16)].reshape(16 // wd, wd, 8, 128)
                                accs[i] = accs[i] + jnp.sum(v * w, axis=0)
                            if ends:
                                accs[k + 1] = accs[k + 1] + jnp.sum(w * w, axis=0)
                        return tuple(accs)
                    accs = lax.fori_loop(0, XL // 2, dots, (jnp.zeros((wd, 8, 128), f32),) * count)
                    accs = [jnp.sum(a, axis=0) for a in accs]
                    items = [(i, accs[i]) for i in range(k + 1)] + [(16 + i, ACC[i]) for i in range(k + 1)]
                    if ends:
                        items.append((32, accs[k + 1]))
                    sync_start(par, items)

            @pl.when(step > 0)
            def _():
                sync_all(1 - par).wait_send()

            @pl.when(step < CYCLES * RESTART - 1)
            def _():
                seams(WS)
                sweep(WS, XL, to_n(Set(VV, 1 + b)))

            @pl.when(CYCLES * RESTART - 1 - step > 0)
            def _():
                seams(Set(VV, 1 + b))
                r1, r2 = (jnp.concatenate([t] * 8, axis=0) for t in poly(c, nxt)[1:])

                def put(r8, row, size, u, n):
                    Set(VV, 3 + b).put(row, size, n)
                    MW[r8 * 8:r8 * 8 + size, :] = WS.get(row, size) + r1 * u + r2 * n
                sweep(Set(VV, 1 + b), XL, put)

            @pl.when(j > 0)
            def _():
                halo_xy(RU.at[b], u_recv.at[b]).wait_send()
                halo_z(RU.at[b], z_recv.at[b]).wait_send()

            @pl.when(j < RESTART - 1)
            def _():
                pack_xy(of_mw, SU)
                halo_start(SU, RU.at[b], u_send, u_recv.at[b], (0, 1))
                pack_z(of_mw, SU)
                halo_start(SU, RU.at[b], z_send, z_recv.at[b], (2,))

            @pl.when(step <= last_halo + 1)
            def _():
                @pl.when(step > 0)
                def _():
                    whole(SB, RB.at[slot], h_send, h_recv.at[0]).wait_send()

                @pl.when(step <= last_halo)
                def _():
                    three_at_once(b, RB.at[slot], h_recv.at[step % 3])

                @pl.when(j > 0)
                def _():
                    whole(SB, RB.at[slot], h_send, h_recv.at[(step + 2) % 3]).wait_recv()

            prev = c * RESTART + (1 - c) * (j - 1) + c * ((j + 2) % 3)
            for k in range(RESTART):
                @pl.when(j == k)
                def _():
                    if k < RESTART - 1:
                        q, r1, r2 = poly(c, k + 1)
                        e = [EC[i] for i in range(k + 1)] if k else None

                        size = 8 if k < 4 else 4

                        def body(r, row, cy):
                            for y in range(0, 8, size):
                                at = pl.ds(r * 8 + y, size)
                                if k:
                                    n = e[k] * v8(Set(VV, 2 - b).get(row + 8 * y, 8 * size))
                                    n2 = e[k] * v8(Set(VV, 4 - b).get(row + 8 * y, 8 * size))
                                    for m in range(k):
                                        nm, n2m = NU[m, at], N2U[m, at]
                                        n = n - e[m] * nm
                                        n2 = n2 - e[m] * n2m
                                        MU[m, at] = U[m, at] + r1 * nm + r2 * n2m
                                    NU[k, at] = n
                                    N2U[k, at] = n2
                                else:
                                    n, n2 = NU[0, at], N2U[0, at]
                                MU[k, at] = U[k, at] + r1 * n + r2 * n2
                            return cy
                        if k < LATE - 1:
                            all_planes(body, 0)

                        if k:
                            for t in range(3):
                                g = e[k] * v8(RB[prev, t])
                                for i in range(k):
                                    g = g - e[i] * v8(GU[i, t])
                                GU[k, t] = g.reshape(GROWS, 128)

                        @pl.loop(0, k + 1)
                        def _(i):
                            g = v8(GU[i, 0]) + r1 * v8(GU[i, 1]) + r2 * v8(GU[i, 2])
                            GMU[i] = g.reshape(GROWS, 128)
                    if k >= 2:
                        est = givens(k - 2, NRM[k - 1] * MISC[3])
                        RES[c] = jnp.where(lane8 == k - 1, est, RES[c])

            tot = sync_wait(par)

            for k in range(RESTART):
                @pl.when(j == k)
                def _():
                    nn = bc(tot, 16 + k)
                    nrm = jnp.sqrt(nn)
                    sg = 1.0 / nrm
                    SIG[k] = sg
                    NRM[k] = nrm
                    sig = SIG[0:k + 1] * sg
                    h = jnp.stack([bc(tot, i) for i in range(k + 1)]) * sig
                    gcol = jnp.stack([bc(tot, 16 + i) for i in range(k + 1)]) * sig
                    GM[k, 0:k + 1] = gcol
                    if k > 0:
                        GM[0:k, k] = gcol[0:k]

                    def gram_times(x):
                        out = gcol * x[k]
                        for m in range(k):
                            out = out + GM[m, 0:k + 1] * x[m]
                        return out
                    cf = 2.0 * h - gram_times(h)
                    RM[0:k + 1, k] = cf
                    if k == 0:
                        beta = MISC[0] * nrm
                        MISC[4] = beta
                        GV[0] = beta
                        RES[c] = jnp.where(lane8 == 0, beta, 0.0)
                        wn = jnp.sqrt(bc(tot, 32)) * sg
                        MISC[3] = wn
                        rho = 1.0 / wn
                        MISC[2] = rho
                    else:
                        rho = MISC[2]
                    if k < RESTART - 1:
                        es = rho * cf * SIG[0:k + 1]
                        ew = rho * sg
                        EC[0:k + 1] = es
                        EC[k + 1] = ew
                        q = poly(c, k + 1)[0]

                        size = 8 if k < 2 else 4 if k < 5 else 2

                        def body(r, row, accs):
                            accs = list(accs)
                            for y in range(0, 8, size):
                                at = pl.ds(r * 8 + y, size)
                                v = [U[m, at] for m in range(k + 1)]
                                u = ew * v8(WS.get(row + 8 * y, 8 * size))
                                if k < LATE - 1:
                                    z = ew * v8(MW[pl.ds(pl.multiple_of(r * 64 + 8 * y, 8), 8 * size), :])
                                for m in range(k + 1):
                                    u = u - es[m] * v[m]
                                    if k < LATE - 1:
                                        z = z - es[m] * MU[m, at]
                                U[k + 1, at] = u
                                if k < LATE - 1:
                                    z = q * z
                                    Z[k + 1, at] = z
                                    ZS.put(row + 8 * y, 8 * size, z.reshape(8 * size, 128))
                                else:
                                    WS.put(row + 8 * y, 8 * size, u.reshape(8 * size, 128))
                                for m in range(k + 1):
                                    accs[m] = accs[m] + jnp.sum(u * v[m], axis=0)
                                accs[k + 1] = accs[k + 1] + jnp.sum(u * u, axis=0)
                            return tuple(accs)
                        accs = all_planes(body, (zero8,) * (k + 2))
                        ACC[0:k + 2] = jnp.stack(accs)
                        halo_z(RU.at[b], z_recv.at[b]).wait_recv()
                        ghost_of_z(k + 1, es, ew, b, q, slice(56, 120))
                    else:
                        wn2 = bc(tot, 32) * sg * sg
                        drop = jnp.sum(cf * (2.0 * h - gram_times(cf)), axis=0)
                        sub = jnp.sqrt(jnp.maximum(wn2 - drop, 0.0))
                        est = givens(k - 1, nrm * MISC[3])
                        RES[c] = jnp.where(lane8 == k, est, RES[c])
                        est = givens(k, sub)
                        RES[c] = jnp.where(lane8 == k + 1, est, RES[c])
                        g = [GV[i] for i in range(RESTART)]
                        for i in reversed(range(RESTART)):
                            y = g[i] / RM[i, i]
                            YY[i] = y * SIG[i]
                            for m in range(i):
                                g[m] = g[m] - RM[m, i] * y

        yy = [YY[i] for i in range(RESTART)]

        def update(r, row, cy):
            x = v8(XS.get(row, 64))
            for m in range(RESTART):
                x = x + yy[m] * Z[m, pl.ds(r * 8, 8)]
            x = x.reshape(64, 128)
            XS.put(row, 64, x)
            MW[pl.ds(pl.multiple_of(r * 64, 8), 64), :] = x
            return cy
        all_planes(update, 0)

        @pl.when(c == 0)
        def _():
            inv = MISC[1]
            whole(SB, RB.at[RESTART - 1], h_send, h_recv.at[(RESTART - 1) % 3]).wait_recv()

            g = v8(GX[...])
            for m in range(RESTART):
                g = g + yy[m] * v8(GZ[m])
            GX[...] = g.reshape(GROWS, 128)
            for t in range(3):
                g = yy[0] * v8(RB[0, t])
                for m in range(1, RESTART):
                    g = g + yy[m] * v8(RB[m, t])
                GU[0, t] = (v8(GU[0, t]) - inv * g).reshape(GROWS, 128)

    cp = pltpu.make_async_copy(MW, out_hbm, l_sem.at[0])
    cp.start()
    sync_all((CYCLES * RESTART) % 2).wait_send()
    rows = jnp.where(lax.broadcasted_iota(jnp.int32, (8, 128), 0) == 0, RES[0], RES[1]) * out_scale
    res_ref[...] = rows
    cp.wait()


def unpack(x_hbm, r_hbm, out_hbm, res_ref, xin, rin, out, in_sem, out_sem):
    f32 = jnp.float32
    parts = 3
    n = XL // parts
    loads = [[pltpu.make_async_copy(x_hbm.at[zl, pl.ds(t * n, n)], xin.at[zl, pl.ds(t * n, n)], in_sem.at[t, zl])
              for zl in range(2)] for t in range(parts)]
    stores = [[pltpu.make_async_copy(out.at[h, pl.ds(t * n, n)], out_hbm.at[h, pl.ds(t * n, n)], out_sem.at[t, h])
               for h in range(4)] for t in range(parts)]
    rows = pltpu.make_async_copy(r_hbm, rin, in_sem.at[parts, 0])
    for cp in [c for t in loads for c in t] + [rows]:
        cp.start()
    a = lax.broadcasted_iota(jnp.int32, (256, 256), 0)
    d = lax.broadcasted_iota(jnp.int32, (256, 256), 1)
    a0 = a - jnp.where(a >= 128, 128, 0)
    h = jnp.where(a0 >= 96, 3, jnp.where(a0 >= 64, 2, jnp.where(a0 >= 32, 1, 0)))
    m = jnp.where(d == 64 * h + 2 * (a0 - 32 * h) + jnp.where(a >= 128, 1, 0), 1.0, 0.0).astype(jnp.bfloat16)
    for t in range(parts):
        for cp in loads[t]:
            cp.wait()
        for i in range(t * n, t * n + n):
            v = jnp.concatenate([xin[0, i], xin[1, i]], axis=1)
            a1 = v.astype(jnp.bfloat16)
            v = v - a1.astype(f32)
            a2 = v.astype(jnp.bfloat16)
            a3 = (v - a2.astype(f32)).astype(jnp.bfloat16)
            o = [jnp.dot(p, m, preferred_element_type=f32) for p in (a1, a2, a3)]
            o = (o[2] + o[1]) + o[0]
            for h in range(4):
                out[h, i] = o[:, 64 * h:64 * h + 64]
        for cp in stores[t]:
            cp.start()
    rows.wait()
    res_ref[...] = rin[0:CYCLES, 0:RESTART + 1]
    for cp in [c for t in stores for c in t]:
        cp.wait()


def solution(mesh):
    grid_spec = P(('sys', 'gx'), 'gy', 'gz')
    vel_spec = P(None, ('sys', 'gx'), 'gy', 'gz')
    table_spec = P('sys', None)
    f32 = jnp.float32

    def local_solve(source, initial, velocity, damping):
        big = (SETR, 128)
        vol, flat = (NP * 8, 8, 128), (NP * 64, 128)
        v = lambda *s: pltpu.VMEM(s, f32)
        n = RESTART
        scratch = [
            v(n, *vol), v(LATE - 1, *vol), v(LATE - 1, *vol), v(LATE - 1, *vol), v(n, *vol),
            v(*big), v(*big), v(5, *big), v(*flat),
            v(*flat), v(*flat), v(*flat), v(*flat), v(*flat), v(*flat), v(128, 128), v(NP, 128), v(NP, 128),
            v(n - 1, 3, GROWS, 128), v(n - 1, GROWS, 128), v(n + 3, 3, GROWS, 128), v(2, GROWS, 128),
            v(3, GROWS, 128), v(GROWS, 128), v(n, GROWS, 128), v(GROWS, 128), v(64, 128),
            v(2, 8, 128), v(n + 1, 8, 128), v(n, n, 8, 128), v(n, n, 8, 128),
            v(n, 8, 128), v(n + 1, 8, 128), v(n, 8, 128), v(n, 8, 128), v(n + 1, 8, 128), v(n, 8, 128), v(n, 8, 128),
            v(CYCLES, 8, 128), v(8, 8, 128), v(4, 48, 64, 64), pltpu.VMEM((256, 256), jnp.bfloat16),
            pltpu.SemaphoreType.DMA((2,)), pltpu.SemaphoreType.DMA((2,)), pltpu.SemaphoreType.DMA,
            pltpu.SemaphoreType.DMA((3,)), pltpu.SemaphoreType.DMA, pltpu.SemaphoreType.DMA((2,)),
            pltpu.SemaphoreType.DMA, pltpu.SemaphoreType.DMA((2,)), pltpu.SemaphoreType.DMA, pltpu.SemaphoreType.DMA((4,)),
        ]
        hbm = pl.BlockSpec(memory_space=pl.ANY)
        packed, rows = pl.pallas_call(
            kernel,
            out_shape=(jax.ShapeDtypeStruct(flat, f32), jax.ShapeDtypeStruct((8, 128), f32)),
            in_specs=[hbm, hbm, hbm, pl.BlockSpec(memory_space=pltpu.SMEM)],
            out_specs=(hbm, pl.BlockSpec(memory_space=pltpu.VMEM)),
            scratch_shapes=scratch,
            compiler_params=pltpu.CompilerParams(
                collective_id=0, has_side_effects=True, vmem_limit_bytes=67043328),
            name='fgmres',
        )(source, initial, velocity, damping)
        out, res = pl.pallas_call(
            unpack,
            out_shape=(jax.ShapeDtypeStruct((4, XL, 64, 64), f32), jax.ShapeDtypeStruct((CYCLES, n + 1), f32)),
            in_specs=[hbm, hbm],
            out_specs=(hbm, pl.BlockSpec(memory_space=pltpu.VMEM)),
            scratch_shapes=[v(2, XL, 64, 128), v(8, 128), v(4, XL, 64, 64),
                            pltpu.SemaphoreType.DMA((4, 2)), pltpu.SemaphoreType.DMA((3, 4))],
            name='unpack',
        )(packed.reshape(2, XL, 64, 128), rows)
        return out.reshape(source.shape), res

    return jax.shard_map(local_solve, mesh=mesh, in_specs=(grid_spec, grid_spec, vel_spec, table_spec),
                         out_specs=(grid_spec, table_spec), check_vma=False)
```

```python
import math
import jax
import jax.numpy as jnp
from jax import lax
from jax.experimental import pallas as pl
from jax.experimental.pallas import tpu as pltpu
from jax.sharding import PartitionSpec as P

MESH = pl.DeviceIdType.MESH
RESTART = 10
CYCLES = 2
XL = 12
NP = 2 * XL
PZ = XL + 2
LO, HI, ROWS = 8, 72, 80
SETR = 2 * PZ * ROWS
LATE = 8
XG, YG, ZG = slice(0, 32), slice(32, 56), slice(56, 120)
GROWS = 120
UX = 2


def pairs(unroll, body, carry=()):
    if unroll == XL:
        for i in range(XL):
            carry = body(i, carry)
        return carry

    def trip(t, carry):
        for i in range(unroll):
            carry = body(t * unroll + i, carry)
        return carry
    return lax.fori_loop(0, XL // unroll, trip, carry)


def v8(x):
    return x.reshape(-1, 8, 128)


class Set:
    def __init__(self, ref, t=None):
        self.ref, self.t = ref, t

    def index(self, start, size):
        rows = pl.ds(start, size) if not isinstance(start, int) else slice(start, start + size)
        return (rows, slice(None)) if self.t is None else (self.t, rows, slice(None))

    def get(self, start, size):
        return self.ref[self.index(start, size)]

    def put(self, start, size, v):
        self.ref[self.index(start, size)] = v

    def view(self, start, size):
        return self.ref.at[self.index(start, size)]


def row0(p):
    r = p * ROWS + LO
    return r if isinstance(r, int) else pl.multiple_of(r, 8)


def all_planes(body, carry, step=1):
    def trip(t, carry):
        for zl in range(2):
            for i in range(step):
                x = t * step + i
                carry = body(x + zl * XL, row0(x + (zl * PZ + 1)), carry)
        return carry
    return lax.fori_loop(0, XL // step, trip, carry)


def kernel(src_hbm, ini_hbm, vel_hbm, damp_ref, out_hbm, res_ref,
           U, NU, N2U, MU, Z, ZC, X, W, T1, T2, MW, SRC, CZP, CZM, HVX, HVY, CZA, CGX, CGY, YB,
           GU, GMU, RB, RU, SB, SU, GZ, GX, GX2, SS, ACC, GM, RM, SIG, EC, CS, SN, GV, YY, NRM, RES, MISC, STG, DEAL,
           s_send, s_recv, h_send, h_recv, u_send, u_recv, z_send, z_recv, x_recv, l_sem):
    f32 = jnp.float32
    gx, gy, gz = lax.axis_index('gx'), lax.axis_index('gy'), lax.axis_index('gz')
    peers = {}
    for p in range(1, 8):
        a, b, c = p // 4, (p // 2) % 2, p % 2
        peers[p] = {'gx': 1 - gx if a else gx, 'gy': 1 - gy if b else gy, 'gz': 1 - gz if c else gz}
    side = {0: 4, 1: 2, 2: 1}

    def load(q, slot, h, src):
        return pltpu.make_async_copy(src.at[pl.ds(XL * h, XL)], STG.at[slot, pl.ds(XL * h, XL)], l_sem.at[q, h])

    def load_start(q, slot, src):
        for h in range(4):
            load(q, slot, h, src).start()
    load_start(0, 0, ini_hbm)
    bar = pltpu.get_barrier_semaphore()
    for p in range(1, 8):
        pl.semaphore_signal(bar, inc=1, device_id=peers[p], device_id_type=MESH)

    lane = lax.broadcasted_iota(jnp.int32, (64, 128), 1)
    lane8 = lane[0:8]
    left = lane < 64
    zh = jnp.where(left, jnp.where(lane < 32, lane, lane - 32), jnp.where(lane < 96, lane - 64, lane - 96))
    zh32 = zh[0:32]
    first_q, last_q = lane < 32, lane >= 96
    zero64 = jnp.zeros((64, 128), f32)
    zero8 = jnp.zeros((8, 128), f32)
    hi_x = (1 - gx).astype(f32)
    l0 = 31 * (1 - gz)
    o_x = 96 * (1 - gx)
    y_send = 63 * (1 - gy)
    y_pad = HI - 65 * gy
    edge_lo = zh32 == 32 * (1 - gz)
    edge_hi = zh32 == 31 + 32 * gz
    WS, ZS, XS = Set(W), Set(ZC), Set(X)

    def seams(V, ghost=None):
        for zl in range(2):
            b = zl * PZ
            a = pltpu.roll(V.get(row0(b + XL), 64), 32, 1)
            d = pltpu.roll(V.get(row0(b + 1), 64), 96, 1)
            lo = 0.0 if ghost is None else ghost[zl] * (1.0 - hi_x)
            hi = 0.0 if ghost is None else ghost[zl] * hi_x
            V.put(row0(b), 64, jnp.where(first_q, lo, a))
            V.put(row0(b + XL + 1), 64, jnp.where(last_q, hi, d))

    def neighbours(V, i, put, ghost=None):
        size = 64 if ghost is None else 32
        for y in range(0, 64, size):
            co = lambda C, r: C[r * 64 + y:r * 64 + y + size, :]
            at = lambda q, d: V.get(row0(q) + y + d, size)
            u0, u1 = at(i + 1, 0), at(i + (PZ + 1), 0)
            below, above = pltpu.roll(u1, 1, 1), pltpu.roll(u0, 127, 1)
            if ghost is None:
                cm0, cp1 = co(CZM, i), co(CZP, i + XL)
            else:
                g = pltpu.roll(ghost[y:y + size, :], (l0 - i + 128) % 128, 1)
                below = jnp.where(edge_lo, g, below)
                above = jnp.where(edge_hi, g, above)
                cm0, cp1 = co(CZA, i), co(CZA, i + XL)
            for zl, u, n in ((0, u0, co(CZP, i) * u1 + cm0 * below), (1, u1, co(CZM, i + XL) * u0 + cp1 * above)):
                q, r = i + (zl * PZ + 1), i + zl * XL
                yp, ym = at(q, 1), at(q, -1)
                xp, xm = at(q + 1, 0), at(q - 1, 0)
                n = n + (xp + xm) - co(HVX, r) * (xp - xm)
                n = n + (yp + ym) - co(HVY, r) * (yp - ym)
                put(r * 8 + y // 8, row0(q) + y, size, u, n)

    def spread_x(rec):
        g = rec[XG, :]
        return [jnp.concatenate([pltpu.roll(g, (o_x - 64 * zl - 32 * yh + 128) % 128, 1) for yh in range(2)], axis=0)
                for zl in range(2)]

    def fill_ghosts(V, rec):
        seams(V, spread_x(rec))

        @pl.loop(0, 2)
        def _(zl):
            for i in range(XL):
                V.put((zl * PZ + (i + 1)) * ROWS + y_pad, 1, rec[pl.ds(zl * XL + (i + 32), 1), :])

    def add_ghosts_xy(rec):
        pd = (XL - 1) * (1 - gx)
        for zl, g in enumerate(spread_x(rec)):
            row = (pd + (zl * PZ + 1)) * ROWS + LO
            WS.put(row, 64, WS.get(row, 64) - CGX[64 * zl:64 * zl + 64, :] * g)
        YB[...] = CGY[...] * rec[YG, :]
        for r in range(NP):
            row = row0(r % XL + r // XL * PZ + 1) + y_send
            WS.put(row, 1, WS.get(row, 1) - YB[r:r + 1, :])

    def pack_xy(get, out):
        pd = (XL - 1) * (1 - gx)
        acc = zero64[0:32]
        for zl in range(2):
            for yh in range(2):
                slot = 2 * zl + yh
                r = pltpu.roll(get(zl, pd, 32 * yh, 32), (32 * slot - o_x + 128) % 128, 1)
                here = jnp.logical_and(lane[0:32] >= 32 * slot, lane[0:32] < 32 * slot + 32)
                acc = jnp.where(here, r, acc)
        out[XG, :] = acc

        for zl in range(2):
            for i in range(XL):
                r = 32 + zl * XL + i
                out[r:r + 1, :] = get(zl, i, y_send, 1)

    def pack_z(get, out):
        acc = zero64
        for i in range(XL):
            r = pltpu.roll(get(1 - gz, i, 0, 64), (i - l0 + 128) % 128, 1)
            acc = jnp.where(zh == i, r, acc)
        out[ZG, :] = acc

    def pack(get, out):
        pack_xy(get, out)
        pack_z(get, out)

    def of_set(V):
        return lambda zl, i, y, n: V.get((zl * PZ + i + 1) * ROWS + LO + y, n)

    def of_mw(zl, i, y, n):
        return MW[pl.ds((zl * XL + i) * 64 + y, n), :]

    def halo_start(src, dst, send, recv, axes=(0, 1, 2)):
        for ax in axes:
            rows = (XG, YG, ZG)[ax]
            pltpu.make_async_remote_copy(
                src_ref=src.at[rows, :], dst_ref=dst.at[rows, :], send_sem=send, recv_sem=recv,
                device_id=peers[side[ax]], device_id_type=MESH).start()

    def whole(src, dst, send, recv):
        return pltpu.make_async_remote_copy(src_ref=src, dst_ref=dst, send_sem=send, recv_sem=recv,
                                            device_id=peers[1], device_id_type=MESH)

    def three_at_once(b, dst, recv):
        sets = (WS, Set(T1, b), Set(T2, b))
        for q, t in enumerate(sets):
            pack_xy(of_set(t), SB.at[q])
        for q, t in enumerate(sets):
            pack_z(of_set(t), SB.at[q])
        for q in range(3):
            halo_start(SB.at[q], dst.at[q], h_send, recv)

    def sync_all(par):
        return pltpu.make_async_remote_copy(
            src_ref=SS.at[par, pl.ds(1, 7), :], dst_ref=SS.at[par, pl.ds(1, 7), :],
            send_sem=s_send.at[par], recv_sem=s_recv.at[par], device_id=peers[1], device_id_type=MESH)

    def sync_start(par, items):
        row = zero8
        for idx, acc in items:
            row = jnp.where(lane8 == idx, jnp.sum(acc, axis=1, keepdims=True), row)
        row = row + pltpu.roll(row, 4, 0)
        row = row + pltpu.roll(row, 2, 0)
        row = row + pltpu.roll(row, 1, 0)
        SS[par, 0:1, :] = row[0:1]
        for p in range(1, 8):
            pltpu.make_async_remote_copy(
                src_ref=SS.at[par, pl.ds(0, 1), :], dst_ref=SS.at[par, pl.ds(p, 1), :],
                send_sem=s_send.at[par], recv_sem=s_recv.at[par],
                device_id=peers[p], device_id_type=MESH).start()

    def sync_wait(par):
        sync_all(par).wait_recv()
        tot = SS[par]
        tot = tot + pltpu.roll(tot, 4, 0)
        tot = tot + pltpu.roll(tot, 2, 0)
        return tot + pltpu.roll(tot, 1, 0)

    def bc(tot, k):
        return jnp.broadcast_to(tot[:, k:k + 1], (8, 128))

    def fold(x):
        return jnp.sum(v8(x), axis=0)

    def poly(c, j):
        s = damp_ref[c, j] / 6.0
        a0, a1, a2 = 3.0 * s, 3.0 * s * s, s * s * s
        q = jnp.full((8, 128), a0 - 6.0 * a1 + 36.0 * a2, f32)
        return q, (a1 - 12.0 * a2) / q, a2 / q

    @pl.loop(0, 2 * PZ)
    def _(p):
        for V in (ZS, XS, WS, Set(T1, 0), Set(T1, 1)):
            V.put(pl.multiple_of(p * ROWS, 8), 8, zero8)
            V.put(pl.multiple_of(p * ROWS + HI, 8), 8, zero8)

    a = lax.broadcasted_iota(jnp.int32, (256, 256), 0)
    d = lax.broadcasted_iota(jnp.int32, (256, 256), 1)
    d0 = d - jnp.where(d >= 128, 128, 0)
    h = jnp.where(d0 >= 96, 3, jnp.where(d0 >= 64, 2, jnp.where(d0 >= 32, 1, 0)))
    target = 64 * h + 2 * (d0 - 32 * h) + jnp.where(d >= 128, 1, 0)
    DEAL[...] = jnp.where(a == target, 1.0, 0.0).astype(jnp.bfloat16)

    def convert(ref, i):
        v = jnp.concatenate([ref[h * XL + i] for h in range(4)], axis=1)
        a1 = v.astype(jnp.bfloat16)
        v = v - a1.astype(f32)
        a2 = v.astype(jnp.bfloat16)
        a3 = (v - a2.astype(f32)).astype(jnp.bfloat16)
        m = DEAL[...]
        out = [jnp.dot(p, m, preferred_element_type=f32) for p in (a1, a2, a3)]
        out = (out[2] + out[1]) + out[0]
        return out[:, 0:128], out[:, 128:256]

    @pl.loop(0, 5)
    def _(q):
        for h in range(4):
            load(q, q % 4, h, ini_hbm).wait()

        @pl.when(q == 0)
        def _():
            for d in range(3):
                load_start(1 + d, 1 + d, vel_hbm.at[d])
        for i in range(XL):
            for zl, v in enumerate(convert(STG.at[q % 4], i)):
                U[q, (i + zl * XL) * 8:(i + zl * XL) * 8 + 8] = v8(v)

        @pl.when(q == 0)
        def _():
            load_start(4, 0, src_hbm)

            def take_x(r, row, c):
                XS.put(row, 64, U[0, pl.ds(r * 8, 8)].reshape(64, 128))
                return c
            all_planes(take_x, 0)
            pack(of_set(XS), SU)
            pl.semaphore_wait(bar, 7)
            halo_start(SU, GX, u_send, x_recv)

    @pl.loop(0, XL)
    def _(i):
        at = lambda q, r: U[q, pl.ds(r * 8, 8)].reshape(64, 128)
        low = pl.ds(pl.multiple_of(i * 64, 8), 64)
        high = pl.ds(pl.multiple_of((i + XL) * 64, 8), 64)
        for rows, r in ((low, i), (high, i + XL)):
            HVX[rows, :] = 0.5 * at(1, r)
            HVY[rows, :] = 0.5 * at(2, r)
            SRC[rows, :] = at(4, r)
        h0, h1 = at(3, i), at(3, i + XL)
        cm0, cp1 = 1.0 + 0.5 * h0, 1.0 - 0.5 * h1
        CZP[low, :] = 1.0 - 0.5 * h0
        CZM[low, :] = jnp.where(zh == 0, 0.0, cm0)
        CZA[low, :] = jnp.where(zh == 32 * gz, 0.0, cm0)
        CZM[high, :] = 1.0 + 0.5 * h1
        CZP[high, :] = jnp.where(zh == 31, 0.0, cp1)
        CZA[high, :] = jnp.where(zh == 63 - 32 * gz, 0.0, cp1)

    pd = (XL - 1) * (1 - gx)
    at_x = jnp.logical_and(lane >= o_x, lane < o_x + 32)
    sign_x, sign_y = (2 * gx - 1).astype(f32), (2 * gy - 1).astype(f32)
    for zl in range(2):
        hv = HVX[pl.ds(pl.multiple_of((zl * XL + pd) * 64, 8), 64), :]
        CGX[64 * zl:64 * zl + 64, :] = jnp.where(at_x, 1.0 + sign_x * hv, 0.0)

    @pl.loop(0, NP)
    def _(r):
        CGY[pl.ds(r, 1), :] = 1.0 + sign_y * HVY[pl.ds(r * 64 + y_send, 1), :]
    whole(SU, GX, u_send, x_recv).wait()

    def halo_xy(dst, recv):
        return whole(SU.at[pl.ds(0, 56), :], dst.at[pl.ds(0, 56), :], u_send, recv)

    def halo_z(dst, recv):
        return whole(SU.at[pl.ds(56, 64), :], dst.at[pl.ds(56, 64), :], z_send, recv)

    def ghost_of_z(k, e, ew, b, q, rows):
        g = ew * v8(RU[b, rows, :])
        for i in range(k):
            g = g - e[i] * v8(GMU[i, rows, :])
        GZ[k, rows, :] = (q * g).reshape(-1, 128)

    def sweep(V, unroll, put, ghost=None):
        def one(i, c):
            neighbours(V, i, put, ghost)
            return c
        pairs(unroll, one)

    def to_n(V):
        def put(r8, row, size, u, n):
            V.put(row, size, n)
        return put

    def givens(m, sub):
        h = [RM[i, m] for i in range(m + 1)]
        for i in range(m):
            cs, sn = CS[i], SN[i]
            h[i], h[i + 1] = cs * h[i] + sn * h[i + 1], cs * h[i + 1] - sn * h[i]
        d = h[m]
        rad = jnp.sqrt(d * d + sub * sub)
        cs, sn = d / rad, sub / rad
        CS[m] = cs
        SN[m] = sn
        h[m] = cs * d + sn * sub
        RM[0:m + 1, m] = jnp.stack(h)
        g = GV[m]
        GV[m] = cs * g
        GV[m + 1] = -sn * g
        est = MISC[4] * jnp.abs(sn)
        MISC[4] = est
        return est

    out_scale = 1.0 / math.sqrt(1572864.0)
    last_halo = CYCLES * RESTART - 3

    @pl.loop(0, CYCLES)
    def _(c):
        fill_ghosts(XS, GX)

        def put_r(r8, row, size, u, n):
            WS.put(row, size, SRC[r8 * 8:r8 * 8 + size, :] - (6.0 * u - n))
        sweep(XS, XL, put_r, GX.at[ZG, :])

        @pl.when(c == 0)
        def _():
            def one(r, row, acc):
                t = v8(WS.get(row, 64)).reshape(2, 4, 8, 128)
                return acc + jnp.sum(t * t, axis=0)
            acc = all_planes(one, jnp.zeros((4, 8, 128), f32), 2)
            sync_start(0, [(16, jnp.sum(acc, axis=0))])

        @pl.loop(0, RESTART)
        def _(j):
            step = c * RESTART + j
            par = (step + 1) % 2
            b = step % 2
            nxt = (j + 1) % RESTART
            slot = c * RESTART + (1 - c) * j + c * (j % 3)

            @pl.when(j * (j - LATE) >= 0)
            def _():
                seams(WS)
                sweep(WS, XL, to_n(Set(T1, 0)))
                seams(Set(T1, 0))

            @pl.when(j >= LATE)
            def _():
                q, r1, r2 = (jnp.concatenate([t] * 8, axis=0) for t in poly(c, j))

                def put_z(r8, row, size, u, n):
                    z = q * (WS.get(row, size) + r1 * u + r2 * n)
                    ZS.put(row, size, z)
                    Z[j, r8:r8 + size // 8] = v8(z)
                sweep(Set(T1, 0), XL, put_z)

            @pl.when(j == 0)
            def _():
                sweep(Set(T1, 0), XL, to_n(Set(T2, 0)))

                @pl.when(c == 0)
                def _():
                    three_at_once(0, GU.at[0], h_recv.at[1])
                    tot = sync_wait(0)
                    sync_all(0).wait_send()
                    beta0 = jnp.sqrt(bc(tot, 16))
                    MISC[0] = beta0
                    MISC[1] = 1.0 / beta0

                inv0 = MISC[1]
                q, r1, r2 = poly(c, 0)

                def start(r, row, acc):
                    u, n, n2 = (v8(t.get(row, 64)) * inv0 for t in (WS, Set(T1, 0), Set(T2, 0)))
                    z = q * (u + r1 * n + r2 * n2)
                    acc = acc + jnp.sum((u * u).reshape(2, 4, 8, 128), axis=0)
                    at = pl.ds(r * 8, 8)
                    U[0, at] = u
                    NU[0, at] = n
                    N2U[0, at] = n2
                    Z[0, at] = z
                    ZS.put(row, 64, z.reshape(64, 128))
                    return acc
                ACC[0] = jnp.sum(all_planes(start, jnp.zeros((4, 8, 128), f32)), axis=0)

                @pl.when(c == 0)
                def _():
                    whole(SB, GU.at[0], h_send, h_recv.at[1]).wait()

                    for t in range(3):
                        GU[0, t] = (v8(GU[0, t]) * inv0).reshape(GROWS, 128)

                GZ[0] = (q * (v8(GU[0, 0]) + r1 * v8(GU[0, 1]) + r2 * v8(GU[0, 2]))).reshape(GROWS, 128)

            seams(ZS)
            GX2[...] = GZ[j, ZG, :]

            def put_w(r8, row, size, u, n):
                WS.put(row, size, 6.0 * u - n)
            sweep(ZS, XL, put_w, GX2)

            for k in range(1, RESTART):
                @pl.when(j == k)
                def _():
                    halo_xy(RU.at[1 - b], u_recv.at[1 - b]).wait_recv()
                    ghost_of_z(k, [EC[i] for i in range(k)], EC[k], 1 - b, poly(c, k)[0], slice(0, 56))
            add_ghosts_xy(GZ.at[j])

            for k in range(RESTART):
                @pl.when(j == k)
                def _():
                    ends = k == 0 or k == RESTART - 1
                    wd = 4 if k < 4 else 2 if k < 8 else 1
                    count = k + 2 if ends else k + 1

                    def dots(t, accs):
                        accs = list(accs)
                        for zl in range(2):
                            x = t * 2 + zl * XL
                            w = jnp.concatenate([v8(WS.get(row0(t * 2 + (zl * PZ + 1 + i)), 64)) for i in range(2)])
                            w = w.reshape(16 // wd, wd, 8, 128)
                            for i in range(k + 1):
                                v = U[i, pl.ds(x * 8, 16)].reshape(16 // wd, wd, 8, 128)
                                accs[i] = accs[i] + jnp.sum(v * w, axis=0)
                            if ends:
                                accs[k + 1] = accs[k + 1] + jnp.sum(w * w, axis=0)
                        return tuple(accs)
                    accs = lax.fori_loop(0, XL // 2, dots, (jnp.zeros((wd, 8, 128), f32),) * count)
                    accs = [jnp.sum(a, axis=0) for a in accs]
                    items = [(i, accs[i]) for i in range(k + 1)] + [(16 + i, ACC[i]) for i in range(k + 1)]
                    if ends:
                        items.append((32, accs[k + 1]))
                    sync_start(par, items)

            @pl.when(step > 0)
            def _():
                sync_all(1 - par).wait_send()

            @pl.when(step < CYCLES * RESTART - 1)
            def _():
                seams(WS)
                sweep(WS, XL, to_n(Set(T1, b)))

            @pl.when(CYCLES * RESTART - 1 - step > 0)
            def _():
                seams(Set(T1, b))
                r1, r2 = (jnp.concatenate([t] * 8, axis=0) for t in poly(c, nxt)[1:])

                def put(r8, row, size, u, n):
                    Set(T2, b).put(row, size, n)
                    MW[r8 * 8:r8 * 8 + size, :] = WS.get(row, size) + r1 * u + r2 * n
                sweep(Set(T1, b), XL, put)

            @pl.when(j > 0)
            def _():
                halo_xy(RU.at[b], u_recv.at[b]).wait_send()
                halo_z(RU.at[b], z_recv.at[b]).wait_send()

            @pl.when(j < RESTART - 1)
            def _():
                pack_xy(of_mw, SU)
                halo_start(SU, RU.at[b], u_send, u_recv.at[b], (0, 1))
                pack_z(of_mw, SU)
                halo_start(SU, RU.at[b], z_send, z_recv.at[b], (2,))

            @pl.when(step <= last_halo + 1)
            def _():
                @pl.when(step > 0)
                def _():
                    whole(SB, RB.at[slot], h_send, h_recv.at[0]).wait_send()

                @pl.when(step <= last_halo)
                def _():
                    three_at_once(b, RB.at[slot], h_recv.at[step % 3])

                @pl.when(j > 0)
                def _():
                    whole(SB, RB.at[slot], h_send, h_recv.at[(step + 2) % 3]).wait_recv()

            prev = c * RESTART + (1 - c) * (j - 1) + c * ((j + 2) % 3)
            for k in range(RESTART):
                @pl.when(j == k)
                def _():
                    if k < RESTART - 1:
                        q, r1, r2 = poly(c, k + 1)
                        e = [EC[i] for i in range(k + 1)] if k else None

                        size = 8 if k < 4 else 4

                        def body(r, row, cy):
                            for y in range(0, 8, size):
                                at = pl.ds(r * 8 + y, size)
                                if k:
                                    n = e[k] * v8(Set(T1, 1 - b).get(row + 8 * y, 8 * size))
                                    n2 = e[k] * v8(Set(T2, 1 - b).get(row + 8 * y, 8 * size))
                                    for m in range(k):
                                        nm, n2m = NU[m, at], N2U[m, at]
                                        n = n - e[m] * nm
                                        n2 = n2 - e[m] * n2m
                                        MU[m, at] = U[m, at] + r1 * nm + r2 * n2m
                                    NU[k, at] = n
                                    N2U[k, at] = n2
                                else:
                                    n, n2 = NU[0, at], N2U[0, at]
                                MU[k, at] = U[k, at] + r1 * n + r2 * n2
                            return cy
                        if k < LATE - 1:
                            all_planes(body, 0)

                        if k:
                            for t in range(3):
                                g = e[k] * v8(RB[prev, t])
                                for i in range(k):
                                    g = g - e[i] * v8(GU[i, t])
                                GU[k, t] = g.reshape(GROWS, 128)

                        @pl.loop(0, k + 1)
                        def _(i):
                            g = v8(GU[i, 0]) + r1 * v8(GU[i, 1]) + r2 * v8(GU[i, 2])
                            GMU[i] = g.reshape(GROWS, 128)
                    if k >= 2:
                        est = givens(k - 2, NRM[k - 1] * MISC[3])
                        RES[c] = jnp.where(lane8 == k - 1, est, RES[c])

            tot = sync_wait(par)

            for k in range(RESTART):
                @pl.when(j == k)
                def _():
                    nn = bc(tot, 16 + k)
                    nrm = jnp.sqrt(nn)
                    sg = 1.0 / nrm
                    SIG[k] = sg
                    NRM[k] = nrm
                    sig = SIG[0:k + 1] * sg
                    h = jnp.stack([bc(tot, i) for i in range(k + 1)]) * sig
                    gcol = jnp.stack([bc(tot, 16 + i) for i in range(k + 1)]) * sig
                    GM[k, 0:k + 1] = gcol
                    if k > 0:
                        GM[0:k, k] = gcol[0:k]

                    def gram_times(x):
                        out = gcol * x[k]
                        for m in range(k):
                            out = out + GM[m, 0:k + 1] * x[m]
                        return out
                    cf = 2.0 * h - gram_times(h)
                    RM[0:k + 1, k] = cf
                    if k == 0:
                        beta = MISC[0] * nrm
                        MISC[4] = beta
                        GV[0] = beta
                        RES[c] = jnp.where(lane8 == 0, beta, 0.0)
                        wn = jnp.sqrt(bc(tot, 32)) * sg
                        MISC[3] = wn
                        rho = 1.0 / wn
                        MISC[2] = rho
                    else:
                        rho = MISC[2]
                    if k < RESTART - 1:
                        es = rho * cf * SIG[0:k + 1]
                        ew = rho * sg
                        EC[0:k + 1] = es
                        EC[k + 1] = ew
                        q = poly(c, k + 1)[0]

                        size = 8 if k < 2 else 4 if k < 5 else 2

                        def body(r, row, accs):
                            accs = list(accs)
                            for y in range(0, 8, size):
                                at = pl.ds(r * 8 + y, size)
                                v = [U[m, at] for m in range(k + 1)]
                                u = ew * v8(WS.get(row + 8 * y, 8 * size))
                                if k < LATE - 1:
                                    z = ew * v8(MW[pl.ds(pl.multiple_of(r * 64 + 8 * y, 8), 8 * size), :])
                                for m in range(k + 1):
                                    u = u - es[m] * v[m]
                                    if k < LATE - 1:
                                        z = z - es[m] * MU[m, at]
                                U[k + 1, at] = u
                                if k < LATE - 1:
                                    z = q * z
                                    Z[k + 1, at] = z
                                    ZS.put(row + 8 * y, 8 * size, z.reshape(8 * size, 128))
                                else:
                                    WS.put(row + 8 * y, 8 * size, u.reshape(8 * size, 128))
                                for m in range(k + 1):
                                    accs[m] = accs[m] + jnp.sum(u * v[m], axis=0)
                                accs[k + 1] = accs[k + 1] + jnp.sum(u * u, axis=0)
                            return tuple(accs)
                        accs = all_planes(body, (zero8,) * (k + 2))
                        ACC[0:k + 2] = jnp.stack(accs)
                        halo_z(RU.at[b], z_recv.at[b]).wait_recv()
                        ghost_of_z(k + 1, es, ew, b, q, slice(56, 120))
                    else:
                        wn2 = bc(tot, 32) * sg * sg
                        drop = jnp.sum(cf * (2.0 * h - gram_times(cf)), axis=0)
                        sub = jnp.sqrt(jnp.maximum(wn2 - drop, 0.0))
                        est = givens(k - 1, nrm * MISC[3])
                        RES[c] = jnp.where(lane8 == k, est, RES[c])
                        est = givens(k, sub)
                        RES[c] = jnp.where(lane8 == k + 1, est, RES[c])
                        g = [GV[i] for i in range(RESTART)]
                        for i in reversed(range(RESTART)):
                            y = g[i] / RM[i, i]
                            YY[i] = y * SIG[i]
                            for m in range(i):
                                g[m] = g[m] - RM[m, i] * y

        yy = [YY[i] for i in range(RESTART)]

        def update(r, row, cy):
            x = v8(XS.get(row, 64))
            for m in range(RESTART):
                x = x + yy[m] * Z[m, pl.ds(r * 8, 8)]
            x = x.reshape(64, 128)
            XS.put(row, 64, x)
            MW[pl.ds(pl.multiple_of(r * 64, 8), 64), :] = x
            return cy
        all_planes(update, 0)

        @pl.when(c == 0)
        def _():
            inv = MISC[1]
            whole(SB, RB.at[RESTART - 1], h_send, h_recv.at[(RESTART - 1) % 3]).wait_recv()

            g = v8(GX[...])
            for m in range(RESTART):
                g = g + yy[m] * v8(GZ[m])
            GX[...] = g.reshape(GROWS, 128)
            for t in range(3):
                g = yy[0] * v8(RB[0, t])
                for m in range(1, RESTART):
                    g = g + yy[m] * v8(RB[m, t])
                GU[0, t] = (v8(GU[0, t]) - inv * g).reshape(GROWS, 128)

    cp = pltpu.make_async_copy(MW, out_hbm, l_sem.at[0, 0])
    cp.start()
    sync_all((CYCLES * RESTART) % 2).wait_send()
    rows = jnp.where(lax.broadcasted_iota(jnp.int32, (8, 128), 0) == 0, RES[0], RES[1]) * out_scale
    res_ref[...] = rows
    cp.wait()


def unpack(x_hbm, r_hbm, out_hbm, res_ref, xin, rin, out, in_sem, out_sem):
    f32 = jnp.float32
    parts = 3
    n = XL // parts
    loads = [[pltpu.make_async_copy(x_hbm.at[zl, pl.ds(t * n, n)], xin.at[zl, pl.ds(t * n, n)], in_sem.at[t, zl])
              for zl in range(2)] for t in range(parts)]
    stores = [[pltpu.make_async_copy(out.at[h, pl.ds(t * n, n)], out_hbm.at[h, pl.ds(t * n, n)], out_sem.at[t, h])
               for h in range(4)] for t in range(parts)]
    rows = pltpu.make_async_copy(r_hbm, rin, in_sem.at[parts, 0])
    for cp in [c for t in loads for c in t] + [rows]:
        cp.start()
    a = lax.broadcasted_iota(jnp.int32, (256, 256), 0)
    d = lax.broadcasted_iota(jnp.int32, (256, 256), 1)
    a0 = a - jnp.where(a >= 128, 128, 0)
    h = jnp.where(a0 >= 96, 3, jnp.where(a0 >= 64, 2, jnp.where(a0 >= 32, 1, 0)))
    m = jnp.where(d == 64 * h + 2 * (a0 - 32 * h) + jnp.where(a >= 128, 1, 0), 1.0, 0.0).astype(jnp.bfloat16)
    for t in range(parts):
        for cp in loads[t]:
            cp.wait()
        for i in range(t * n, t * n + n):
            v = jnp.concatenate([xin[0, i], xin[1, i]], axis=1)
            a1 = v.astype(jnp.bfloat16)
            v = v - a1.astype(f32)
            a2 = v.astype(jnp.bfloat16)
            a3 = (v - a2.astype(f32)).astype(jnp.bfloat16)
            o = [jnp.dot(p, m, preferred_element_type=f32) for p in (a1, a2, a3)]
            o = (o[2] + o[1]) + o[0]
            for h in range(4):
                out[h, i] = o[:, 64 * h:64 * h + 64]
        for cp in stores[t]:
            cp.start()
    rows.wait()
    res_ref[...] = rin[0:CYCLES, 0:RESTART + 1]
    for cp in [c for t in stores for c in t]:
        cp.wait()


def solution(mesh):
    grid_spec = P(('sys', 'gx'), 'gy', 'gz')
    vel_spec = P(None, ('sys', 'gx'), 'gy', 'gz')
    table_spec = P('sys', None)
    f32 = jnp.float32

    def local_solve(source, initial, velocity, damping):
        big = (SETR, 128)
        vol, flat = (NP * 8, 8, 128), (NP * 64, 128)
        v = lambda *s: pltpu.VMEM(s, f32)
        n = RESTART
        scratch = [
            v(n, *vol), v(LATE - 1, *vol), v(LATE - 1, *vol), v(LATE - 1, *vol), v(n, *vol),
            v(*big), v(*big), v(*big), v(2, *big), v(2, *big), v(*flat),
            v(*flat), v(*flat), v(*flat), v(*flat), v(*flat), v(*flat), v(128, 128), v(NP, 128), v(NP, 128),
            v(n - 1, 3, GROWS, 128), v(n - 1, GROWS, 128), v(n + 3, 3, GROWS, 128), v(2, GROWS, 128),
            v(3, GROWS, 128), v(GROWS, 128), v(n, GROWS, 128), v(GROWS, 128), v(64, 128),
            v(2, 8, 128), v(n + 1, 8, 128), v(n, n, 8, 128), v(n, n, 8, 128),
            v(n, 8, 128), v(n + 1, 8, 128), v(n, 8, 128), v(n, 8, 128), v(n + 1, 8, 128), v(n, 8, 128), v(n, 8, 128),
            v(CYCLES, 8, 128), v(8, 8, 128), v(4, 48, 64, 64), pltpu.VMEM((256, 256), jnp.bfloat16),
            pltpu.SemaphoreType.DMA((2,)), pltpu.SemaphoreType.DMA((2,)), pltpu.SemaphoreType.DMA,
            pltpu.SemaphoreType.DMA((3,)), pltpu.SemaphoreType.DMA, pltpu.SemaphoreType.DMA((2,)),
            pltpu.SemaphoreType.DMA, pltpu.SemaphoreType.DMA((2,)), pltpu.SemaphoreType.DMA, pltpu.SemaphoreType.DMA((5, 4)),
        ]
        hbm = pl.BlockSpec(memory_space=pl.ANY)
        packed, rows = pl.pallas_call(
            kernel,
            out_shape=(jax.ShapeDtypeStruct(flat, f32), jax.ShapeDtypeStruct((8, 128), f32)),
            in_specs=[hbm, hbm, hbm, pl.BlockSpec(memory_space=pltpu.SMEM)],
            out_specs=(hbm, pl.BlockSpec(memory_space=pltpu.VMEM)),
            scratch_shapes=scratch,
            compiler_params=pltpu.CompilerParams(
                collective_id=0, has_side_effects=True, vmem_limit_bytes=67043328),
            name='fgmres',
        )(source, initial, velocity, damping)
        out, res = pl.pallas_call(
            unpack,
            out_shape=(jax.ShapeDtypeStruct((4, XL, 64, 64), f32), jax.ShapeDtypeStruct((CYCLES, n + 1), f32)),
            in_specs=[hbm, hbm],
            out_specs=(hbm, pl.BlockSpec(memory_space=pltpu.VMEM)),
            scratch_shapes=[v(2, XL, 64, 128), v(8, 128), v(4, XL, 64, 64),
                            pltpu.SemaphoreType.DMA((4, 2)), pltpu.SemaphoreType.DMA((3, 4))],
            name='unpack',
        )(packed.reshape(2, XL, 64, 128), rows)
        return out.reshape(source.shape), res

    return jax.shard_map(local_solve, mesh=mesh, in_specs=(grid_spec, grid_spec, vel_spec, table_spec),
                         out_specs=(grid_spec, table_spec), check_vma=False)
```

```python
import math
import jax
import jax.numpy as jnp
from jax import lax
from jax.experimental import pallas as pl
from jax.experimental.pallas import tpu as pltpu
from jax.sharding import PartitionSpec as P

MESH = pl.DeviceIdType.MESH
RESTART = 10
CYCLES = 2
XL = 12
NP = 2 * XL
PZ = XL + 2
LO, HI, ROWS = 8, 72, 80
SETR = 2 * PZ * ROWS
LATE = 8
XG, YG, ZG = slice(0, 32), slice(32, 56), slice(56, 120)
GROWS = 120
DEALT = 2


def pairs(unroll, body, carry=()):
    if unroll == XL:
        for i in range(XL):
            carry = body(i, carry)
        return carry

    def trip(t, carry):
        for i in range(unroll):
            carry = body(t * unroll + i, carry)
        return carry
    return lax.fori_loop(0, XL // unroll, trip, carry)


def v8(x):
    return x.reshape(-1, 8, 128)


class Set:
    def __init__(self, ref, t=None):
        self.ref, self.t = ref, t

    def index(self, start, size):
        rows = pl.ds(start, size) if not isinstance(start, int) else slice(start, start + size)
        return (rows, slice(None)) if self.t is None else (self.t, rows, slice(None))

    def get(self, start, size):
        return self.ref[self.index(start, size)]

    def put(self, start, size, v):
        self.ref[self.index(start, size)] = v

    def view(self, start, size):
        return self.ref.at[self.index(start, size)]


def row0(p):
    r = p * ROWS + LO
    return r if isinstance(r, int) else pl.multiple_of(r, 8)


def rearrange(v, m):
    f32 = jnp.float32
    a1 = v.astype(jnp.bfloat16)
    v = v - a1.astype(f32)
    a2 = v.astype(jnp.bfloat16)
    a3 = (v - a2.astype(f32)).astype(jnp.bfloat16)
    n = v.shape[0]
    o = jnp.dot(jnp.concatenate([a1, a2, a3], axis=0), m, preferred_element_type=f32)
    return (o[2 * n:] + o[n:2 * n]) + o[:n]


def all_planes(body, carry, step=1):
    def trip(t, carry):
        for zl in range(2):
            for i in range(step):
                x = t * step + i
                carry = body(x + zl * XL, row0(x + (zl * PZ + 1)), carry)
        return carry
    return lax.fori_loop(0, XL // step, trip, carry)


def kernel(src_hbm, ini_hbm, vel_hbm, damp_ref, out_hbm, res_ref,
           U, NU, N2U, MU, Z, ZC, X, W, T1, T2, MW, SRC, CZP, CZM, HVX, HVY, CZA, CGX, CGY, YB,
           GU, GMU, RB, RU, SB, SU, GZ, GX, GX2, SS, ACC, GM, RM, SIG, EC, KAP, SW, CS, SN, GV, YY, NRM, RES, MISC, STG, DEAL,
           s_send, s_recv, h_send, h_recv, u_send, u_recv, z_send, z_recv, x_recv, l_sem):
    f32 = jnp.float32
    gx, gy, gz = lax.axis_index('gx'), lax.axis_index('gy'), lax.axis_index('gz')
    peers = {}
    for p in range(1, 8):
        a, b, c = p // 4, (p // 2) % 2, p % 2
        peers[p] = {'gx': 1 - gx if a else gx, 'gy': 1 - gy if b else gy, 'gz': 1 - gz if c else gz}
    side = {0: 4, 1: 2, 2: 1}

    def load(q, slot, h, src):
        return pltpu.make_async_copy(src.at[pl.ds(XL * h, XL)], STG.at[slot, pl.ds(XL * h, XL)], l_sem.at[q, h])

    def load_start(q, slot, src):
        for h in range(4):
            load(q, slot, h, src).start()
    load_start(0, 0, ini_hbm)
    bar = pltpu.get_barrier_semaphore()
    for p in range(1, 8):
        pl.semaphore_signal(bar, inc=1, device_id=peers[p], device_id_type=MESH)

    lane = lax.broadcasted_iota(jnp.int32, (64, 128), 1)
    lane8 = lane[0:8]
    left = lane < 64
    zh = jnp.where(left, jnp.where(lane < 32, lane, lane - 32), jnp.where(lane < 96, lane - 64, lane - 96))
    zh32 = zh[0:32]
    first_q, last_q = lane < 32, lane >= 96
    zero64 = jnp.zeros((64, 128), f32)
    zero8 = jnp.zeros((8, 128), f32)
    hi_x = (1 - gx).astype(f32)
    l0 = 31 * (1 - gz)
    o_x = 96 * (1 - gx)
    y_send = 63 * (1 - gy)
    y_pad = HI - 65 * gy
    edge_lo = zh32 == 32 * (1 - gz)
    edge_hi = zh32 == 31 + 32 * gz
    WS, ZS, XS = Set(W), Set(ZC), Set(X)

    def seams(V, ghost=None):
        for zl in range(2):
            b = zl * PZ
            a = pltpu.roll(V.get(row0(b + XL), 64), 32, 1)
            d = pltpu.roll(V.get(row0(b + 1), 64), 96, 1)
            lo = 0.0 if ghost is None else ghost[zl] * (1.0 - hi_x)
            hi = 0.0 if ghost is None else ghost[zl] * hi_x
            V.put(row0(b), 64, jnp.where(first_q, lo, a))
            V.put(row0(b + XL + 1), 64, jnp.where(last_q, hi, d))

    def neighbours(V, i, put, ghost=None):
        size = 64 if ghost is None else 32
        for y in range(0, 64, size):
            co = lambda C, r: C[r * 64 + y:r * 64 + y + size, :]
            at = lambda q, d: V.get(row0(q) + y + d, size)
            u0, u1 = at(i + 1, 0), at(i + (PZ + 1), 0)
            below, above = pltpu.roll(u1, 1, 1), pltpu.roll(u0, 127, 1)
            if ghost is None:
                cm0, cp1 = co(CZM, i), co(CZP, i + XL)
            else:
                g = pltpu.roll(ghost[y:y + size, :], (l0 - i + 128) % 128, 1)
                below = jnp.where(edge_lo, g, below)
                above = jnp.where(edge_hi, g, above)
                cm0, cp1 = co(CZA, i), co(CZA, i + XL)
            for zl, u, n in ((0, u0, co(CZP, i) * u1 + cm0 * below), (1, u1, co(CZM, i + XL) * u0 + cp1 * above)):
                q, r = i + (zl * PZ + 1), i + zl * XL
                yp, ym = at(q, 1), at(q, -1)
                xp, xm = at(q + 1, 0), at(q - 1, 0)
                n = n + (xp + xm) - co(HVX, r) * (xp - xm)
                n = n + (yp + ym) - co(HVY, r) * (yp - ym)
                put(r * 8 + y // 8, row0(q) + y, size, u, n)

    def spread_x(rec):
        g = rec[XG, :]
        return [jnp.concatenate([pltpu.roll(g, (o_x - 64 * zl - 32 * yh + 128) % 128, 1) for yh in range(2)], axis=0)
                for zl in range(2)]

    def fill_ghosts(V, rec):
        seams(V, spread_x(rec))

        @pl.loop(0, 2)
        def _(zl):
            for i in range(XL):
                V.put((zl * PZ + (i + 1)) * ROWS + y_pad, 1, rec[pl.ds(zl * XL + (i + 32), 1), :])

    def add_ghosts_xy(rec):
        pd = (XL - 1) * (1 - gx)
        for zl, g in enumerate(spread_x(rec)):
            row = (pd + (zl * PZ + 1)) * ROWS + LO
            WS.put(row, 64, WS.get(row, 64) - CGX[64 * zl:64 * zl + 64, :] * g)
        YB[...] = CGY[...] * rec[YG, :]
        for r in range(NP):
            row = row0(r % XL + r // XL * PZ + 1) + y_send
            WS.put(row, 1, WS.get(row, 1) - YB[r:r + 1, :])

    def pack_xy(get, out):
        pd = (XL - 1) * (1 - gx)
        acc = zero64[0:32]
        for zl in range(2):
            for yh in range(2):
                slot = 2 * zl + yh
                r = pltpu.roll(get(zl, pd, 32 * yh, 32), (32 * slot - o_x + 128) % 128, 1)
                here = jnp.logical_and(lane[0:32] >= 32 * slot, lane[0:32] < 32 * slot + 32)
                acc = jnp.where(here, r, acc)
        out[XG, :] = acc

        for zl in range(2):
            for i in range(XL):
                r = 32 + zl * XL + i
                out[r:r + 1, :] = get(zl, i, y_send, 1)

    def pack_z(get, out):
        acc = zero64
        for i in range(XL):
            r = pltpu.roll(get(1 - gz, i, 0, 64), (i - l0 + 128) % 128, 1)
            acc = jnp.where(zh == i, r, acc)
        out[ZG, :] = acc

    def pack(get, out):
        pack_xy(get, out)
        pack_z(get, out)

    def of_set(V):
        return lambda zl, i, y, n: V.get((zl * PZ + i + 1) * ROWS + LO + y, n)

    def of_mw(zl, i, y, n):
        return MW[pl.ds((zl * XL + i) * 64 + y, n), :]

    def halo_start(src, dst, send, recv, axes=(0, 1, 2)):
        for ax in axes:
            rows = (XG, YG, ZG)[ax]
            pltpu.make_async_remote_copy(
                src_ref=src.at[rows, :], dst_ref=dst.at[rows, :], send_sem=send, recv_sem=recv,
                device_id=peers[side[ax]], device_id_type=MESH).start()

    def whole(src, dst, send, recv):
        return pltpu.make_async_remote_copy(src_ref=src, dst_ref=dst, send_sem=send, recv_sem=recv,
                                            device_id=peers[1], device_id_type=MESH)

    def three_at_once(b, dst, recv, recv_z=None):
        sets = (WS, Set(T1, b), Set(T2, b))
        for q, t in enumerate(sets):
            pack_xy(of_set(t), SB.at[q])
        for q, t in enumerate(sets):
            pack_z(of_set(t), SB.at[q])
        for q in range(3):
            halo_start(SB.at[q], dst.at[q], h_send, recv, (0, 1))
            halo_start(SB.at[q], dst.at[q], h_send, recv if recv_z is None else recv_z, (2,))

    def sync_all(par):
        return pltpu.make_async_remote_copy(
            src_ref=SS.at[par, pl.ds(1, 7), :], dst_ref=SS.at[par, pl.ds(1, 7), :],
            send_sem=s_send.at[par], recv_sem=s_recv.at[par], device_id=peers[1], device_id_type=MESH)

    def sync_start(par, items):
        row = zero8
        for idx, acc in items:
            row = jnp.where(lane8 == idx, jnp.sum(acc, axis=1, keepdims=True), row)
        row = row + pltpu.roll(row, 4, 0)
        row = row + pltpu.roll(row, 2, 0)
        row = row + pltpu.roll(row, 1, 0)
        SS[par, 0:1, :] = row[0:1]
        for p in (6, 7, 5, 3, 4, 2, 1):
            pltpu.make_async_remote_copy(
                src_ref=SS.at[par, pl.ds(0, 1), :], dst_ref=SS.at[par, pl.ds(p, 1), :],
                send_sem=s_send.at[par], recv_sem=s_recv.at[par],
                device_id=peers[p], device_id_type=MESH).start()

    def sync_wait(par):
        sync_all(par).wait_recv()
        tot = SS[par]
        tot = tot + pltpu.roll(tot, 4, 0)
        tot = tot + pltpu.roll(tot, 2, 0)
        return tot + pltpu.roll(tot, 1, 0)

    def bc(tot, k):
        return jnp.broadcast_to(tot[:, k:k + 1], (8, 128))

    def fold(x):
        return jnp.sum(v8(x), axis=0)

    def poly(c, j):
        s = damp_ref[c, j] / 6.0
        a0, a1, a2 = 3.0 * s, 3.0 * s * s, s * s * s
        q = jnp.full((8, 128), a0 - 6.0 * a1 + 36.0 * a2, f32)
        return q, (a1 - 12.0 * a2) / q, a2 / q

    @pl.loop(0, 2 * PZ)
    def _(p):
        for V in (ZS, XS, WS, Set(T1, 0), Set(T1, 1)):
            V.put(pl.multiple_of(p * ROWS, 8), 8, zero8)
            V.put(pl.multiple_of(p * ROWS + HI, 8), 8, zero8)

    a = lax.broadcasted_iota(jnp.int32, (256, 256), 0)
    d = lax.broadcasted_iota(jnp.int32, (256, 256), 1)
    d0 = d - jnp.where(d >= 128, 128, 0)
    h = jnp.where(d0 >= 96, 3, jnp.where(d0 >= 64, 2, jnp.where(d0 >= 32, 1, 0)))
    target = 64 * h + 2 * (d0 - 32 * h) + jnp.where(d >= 128, 1, 0)
    DEAL[...] = jnp.where(a == target, 1.0, 0.0).astype(jnp.bfloat16)

    @pl.loop(0, 5)
    def _(q):
        for h in range(4):
            load(q, q % 4, h, ini_hbm).wait()

        @pl.when(q == 0)
        def _():
            for d in range(3):
                load_start(1 + d, 1 + d, vel_hbm.at[d])
        m = DEAL[...]
        for i in range(0, XL, DEALT):
            v = jnp.concatenate([jnp.concatenate([STG[q % 4, h * XL + x] for h in range(4)], axis=1)
                                 for x in range(i, i + DEALT)], axis=0)
            o = rearrange(v, m)
            o = v8(o[:, 0:128]), v8(o[:, 128:256])
            for zl in range(2):
                U[q, (i + zl * XL) * 8:(i + DEALT + zl * XL) * 8] = o[zl]

        @pl.when(q == 0)
        def _():
            load_start(4, 0, src_hbm)

            def take_x(r, row, c):
                XS.put(row, 64, U[0, pl.ds(r * 8, 8)].reshape(64, 128))
                return c
            all_planes(take_x, 0)
            pack(of_set(XS), SU)
            pl.semaphore_wait(bar, 7)
            halo_start(SU, GX, u_send, x_recv)

    @pl.loop(0, XL)
    def _(i):
        at = lambda q, r: U[q, pl.ds(r * 8, 8)].reshape(64, 128)
        low = pl.ds(pl.multiple_of(i * 64, 8), 64)
        high = pl.ds(pl.multiple_of((i + XL) * 64, 8), 64)
        for rows, r in ((low, i), (high, i + XL)):
            HVX[rows, :] = 0.5 * at(1, r)
            HVY[rows, :] = 0.5 * at(2, r)
            SRC[rows, :] = at(4, r)
        h0, h1 = at(3, i), at(3, i + XL)
        cm0, cp1 = 1.0 + 0.5 * h0, 1.0 - 0.5 * h1
        CZP[low, :] = 1.0 - 0.5 * h0
        CZM[low, :] = jnp.where(zh == 0, 0.0, cm0)
        CZA[low, :] = jnp.where(zh == 32 * gz, 0.0, cm0)
        CZM[high, :] = 1.0 + 0.5 * h1
        CZP[high, :] = jnp.where(zh == 31, 0.0, cp1)
        CZA[high, :] = jnp.where(zh == 63 - 32 * gz, 0.0, cp1)

    pd = (XL - 1) * (1 - gx)
    at_x = jnp.logical_and(lane >= o_x, lane < o_x + 32)
    sign_x, sign_y = (2 * gx - 1).astype(f32), (2 * gy - 1).astype(f32)
    for zl in range(2):
        hv = HVX[pl.ds(pl.multiple_of((zl * XL + pd) * 64, 8), 64), :]
        CGX[64 * zl:64 * zl + 64, :] = jnp.where(at_x, 1.0 + sign_x * hv, 0.0)

    @pl.loop(0, NP)
    def _(r):
        CGY[pl.ds(r, 1), :] = 1.0 + sign_y * HVY[pl.ds(r * 64 + y_send, 1), :]
    whole(SU, GX, u_send, x_recv).wait()

    def halo_xy(dst, recv):
        return whole(SU.at[pl.ds(0, 56), :], dst.at[pl.ds(0, 56), :], u_send, recv)

    def halo_z(dst, recv):
        return whole(SU.at[pl.ds(56, 64), :], dst.at[pl.ds(56, 64), :], z_send, recv)

    def ghost_of_z(k, e, b, q, rows):
        g = v8(RU[b, rows, :])
        for i in range(k):
            g = g - e[i] * v8(GMU[i, rows, :])
        GZ[k, rows, :] = (q * g).reshape(-1, 128)

    def first_ghosts(rows, scale, q, r1, r2):
        g = [v8(GU[0, t, rows, :]) for t in range(3)]
        if scale is not None:
            g = [t * scale for t in g]
            for t in range(3):
                GU[0, t, rows, :] = g[t].reshape(-1, 128)
        GZ[0, rows, :] = (q * (g[0] + r1 * g[1] + r2 * g[2])).reshape(-1, 128)

    def sweep(V, unroll, put, ghost=None):
        def one(i, c):
            neighbours(V, i, put, ghost)
            return c
        pairs(unroll, one)

    def to_n(V):
        def put(r8, row, size, u, n):
            V.put(row, size, n)
        return put

    def givens(m, sub):
        h = [RM[i, m] for i in range(m + 1)]
        for i in range(m):
            cs, sn = CS[i], SN[i]
            h[i], h[i + 1] = cs * h[i] + sn * h[i + 1], cs * h[i + 1] - sn * h[i]
        d = h[m]
        rad = jnp.sqrt(d * d + sub * sub)
        cs, sn = d / rad, sub / rad
        CS[m] = cs
        SN[m] = sn
        h[m] = cs * d + sn * sub
        RM[0:m + 1, m] = jnp.stack(h)
        g = GV[m]
        GV[m] = cs * g
        GV[m + 1] = -sn * g
        est = MISC[4] * jnp.abs(sn)
        MISC[4] = est
        return est

    out_scale = 1.0 / math.sqrt(1572864.0)
    last_halo = CYCLES * RESTART - 3

    @pl.loop(0, CYCLES)
    def _(c):
        fill_ghosts(XS, GX)

        def put_r(r8, row, size, u, n):
            WS.put(row, size, SRC[r8 * 8:r8 * 8 + size, :] - (6.0 * u - n))
        sweep(XS, XL, put_r, GX.at[ZG, :])

        @pl.when(c == 0)
        def _():
            def one(r, row, acc):
                t = v8(WS.get(row, 64)).reshape(2, 4, 8, 128)
                return acc + jnp.sum(t * t, axis=0)
            acc = all_planes(one, jnp.zeros((4, 8, 128), f32), 2)
            sync_start(0, [(16, jnp.sum(acc, axis=0))])

        @pl.loop(0, RESTART)
        def _(j):
            step = c * RESTART + j
            par = (step + 1) % 2
            b = step % 2
            nxt = (j + 1) % RESTART
            slot = c * RESTART + (1 - c) * j + c * (j % 3)

            @pl.when(j * (j - LATE) >= 0)
            def _():
                seams(WS)
                sweep(WS, XL, to_n(Set(T1, 0)))
                seams(Set(T1, 0))

            @pl.when(j >= LATE)
            def _():
                q, r1, r2 = poly(c, j)
                q, r1, r2 = (jnp.concatenate([t] * 8, axis=0) for t in (q * KAP[j], r1, r2))

                def put_z(r8, row, size, u, n):
                    z = q * (WS.get(row, size) + r1 * u + r2 * n)
                    ZS.put(row, size, z)
                    Z[j, r8:r8 + size // 8] = v8(z)
                sweep(Set(T1, 0), XL, put_z)

            @pl.when(j == 0)
            def _():
                sweep(Set(T1, 0), XL, to_n(Set(T2, 0)))

                @pl.when(c == 0)
                def _():
                    three_at_once(0, GU.at[0], h_recv.at[1], z_recv.at[1])
                    tot = sync_wait(0)
                    sync_all(0).wait_send()
                    beta0 = jnp.sqrt(bc(tot, 16))
                    MISC[0] = beta0
                    MISC[1] = 1.0 / beta0

                inv0 = MISC[1]
                KAP[0] = jnp.ones((8, 128), f32)
                q, r1, r2 = poly(c, 0)

                def start(r, row, acc):
                    u, n, n2 = (v8(t.get(row, 64)) * inv0 for t in (WS, Set(T1, 0), Set(T2, 0)))
                    z = q * (u + r1 * n + r2 * n2)
                    acc = acc + jnp.sum((u * u).reshape(2, 4, 8, 128), axis=0)
                    at = pl.ds(r * 8, 8)
                    U[0, at] = u
                    NU[0, at] = n
                    N2U[0, at] = n2
                    Z[0, at] = z
                    ZS.put(row, 64, z.reshape(64, 128))
                    return acc
                ACC[0] = jnp.sum(all_planes(start, jnp.zeros((4, 8, 128), f32)), axis=0)

                @pl.when(c == 0)
                def _():
                    whole(SB.at[:, pl.ds(56, 64), :], GU.at[0, :, pl.ds(56, 64), :], h_send, z_recv.at[1]).wait_recv()
                    first_ghosts(slice(56, 120), inv0, q, r1, r2)

                @pl.when(c > 0)
                def _():
                    first_ghosts(slice(0, 120), None, q, r1, r2)

            seams(ZS)
            GX2[...] = GZ[j, ZG, :]

            def put_w(r8, row, size, u, n):
                WS.put(row, size, 6.0 * u - n)
            sweep(ZS, XL, put_w, GX2)

            for k in range(1, RESTART):
                @pl.when(j == k)
                def _():
                    halo_xy(RU.at[1 - b], u_recv.at[1 - b]).wait_recv()
                    ghost_of_z(k, [EC[i] for i in range(k)], 1 - b, KAP[k] * poly(c, k)[0], slice(0, 56))

            @pl.when(step == 0)
            def _():
                whole(SB.at[:, pl.ds(0, 56), :], GU.at[0, :, pl.ds(0, 56), :], h_send, h_recv.at[1]).wait_recv()
                whole(SB, GU.at[0], h_send, h_recv.at[1]).wait_send()
                first_ghosts(slice(0, 56), MISC[1], *poly(c, 0))
            add_ghosts_xy(GZ.at[j])

            for k in range(RESTART):
                @pl.when(j == k)
                def _():
                    ends = k == 0 or k == RESTART - 1
                    wd = 4 if k < 4 else 2 if k < 8 else 1
                    count = k + 2 if ends else k + 1

                    def dots(t, accs):
                        accs = list(accs)
                        for zl in range(2):
                            x = t * 2 + zl * XL
                            w = jnp.concatenate([v8(WS.get(row0(t * 2 + (zl * PZ + 1 + i)), 64)) for i in range(2)])
                            w = w.reshape(16 // wd, wd, 8, 128)
                            for i in range(k + 1):
                                v = U[i, pl.ds(x * 8, 16)].reshape(16 // wd, wd, 8, 128)
                                accs[i] = accs[i] + jnp.sum(v * w, axis=0)
                            if ends:
                                accs[k + 1] = accs[k + 1] + jnp.sum(w * w, axis=0)
                        return tuple(accs)
                    accs = lax.fori_loop(0, XL // 2, dots, (jnp.zeros((wd, 8, 128), f32),) * count)
                    accs = [jnp.sum(a, axis=0) for a in accs]
                    items = [(i, accs[i]) for i in range(k + 1)] + [(16 + i, ACC[i]) for i in range(k + 1)]
                    if ends:
                        items.append((32, accs[k + 1]))
                    sync_start(par, items)

            @pl.when(step > 0)
            def _():
                sync_all(1 - par).wait_send()

            @pl.when(step < CYCLES * RESTART - 1)
            def _():
                seams(WS)
                sweep(WS, XL, to_n(Set(T1, b)))

            @pl.when(CYCLES * RESTART - 1 - step > 0)
            def _():
                seams(Set(T1, b))
                r1, r2 = (jnp.concatenate([t] * 8, axis=0) for t in poly(c, nxt)[1:])

                def put(r8, row, size, u, n):
                    Set(T2, b).put(row, size, n)
                    MW[r8 * 8:r8 * 8 + size, :] = WS.get(row, size) + r1 * u + r2 * n
                sweep(Set(T1, b), XL, put)

            @pl.when(j > 0)
            def _():
                halo_xy(RU.at[b], u_recv.at[b]).wait_send()
                halo_z(RU.at[b], z_recv.at[b]).wait_send()

            @pl.when(j < RESTART - 1)
            def _():
                pack_xy(of_mw, SU)
                halo_start(SU, RU.at[b], u_send, u_recv.at[b], (0, 1))
                pack_z(of_mw, SU)
                halo_start(SU, RU.at[b], z_send, z_recv.at[b], (2,))

            @pl.when(step <= last_halo + 1)
            def _():
                @pl.when(step > 0)
                def _():
                    whole(SB, RB.at[slot], h_send, h_recv.at[0]).wait_send()

                @pl.when(step <= last_halo)
                def _():
                    three_at_once(b, RB.at[slot], h_recv.at[step % 3])

                @pl.when(j > 0)
                def _():
                    whole(SB, RB.at[slot], h_send, h_recv.at[(step + 2) % 3]).wait_recv()

            prev = c * RESTART + (1 - c) * (j - 1) + c * ((j + 2) % 3)
            for k in range(RESTART):
                @pl.when(j == k)
                def _():
                    if k < RESTART - 1:
                        q, r1, r2 = poly(c, k + 1)
                        e = [EC[i] for i in range(k)]

                        size = 8 if k < 4 else 2

                        def body(r, row, cy):
                            for y in range(0, 8, size):
                                at = pl.ds(r * 8 + y, size)
                                if k:
                                    n = v8(Set(T1, 1 - b).get(row + 8 * y, 8 * size))
                                    n2 = v8(Set(T2, 1 - b).get(row + 8 * y, 8 * size))
                                    for m in range(k):
                                        nm, n2m = NU[m, at], N2U[m, at]
                                        n = n - e[m] * nm
                                        n2 = n2 - e[m] * n2m
                                        MU[m, at] = U[m, at] + r1 * nm + r2 * n2m
                                    NU[k, at] = n
                                    N2U[k, at] = n2
                                else:
                                    n, n2 = NU[0, at], N2U[0, at]
                                MU[k, at] = U[k, at] + r1 * n + r2 * n2
                            return cy
                        if k < LATE - 1:
                            all_planes(body, 0)

                        if k:
                            for t in range(3):
                                g = v8(RB[prev, t])
                                for i in range(k):
                                    g = g - e[i] * v8(GU[i, t])
                                GU[k, t] = g.reshape(GROWS, 128)

                        @pl.loop(0, k + 1)
                        def _(i):
                            g = v8(GU[i, 0]) + r1 * v8(GU[i, 1]) + r2 * v8(GU[i, 2])
                            GMU[i] = g.reshape(GROWS, 128)
                    if k >= 2:
                        est = givens(k - 2, NRM[k - 1] * SW[k - 2])
                        RES[c] = jnp.where(lane8 == k - 1, est, RES[c])

            tot = sync_wait(par)

            for k in range(RESTART):
                @pl.when(j == k)
                def _():
                    nn = bc(tot, 16 + k)
                    nrm = jnp.sqrt(nn)
                    sg = 1.0 / nrm
                    SIG[k] = sg
                    NRM[k] = nrm
                    kap = KAP[k]
                    sw = sg / kap
                    SW[k] = sw
                    sig = SIG[0:k + 1]
                    h = jnp.stack([bc(tot, i) for i in range(k + 1)]) * (sig * sw)
                    gcol = jnp.stack([bc(tot, 16 + i) for i in range(k + 1)]) * (sig * sg)
                    GM[k, 0:k + 1] = gcol
                    if k > 0:
                        GM[0:k, k] = gcol[0:k]

                    def gram_times(x):
                        out = gcol * x[k]
                        for m in range(k):
                            out = out + GM[m, 0:k + 1] * x[m]
                        return out
                    cf = 2.0 * h - gram_times(h)
                    RM[0:k + 1, k] = cf
                    if k == 0:
                        beta = MISC[0] * nrm
                        MISC[4] = beta
                        GV[0] = beta
                        RES[c] = jnp.where(lane8 == 0, beta, 0.0)
                        wn = jnp.sqrt(bc(tot, 32)) * sw
                        rho = 1.0 / wn
                        MISC[2] = rho
                    else:
                        rho = MISC[2]
                    if k < RESTART - 1:
                        es = cf * (sig * (kap * nrm))
                        EC[0:k + 1] = es
                        KAP[k + 1] = rho * sg
                        q = (rho * sg) * poly(c, k + 1)[0]

                        size = 8 if k < 2 else 4 if k < 5 else 2

                        def body(r, row, accs):
                            accs = list(accs)
                            for y in range(0, 8, size):
                                at = pl.ds(r * 8 + y, size)
                                v = [U[m, at] for m in range(k + 1)]
                                u = v8(WS.get(row + 8 * y, 8 * size))
                                if k < LATE - 1:
                                    z = v8(MW[pl.ds(pl.multiple_of(r * 64 + 8 * y, 8), 8 * size), :])
                                for m in range(k + 1):
                                    u = u - es[m] * v[m]
                                    if k < LATE - 1:
                                        z = z - es[m] * MU[m, at]
                                U[k + 1, at] = u
                                if k < LATE - 1:
                                    z = q * z
                                    Z[k + 1, at] = z
                                    ZS.put(row + 8 * y, 8 * size, z.reshape(8 * size, 128))
                                else:
                                    WS.put(row + 8 * y, 8 * size, u.reshape(8 * size, 128))
                                for m in range(k + 1):
                                    accs[m] = accs[m] + jnp.sum(u * v[m], axis=0)
                                accs[k + 1] = accs[k + 1] + jnp.sum(u * u, axis=0)
                            return tuple(accs)
                        accs = all_planes(body, (zero8,) * (k + 2))
                        ACC[0:k + 2] = jnp.stack(accs)
                        halo_z(RU.at[b], z_recv.at[b]).wait_recv()
                        ghost_of_z(k + 1, es, b, q, slice(56, 120))
                    else:
                        wn2 = bc(tot, 32) * sw * sw
                        drop = jnp.sum(cf * (2.0 * h - gram_times(cf)), axis=0)
                        sub = jnp.sqrt(jnp.maximum(wn2 - drop, 0.0))
                        est = givens(k - 1, nrm * SW[k - 1])
                        RES[c] = jnp.where(lane8 == k, est, RES[c])
                        est = givens(k, sub)
                        RES[c] = jnp.where(lane8 == k + 1, est, RES[c])
                        g = [GV[i] for i in range(RESTART)]
                        for i in reversed(range(RESTART)):
                            y = g[i] / RM[i, i]
                            YY[i] = y * SW[i]
                            for m in range(i):
                                g[m] = g[m] - RM[m, i] * y

        yy = [YY[i] for i in range(RESTART)]

        def update(r, row, cy):
            x = v8(XS.get(row, 64))
            for m in range(RESTART):
                x = x + yy[m] * Z[m, pl.ds(r * 8, 8)]
            x = x.reshape(64, 128)
            XS.put(row, 64, x)
            MW[pl.ds(pl.multiple_of(r * 64, 8), 64), :] = x
            return cy
        all_planes(update, 0)

        @pl.when(c == 0)
        def _():
            inv = MISC[1]
            whole(SB, RB.at[RESTART - 1], h_send, h_recv.at[(RESTART - 1) % 3]).wait_recv()

            g = v8(GX[...])
            for m in range(RESTART):
                g = g + yy[m] * v8(GZ[m])
            GX[...] = g.reshape(GROWS, 128)
            for t in range(3):
                g = yy[0] * v8(RB[0, t])
                for m in range(1, RESTART):
                    g = g + yy[m] * v8(RB[m, t])
                GU[0, t] = (v8(GU[0, t]) - inv * g).reshape(GROWS, 128)

    cp = pltpu.make_async_copy(MW, out_hbm, l_sem.at[0, 0])
    cp.start()
    sync_all((CYCLES * RESTART) % 2).wait_send()
    rows = jnp.where(lax.broadcasted_iota(jnp.int32, (8, 128), 0) == 0, RES[0], RES[1]) * out_scale
    res_ref[...] = rows
    cp.wait()


def unpack(x_hbm, r_hbm, out_hbm, res_ref, xin, rin, out, in_sem, out_sem):
    parts = 3
    n = XL // parts
    loads = [[pltpu.make_async_copy(x_hbm.at[zl, pl.ds(t * n, n)], xin.at[zl, pl.ds(t * n, n)], in_sem.at[t, zl])
              for zl in range(2)] for t in range(parts)]
    stores = [[pltpu.make_async_copy(out.at[h, pl.ds(t * n, n)], out_hbm.at[h, pl.ds(t * n, n)], out_sem.at[t, h])
               for h in range(4)] for t in range(parts)]
    rows = pltpu.make_async_copy(r_hbm, rin, in_sem.at[parts, 0])
    for cp in [c for t in loads for c in t] + [rows]:
        cp.start()
    a = lax.broadcasted_iota(jnp.int32, (256, 256), 0)
    d = lax.broadcasted_iota(jnp.int32, (256, 256), 1)
    a0 = a - jnp.where(a >= 128, 128, 0)
    h = jnp.where(a0 >= 96, 3, jnp.where(a0 >= 64, 2, jnp.where(a0 >= 32, 1, 0)))
    m = jnp.where(d == 64 * h + 2 * (a0 - 32 * h) + jnp.where(a >= 128, 1, 0), 1.0, 0.0).astype(jnp.bfloat16)
    for t in range(parts):
        for cp in loads[t]:
            cp.wait()
        for i in range(t * n, t * n + n, 2):
            v = jnp.concatenate([jnp.concatenate([xin[0, x], xin[1, x]], axis=1) for x in (i, i + 1)], axis=0)
            o = rearrange(v, m)
            for x in range(2):
                for h in range(4):
                    out[h, i + x] = o[64 * x:64 * x + 64, 64 * h:64 * h + 64]
        for cp in stores[t]:
            cp.start()
    rows.wait()
    res_ref[...] = rin[0:CYCLES, 0:RESTART + 1]
    for cp in [c for t in stores for c in t]:
        cp.wait()


def solution(mesh):
    grid_spec = P(('sys', 'gx'), 'gy', 'gz')
    vel_spec = P(None, ('sys', 'gx'), 'gy', 'gz')
    table_spec = P('sys', None)
    f32 = jnp.float32

    def local_solve(source, initial, velocity, damping):
        big = (SETR, 128)
        vol, flat = (NP * 8, 8, 128), (NP * 64, 128)
        v = lambda *s: pltpu.VMEM(s, f32)
        n = RESTART
        scratch = [
            v(n, *vol), v(LATE - 1, *vol), v(LATE - 1, *vol), v(LATE - 1, *vol), v(n, *vol),
            v(*big), v(*big), v(*big), v(2, *big), v(2, *big), v(*flat),
            v(*flat), v(*flat), v(*flat), v(*flat), v(*flat), v(*flat), v(128, 128), v(NP, 128), v(NP, 128),
            v(n - 1, 3, GROWS, 128), v(n - 1, GROWS, 128), v(n + 3, 3, GROWS, 128), v(2, GROWS, 128),
            v(3, GROWS, 128), v(GROWS, 128), v(n, GROWS, 128), v(GROWS, 128), v(64, 128),
            v(2, 8, 128), v(n + 1, 8, 128), v(n, n, 8, 128), v(n, n, 8, 128),
            v(n, 8, 128), v(n, 8, 128), v(n, 8, 128), v(n, 8, 128), v(n, 8, 128), v(n, 8, 128), v(n + 1, 8, 128), v(n, 8, 128), v(n, 8, 128),
            v(CYCLES, 8, 128), v(8, 8, 128), v(4, 48, 64, 64), pltpu.VMEM((256, 256), jnp.bfloat16),
            pltpu.SemaphoreType.DMA((2,)), pltpu.SemaphoreType.DMA((2,)), pltpu.SemaphoreType.DMA,
            pltpu.SemaphoreType.DMA((3,)), pltpu.SemaphoreType.DMA, pltpu.SemaphoreType.DMA((2,)),
            pltpu.SemaphoreType.DMA, pltpu.SemaphoreType.DMA((2,)), pltpu.SemaphoreType.DMA, pltpu.SemaphoreType.DMA((5, 4)),
        ]
        hbm = pl.BlockSpec(memory_space=pl.ANY)
        packed, rows = pl.pallas_call(
            kernel,
            out_shape=(jax.ShapeDtypeStruct(flat, f32), jax.ShapeDtypeStruct((8, 128), f32)),
            in_specs=[hbm, hbm, hbm, pl.BlockSpec(memory_space=pltpu.SMEM)],
            out_specs=(hbm, pl.BlockSpec(memory_space=pltpu.VMEM)),
            scratch_shapes=scratch,
            compiler_params=pltpu.CompilerParams(
                collective_id=0, has_side_effects=True, vmem_limit_bytes=67043328),
            name='fgmres',
        )(source, initial, velocity, damping)
        out, res = pl.pallas_call(
            unpack,
            out_shape=(jax.ShapeDtypeStruct((4, XL, 64, 64), f32), jax.ShapeDtypeStruct((CYCLES, n + 1), f32)),
            in_specs=[hbm, hbm],
            out_specs=(hbm, pl.BlockSpec(memory_space=pltpu.VMEM)),
            scratch_shapes=[v(2, XL, 64, 128), v(8, 128), v(4, XL, 64, 64),
                            pltpu.SemaphoreType.DMA((4, 2)), pltpu.SemaphoreType.DMA((3, 4))],
            name='unpack',
        )(packed.reshape(2, XL, 64, 128), rows)
        return out.reshape(source.shape), res

    return jax.shard_map(local_solve, mesh=mesh, in_specs=(grid_spec, grid_spec, vel_spec, table_spec),
                         out_specs=(grid_spec, table_spec), check_vma=False)
```

```python
import math
import jax
import jax.numpy as jnp
from jax import lax
from jax.experimental import pallas as pl
from jax.experimental.pallas import tpu as pltpu
from jax.sharding import PartitionSpec as P

MESH = pl.DeviceIdType.MESH
RESTART = 10
CYCLES = 2
XL = 12
NP = 2 * XL
PZ = XL + 2
LO, HI, ROWS = 8, 72, 80
SETR = 2 * PZ * ROWS
LATE = 8
XG, YG, ZG = slice(0, 32), slice(32, 56), slice(56, 120)
GROWS = 120
DEALT = 2


def pairs(unroll, body, carry=()):
    if unroll == XL:
        for i in range(XL):
            carry = body(i, carry)
        return carry

    def trip(t, carry):
        for i in range(unroll):
            carry = body(t * unroll + i, carry)
        return carry
    return lax.fori_loop(0, XL // unroll, trip, carry)


def v8(x):
    return x.reshape(-1, 8, 128)


class Set:
    def __init__(self, ref, t=None):
        self.ref, self.t = ref, t

    def index(self, start, size):
        rows = pl.ds(start, size) if not isinstance(start, int) else slice(start, start + size)
        return (rows, slice(None)) if self.t is None else (self.t, rows, slice(None))

    def get(self, start, size):
        return self.ref[self.index(start, size)]

    def put(self, start, size, v):
        self.ref[self.index(start, size)] = v

    def view(self, start, size):
        return self.ref.at[self.index(start, size)]


def row0(p):
    r = p * ROWS + LO
    return r if isinstance(r, int) else pl.multiple_of(r, 8)


def rearrange(v, m):
    f32 = jnp.float32
    a1 = v.astype(jnp.bfloat16)
    v = v - a1.astype(f32)
    a2 = v.astype(jnp.bfloat16)
    a3 = (v - a2.astype(f32)).astype(jnp.bfloat16)
    n = v.shape[0]
    o = jnp.dot(jnp.concatenate([a1, a2, a3], axis=0), m, preferred_element_type=f32)
    return (o[2 * n:] + o[n:2 * n]) + o[:n]


def all_planes(body, carry, step=1):
    def trip(t, carry):
        for zl in range(2):
            for i in range(step):
                x = t * step + i
                carry = body(x + zl * XL, row0(x + (zl * PZ + 1)), carry)
        return carry
    return lax.fori_loop(0, XL // step, trip, carry)


def kernel(src_hbm, ini_hbm, vel_hbm, damp_ref, out_ref, res_ref,
           U, NU, N2U, MU, Z, ZC, X, W, T1, T2, MW, SRC, CZP, CZM, HVX, HVY, CZA, CGX, CGY, YB,
           GU, GMU, RB, RU, SB, SU, GZ, GX, GX2, SS, ACC, GM, RM, SIG, EC, KAP, SW, CS, SN, GV, YY, NRM, RES, MISC, STG, DEAL,
           s_send, s_recv, h_send, h_recv, u_send, u_recv, z_send, z_recv, x_recv, l_sem):
    f32 = jnp.float32
    gx, gy, gz = lax.axis_index('gx'), lax.axis_index('gy'), lax.axis_index('gz')
    peers = {}
    for p in range(1, 8):
        a, b, c = p // 4, (p // 2) % 2, p % 2
        peers[p] = {'gx': 1 - gx if a else gx, 'gy': 1 - gy if b else gy, 'gz': 1 - gz if c else gz}
    side = {0: 4, 1: 2, 2: 1}

    def load(q, slot, h, src):
        return pltpu.make_async_copy(src.at[pl.ds(XL * h, XL)], STG.at[slot, pl.ds(XL * h, XL)], l_sem.at[q, h])

    def load_start(q, slot, src):
        for h in range(4):
            load(q, slot, h, src).start()
    load_start(0, 0, ini_hbm)
    bar = pltpu.get_barrier_semaphore()
    for p in range(1, 8):
        pl.semaphore_signal(bar, inc=1, device_id=peers[p], device_id_type=MESH)

    lane = lax.broadcasted_iota(jnp.int32, (64, 128), 1)
    lane8 = lane[0:8]
    left = lane < 64
    zh = jnp.where(left, jnp.where(lane < 32, lane, lane - 32), jnp.where(lane < 96, lane - 64, lane - 96))
    zh32 = zh[0:32]
    first_q, last_q = lane < 32, lane >= 96
    zero64 = jnp.zeros((64, 128), f32)
    zero8 = jnp.zeros((8, 128), f32)
    hi_x = (1 - gx).astype(f32)
    l0 = 31 * (1 - gz)
    o_x = 96 * (1 - gx)
    y_send = 63 * (1 - gy)
    y_pad = HI - 65 * gy
    edge_lo = zh32 == 32 * (1 - gz)
    edge_hi = zh32 == 31 + 32 * gz
    WS, ZS, XS = Set(W), Set(ZC), Set(X)

    def seams(V, ghost=None):
        for zl in range(2):
            b = zl * PZ
            a = pltpu.roll(V.get(row0(b + XL), 64), 32, 1)
            d = pltpu.roll(V.get(row0(b + 1), 64), 96, 1)
            lo = 0.0 if ghost is None else ghost[zl] * (1.0 - hi_x)
            hi = 0.0 if ghost is None else ghost[zl] * hi_x
            V.put(row0(b), 64, jnp.where(first_q, lo, a))
            V.put(row0(b + XL + 1), 64, jnp.where(last_q, hi, d))

    def neighbours(V, i, put, ghost=None):
        size = 64 if ghost is None else 32
        for y in range(0, 64, size):
            co = lambda C, r: C[r * 64 + y:r * 64 + y + size, :]
            at = lambda q, d: V.get(row0(q) + y + d, size)
            u0, u1 = at(i + 1, 0), at(i + (PZ + 1), 0)
            below, above = pltpu.roll(u1, 1, 1), pltpu.roll(u0, 127, 1)
            if ghost is None:
                cm0, cp1 = co(CZM, i), co(CZP, i + XL)
            else:
                g = pltpu.roll(ghost[y:y + size, :], (l0 - i + 128) % 128, 1)
                below = jnp.where(edge_lo, g, below)
                above = jnp.where(edge_hi, g, above)
                cm0, cp1 = co(CZA, i), co(CZA, i + XL)
            for zl, u, n in ((0, u0, co(CZP, i) * u1 + cm0 * below), (1, u1, co(CZM, i + XL) * u0 + cp1 * above)):
                q, r = i + (zl * PZ + 1), i + zl * XL
                yp, ym = at(q, 1), at(q, -1)
                xp, xm = at(q + 1, 0), at(q - 1, 0)
                n = n + (xp + xm) - co(HVX, r) * (xp - xm)
                n = n + (yp + ym) - co(HVY, r) * (yp - ym)
                put(r * 8 + y // 8, row0(q) + y, size, u, n)

    def spread_x(rec):
        g = rec[XG, :]
        return [jnp.concatenate([pltpu.roll(g, (o_x - 64 * zl - 32 * yh + 128) % 128, 1) for yh in range(2)], axis=0)
                for zl in range(2)]

    def fill_ghosts(V, rec):
        seams(V, spread_x(rec))

        @pl.loop(0, 2)
        def _(zl):
            for i in range(XL):
                V.put((zl * PZ + (i + 1)) * ROWS + y_pad, 1, rec[pl.ds(zl * XL + (i + 32), 1), :])

    def add_ghosts_xy(rec):
        pd = (XL - 1) * (1 - gx)
        for zl, g in enumerate(spread_x(rec)):
            row = (pd + (zl * PZ + 1)) * ROWS + LO
            WS.put(row, 64, WS.get(row, 64) - CGX[64 * zl:64 * zl + 64, :] * g)
        YB[...] = CGY[...] * rec[YG, :]
        for r in range(NP):
            row = row0(r % XL + r // XL * PZ + 1) + y_send
            WS.put(row, 1, WS.get(row, 1) - YB[r:r + 1, :])

    def pack_xy(get, out):
        pd = (XL - 1) * (1 - gx)
        acc = zero64[0:32]
        for zl in range(2):
            for yh in range(2):
                slot = 2 * zl + yh
                r = pltpu.roll(get(zl, pd, 32 * yh, 32), (32 * slot - o_x + 128) % 128, 1)
                here = jnp.logical_and(lane[0:32] >= 32 * slot, lane[0:32] < 32 * slot + 32)
                acc = jnp.where(here, r, acc)
        out[XG, :] = acc

        for zl in range(2):
            for i in range(XL):
                r = 32 + zl * XL + i
                out[r:r + 1, :] = get(zl, i, y_send, 1)

    def pack_z(get, out):
        acc = zero64
        for i in range(XL):
            r = pltpu.roll(get(1 - gz, i, 0, 64), (i - l0 + 128) % 128, 1)
            acc = jnp.where(zh == i, r, acc)
        out[ZG, :] = acc

    def pack(get, out):
        pack_xy(get, out)
        pack_z(get, out)

    def of_set(V):
        return lambda zl, i, y, n: V.get((zl * PZ + i + 1) * ROWS + LO + y, n)

    def of_mw(zl, i, y, n):
        return MW[pl.ds((zl * XL + i) * 64 + y, n), :]

    def halo_start(src, dst, send, recv, axes=(0, 1, 2)):
        for ax in axes:
            rows = (XG, YG, ZG)[ax]
            pltpu.make_async_remote_copy(
                src_ref=src.at[rows, :], dst_ref=dst.at[rows, :], send_sem=send, recv_sem=recv,
                device_id=peers[side[ax]], device_id_type=MESH).start()

    def whole(src, dst, send, recv):
        return pltpu.make_async_remote_copy(src_ref=src, dst_ref=dst, send_sem=send, recv_sem=recv,
                                            device_id=peers[1], device_id_type=MESH)

    def three_at_once(b, dst, recv, recv_z=None):
        sets = (WS, Set(T1, b), Set(T2, b))
        for q, t in enumerate(sets):
            pack_xy(of_set(t), SB.at[q])
        for q, t in enumerate(sets):
            pack_z(of_set(t), SB.at[q])
        for q in range(3):
            halo_start(SB.at[q], dst.at[q], h_send, recv, (0, 1))
            halo_start(SB.at[q], dst.at[q], h_send, recv if recv_z is None else recv_z, (2,))

    def sync_all(par):
        return pltpu.make_async_remote_copy(
            src_ref=SS.at[par, pl.ds(1, 7), :], dst_ref=SS.at[par, pl.ds(1, 7), :],
            send_sem=s_send.at[par], recv_sem=s_recv.at[par], device_id=peers[1], device_id_type=MESH)

    def sync_start(par, items):
        row = zero8
        for idx, acc in items:
            row = jnp.where(lane8 == idx, jnp.sum(acc, axis=1, keepdims=True), row)
        row = row + pltpu.roll(row, 4, 0)
        row = row + pltpu.roll(row, 2, 0)
        row = row + pltpu.roll(row, 1, 0)
        SS[par, 0:1, :] = row[0:1]
        for p in (6, 7, 5, 3, 4, 2, 1):
            pltpu.make_async_remote_copy(
                src_ref=SS.at[par, pl.ds(0, 1), :], dst_ref=SS.at[par, pl.ds(p, 1), :],
                send_sem=s_send.at[par], recv_sem=s_recv.at[par],
                device_id=peers[p], device_id_type=MESH).start()

    def sync_wait(par):
        sync_all(par).wait_recv()
        tot = SS[par]
        tot = tot + pltpu.roll(tot, 4, 0)
        tot = tot + pltpu.roll(tot, 2, 0)
        return tot + pltpu.roll(tot, 1, 0)

    def bc(tot, k):
        return jnp.broadcast_to(tot[:, k:k + 1], (8, 128))

    def fold(x):
        return jnp.sum(v8(x), axis=0)

    def poly(c, j):
        s = damp_ref[c, j] / 6.0
        a0, a1, a2 = 3.0 * s, 3.0 * s * s, s * s * s
        q = jnp.full((8, 128), a0 - 6.0 * a1 + 36.0 * a2, f32)
        return q, (a1 - 12.0 * a2) / q, a2 / q

    @pl.loop(0, 2 * PZ)
    def _(p):
        for V in (ZS, XS, WS, Set(T1, 0), Set(T1, 1)):
            V.put(pl.multiple_of(p * ROWS, 8), 8, zero8)
            V.put(pl.multiple_of(p * ROWS + HI, 8), 8, zero8)

    a = lax.broadcasted_iota(jnp.int32, (256, 256), 0)
    d = lax.broadcasted_iota(jnp.int32, (256, 256), 1)
    d0 = d - jnp.where(d >= 128, 128, 0)
    h = jnp.where(d0 >= 96, 3, jnp.where(d0 >= 64, 2, jnp.where(d0 >= 32, 1, 0)))
    target = 64 * h + 2 * (d0 - 32 * h) + jnp.where(d >= 128, 1, 0)
    DEAL[...] = jnp.where(a == target, 1.0, 0.0).astype(jnp.bfloat16)

    @pl.loop(0, 5)
    def _(q):
        for h in range(4):
            load(q, q % 4, h, ini_hbm).wait()

        @pl.when(q == 0)
        def _():
            for d in range(3):
                load_start(1 + d, 1 + d, vel_hbm.at[d])
        m = DEAL[...]
        for i in range(0, XL, DEALT):
            v = jnp.concatenate([jnp.concatenate([STG[q % 4, h * XL + x] for h in range(4)], axis=1)
                                 for x in range(i, i + DEALT)], axis=0)
            o = rearrange(v, m)
            o = v8(o[:, 0:128]), v8(o[:, 128:256])
            for zl in range(2):
                U[q, (i + zl * XL) * 8:(i + DEALT + zl * XL) * 8] = o[zl]

        @pl.when(q == 0)
        def _():
            load_start(4, 0, src_hbm)

            def take_x(r, row, c):
                XS.put(row, 64, U[0, pl.ds(r * 8, 8)].reshape(64, 128))
                return c
            all_planes(take_x, 0)
            pack(of_set(XS), SU)
            pl.semaphore_wait(bar, 7)
            halo_start(SU, GX, u_send, x_recv)

    @pl.loop(0, XL)
    def _(i):
        at = lambda q, r: U[q, pl.ds(r * 8, 8)].reshape(64, 128)
        low = pl.ds(pl.multiple_of(i * 64, 8), 64)
        high = pl.ds(pl.multiple_of((i + XL) * 64, 8), 64)
        for rows, r in ((low, i), (high, i + XL)):
            HVX[rows, :] = 0.5 * at(1, r)
            HVY[rows, :] = 0.5 * at(2, r)
            SRC[rows, :] = at(4, r)
        h0, h1 = at(3, i), at(3, i + XL)
        cm0, cp1 = 1.0 + 0.5 * h0, 1.0 - 0.5 * h1
        CZP[low, :] = 1.0 - 0.5 * h0
        CZM[low, :] = jnp.where(zh == 0, 0.0, cm0)
        CZA[low, :] = jnp.where(zh == 32 * gz, 0.0, cm0)
        CZM[high, :] = 1.0 + 0.5 * h1
        CZP[high, :] = jnp.where(zh == 31, 0.0, cp1)
        CZA[high, :] = jnp.where(zh == 63 - 32 * gz, 0.0, cp1)

    pd = (XL - 1) * (1 - gx)
    at_x = jnp.logical_and(lane >= o_x, lane < o_x + 32)
    sign_x, sign_y = (2 * gx - 1).astype(f32), (2 * gy - 1).astype(f32)
    for zl in range(2):
        hv = HVX[pl.ds(pl.multiple_of((zl * XL + pd) * 64, 8), 64), :]
        CGX[64 * zl:64 * zl + 64, :] = jnp.where(at_x, 1.0 + sign_x * hv, 0.0)

    @pl.loop(0, NP)
    def _(r):
        CGY[pl.ds(r, 1), :] = 1.0 + sign_y * HVY[pl.ds(r * 64 + y_send, 1), :]
    whole(SU, GX, u_send, x_recv).wait()

    def halo_xy(dst, recv):
        return whole(SU.at[pl.ds(0, 56), :], dst.at[pl.ds(0, 56), :], u_send, recv)

    def halo_z(dst, recv):
        return whole(SU.at[pl.ds(56, 64), :], dst.at[pl.ds(56, 64), :], z_send, recv)

    def ghost_of_z(k, e, b, q, rows):
        g = v8(RU[b, rows, :])
        for i in range(k):
            g = g - e[i] * v8(GMU[i, rows, :])
        GZ[k, rows, :] = (q * g).reshape(-1, 128)

    def first_ghosts(rows, scale, q, r1, r2):
        g = [v8(GU[0, t, rows, :]) for t in range(3)]
        if scale is not None:
            g = [t * scale for t in g]
            for t in range(3):
                GU[0, t, rows, :] = g[t].reshape(-1, 128)
        GZ[0, rows, :] = (q * (g[0] + r1 * g[1] + r2 * g[2])).reshape(-1, 128)

    def sweep(V, unroll, put, ghost=None):
        def one(i, c):
            neighbours(V, i, put, ghost)
            return c
        pairs(unroll, one)

    def to_n(V):
        def put(r8, row, size, u, n):
            V.put(row, size, n)
        return put

    def givens(m, sub):
        h = [RM[i, m] for i in range(m + 1)]
        for i in range(m):
            cs, sn = CS[i], SN[i]
            h[i], h[i + 1] = cs * h[i] + sn * h[i + 1], cs * h[i + 1] - sn * h[i]
        d = h[m]
        rad = jnp.sqrt(d * d + sub * sub)
        cs, sn = d / rad, sub / rad
        CS[m] = cs
        SN[m] = sn
        h[m] = cs * d + sn * sub
        RM[0:m + 1, m] = jnp.stack(h)
        g = GV[m]
        GV[m] = cs * g
        GV[m + 1] = -sn * g
        est = MISC[4] * jnp.abs(sn)
        MISC[4] = est
        return est

    out_scale = 1.0 / math.sqrt(1572864.0)
    last_halo = CYCLES * RESTART - 3

    @pl.loop(0, CYCLES)
    def _(c):
        fill_ghosts(XS, GX)

        def put_r(r8, row, size, u, n):
            WS.put(row, size, SRC[r8 * 8:r8 * 8 + size, :] - (6.0 * u - n))
        sweep(XS, XL, put_r, GX.at[ZG, :])

        @pl.when(c == 0)
        def _():
            def one(r, row, acc):
                t = v8(WS.get(row, 64)).reshape(2, 4, 8, 128)
                return acc + jnp.sum(t * t, axis=0)
            acc = all_planes(one, jnp.zeros((4, 8, 128), f32), 2)
            sync_start(0, [(16, jnp.sum(acc, axis=0))])

        @pl.loop(0, RESTART)
        def _(j):
            step = c * RESTART + j
            par = (step + 1) % 2
            b = step % 2
            nxt = (j + 1) % RESTART
            slot = c * RESTART + (1 - c) * j + c * (j % 3)

            @pl.when(j * (j - LATE) >= 0)
            def _():
                seams(WS)
                sweep(WS, XL, to_n(Set(T1, 0)))
                seams(Set(T1, 0))

            @pl.when(j >= LATE)
            def _():
                q, r1, r2 = poly(c, j)
                q, r1, r2 = (jnp.concatenate([t] * 8, axis=0) for t in (q * KAP[j], r1, r2))

                def put_z(r8, row, size, u, n):
                    z = q * (WS.get(row, size) + r1 * u + r2 * n)
                    ZS.put(row, size, z)
                    Z[j, r8:r8 + size // 8] = v8(z)
                sweep(Set(T1, 0), XL, put_z)

            @pl.when(j == 0)
            def _():
                sweep(Set(T1, 0), XL, to_n(Set(T2, 0)))

                @pl.when(c == 0)
                def _():
                    three_at_once(0, GU.at[0], h_recv.at[1], z_recv.at[1])
                    tot = sync_wait(0)
                    sync_all(0).wait_send()
                    beta0 = jnp.sqrt(bc(tot, 16))
                    MISC[0] = beta0
                    MISC[1] = 1.0 / beta0

                inv0 = MISC[1]
                KAP[0] = jnp.ones((8, 128), f32)
                q, r1, r2 = poly(c, 0)

                def start(r, row, acc):
                    u, n, n2 = (v8(t.get(row, 64)) * inv0 for t in (WS, Set(T1, 0), Set(T2, 0)))
                    z = q * (u + r1 * n + r2 * n2)
                    acc = acc + jnp.sum((u * u).reshape(2, 4, 8, 128), axis=0)
                    at = pl.ds(r * 8, 8)
                    U[0, at] = u
                    NU[0, at] = n
                    N2U[0, at] = n2
                    Z[0, at] = z
                    ZS.put(row, 64, z.reshape(64, 128))
                    return acc
                ACC[0] = jnp.sum(all_planes(start, jnp.zeros((4, 8, 128), f32)), axis=0)

                @pl.when(c == 0)
                def _():
                    whole(SB.at[:, pl.ds(56, 64), :], GU.at[0, :, pl.ds(56, 64), :], h_send, z_recv.at[1]).wait_recv()
                    first_ghosts(slice(56, 120), inv0, q, r1, r2)

                @pl.when(c > 0)
                def _():
                    first_ghosts(slice(0, 120), None, q, r1, r2)

            seams(ZS)
            GX2[...] = GZ[j, ZG, :]

            def put_w(r8, row, size, u, n):
                WS.put(row, size, 6.0 * u - n)
            sweep(ZS, XL, put_w, GX2)

            for k in range(1, RESTART):
                @pl.when(j == k)
                def _():
                    halo_xy(RU.at[1 - b], u_recv.at[1 - b]).wait_recv()
                    ghost_of_z(k, [EC[i] for i in range(k)], 1 - b, KAP[k] * poly(c, k)[0], slice(0, 56))

            @pl.when(step == 0)
            def _():
                whole(SB.at[:, pl.ds(0, 56), :], GU.at[0, :, pl.ds(0, 56), :], h_send, h_recv.at[1]).wait_recv()
                whole(SB, GU.at[0], h_send, h_recv.at[1]).wait_send()
                first_ghosts(slice(0, 56), MISC[1], *poly(c, 0))
            add_ghosts_xy(GZ.at[j])

            for k in range(RESTART):
                @pl.when(j == k)
                def _():
                    ends = k == 0 or k == RESTART - 1
                    wd = 4 if k < 4 else 2 if k < 8 else 1
                    count = k + 2 if ends else k + 1

                    def dots(t, accs):
                        accs = list(accs)
                        for zl in range(2):
                            x = t * 2 + zl * XL
                            w = jnp.concatenate([v8(WS.get(row0(t * 2 + (zl * PZ + 1 + i)), 64)) for i in range(2)])
                            w = w.reshape(16 // wd, wd, 8, 128)
                            for i in range(k + 1):
                                v = U[i, pl.ds(x * 8, 16)].reshape(16 // wd, wd, 8, 128)
                                accs[i] = accs[i] + jnp.sum(v * w, axis=0)
                            if ends:
                                accs[k + 1] = accs[k + 1] + jnp.sum(w * w, axis=0)
                        return tuple(accs)
                    accs = lax.fori_loop(0, XL // 2, dots, (jnp.zeros((wd, 8, 128), f32),) * count)
                    accs = [jnp.sum(a, axis=0) for a in accs]
                    items = [(i, accs[i]) for i in range(k + 1)] + [(16 + i, ACC[i]) for i in range(k + 1)]
                    if ends:
                        items.append((32, accs[k + 1]))
                    sync_start(par, items)

            @pl.when(step > 0)
            def _():
                sync_all(1 - par).wait_send()

            @pl.when(step < CYCLES * RESTART - 1)
            def _():
                seams(WS)
                sweep(WS, XL, to_n(Set(T1, b)))

            @pl.when(CYCLES * RESTART - 1 - step > 0)
            def _():
                seams(Set(T1, b))
                r1, r2 = (jnp.concatenate([t] * 8, axis=0) for t in poly(c, nxt)[1:])

                def put(r8, row, size, u, n):
                    Set(T2, b).put(row, size, n)
                    MW[r8 * 8:r8 * 8 + size, :] = WS.get(row, size) + r1 * u + r2 * n
                sweep(Set(T1, b), XL, put)

            @pl.when(j > 0)
            def _():
                halo_xy(RU.at[b], u_recv.at[b]).wait_send()
                halo_z(RU.at[b], z_recv.at[b]).wait_send()

            @pl.when(j < RESTART - 1)
            def _():
                pack_xy(of_mw, SU)
                halo_start(SU, RU.at[b], u_send, u_recv.at[b], (0, 1))
                pack_z(of_mw, SU)
                halo_start(SU, RU.at[b], z_send, z_recv.at[b], (2,))

            @pl.when(step <= last_halo + 1)
            def _():
                @pl.when(step > 0)
                def _():
                    whole(SB, RB.at[slot], h_send, h_recv.at[0]).wait_send()

                @pl.when(step <= last_halo)
                def _():
                    three_at_once(b, RB.at[slot], h_recv.at[step % 3])

                @pl.when(j > 0)
                def _():
                    whole(SB, RB.at[slot], h_send, h_recv.at[(step + 2) % 3]).wait_recv()

            prev = c * RESTART + (1 - c) * (j - 1) + c * ((j + 2) % 3)
            for k in range(RESTART):
                @pl.when(j == k)
                def _():
                    if k < RESTART - 1:
                        q, r1, r2 = poly(c, k + 1)
                        e = [EC[i] for i in range(k)]

                        size = 8 if k < 4 else 2

                        def body(r, row, cy):
                            for y in range(0, 8, size):
                                at = pl.ds(r * 8 + y, size)
                                if k:
                                    n = v8(Set(T1, 1 - b).get(row + 8 * y, 8 * size))
                                    n2 = v8(Set(T2, 1 - b).get(row + 8 * y, 8 * size))
                                    for m in range(k):
                                        nm, n2m = NU[m, at], N2U[m, at]
                                        n = n - e[m] * nm
                                        n2 = n2 - e[m] * n2m
                                        MU[m, at] = U[m, at] + r1 * nm + r2 * n2m
                                    NU[k, at] = n
                                    N2U[k, at] = n2
                                else:
                                    n, n2 = NU[0, at], N2U[0, at]
                                MU[k, at] = U[k, at] + r1 * n + r2 * n2
                            return cy
                        if k < LATE - 1:
                            all_planes(body, 0)

                        if k:
                            for t in range(3):
                                g = v8(RB[prev, t])
                                for i in range(k):
                                    g = g - e[i] * v8(GU[i, t])
                                GU[k, t] = g.reshape(GROWS, 128)

                        @pl.loop(0, k + 1)
                        def _(i):
                            g = v8(GU[i, 0]) + r1 * v8(GU[i, 1]) + r2 * v8(GU[i, 2])
                            GMU[i] = g.reshape(GROWS, 128)
                    if k >= 2:
                        est = givens(k - 2, NRM[k - 1] * SW[k - 2])
                        RES[c] = jnp.where(lane8 == k - 1, est, RES[c])

            tot = sync_wait(par)

            for k in range(RESTART):
                @pl.when(j == k)
                def _():
                    nn = bc(tot, 16 + k)
                    nrm = jnp.sqrt(nn)
                    sg = 1.0 / nrm
                    SIG[k] = sg
                    NRM[k] = nrm
                    kap = KAP[k]
                    sw = sg / kap
                    SW[k] = sw
                    sig = SIG[0:k + 1]
                    h = jnp.stack([bc(tot, i) for i in range(k + 1)]) * (sig * sw)
                    gcol = jnp.stack([bc(tot, 16 + i) for i in range(k + 1)]) * (sig * sg)
                    GM[k, 0:k + 1] = gcol
                    if k > 0:
                        GM[0:k, k] = gcol[0:k]

                    def gram_times(x):
                        out = gcol * x[k]
                        for m in range(k):
                            out = out + GM[m, 0:k + 1] * x[m]
                        return out
                    cf = 2.0 * h - gram_times(h)
                    RM[0:k + 1, k] = cf
                    if k == 0:
                        beta = MISC[0] * nrm
                        MISC[4] = beta
                        GV[0] = beta
                        RES[c] = jnp.where(lane8 == 0, beta, 0.0)
                        wn = jnp.sqrt(bc(tot, 32)) * sw
                        rho = 1.0 / wn
                        MISC[2] = rho
                    else:
                        rho = MISC[2]
                    if k < RESTART - 1:
                        es = cf * (sig * (kap * nrm))
                        EC[0:k + 1] = es
                        KAP[k + 1] = rho * sg
                        q = (rho * sg) * poly(c, k + 1)[0]

                        size = 8 if k < 2 else 4 if k < 5 else 2

                        def body(r, row, accs):
                            accs = list(accs)
                            for y in range(0, 8, size):
                                at = pl.ds(r * 8 + y, size)
                                v = [U[m, at] for m in range(k + 1)]
                                u = v8(WS.get(row + 8 * y, 8 * size))
                                if k < LATE - 1:
                                    z = v8(MW[pl.ds(pl.multiple_of(r * 64 + 8 * y, 8), 8 * size), :])
                                for m in range(k + 1):
                                    u = u - es[m] * v[m]
                                    if k < LATE - 1:
                                        z = z - es[m] * MU[m, at]
                                U[k + 1, at] = u
                                if k < LATE - 1:
                                    z = q * z
                                    Z[k + 1, at] = z
                                    ZS.put(row + 8 * y, 8 * size, z.reshape(8 * size, 128))
                                else:
                                    WS.put(row + 8 * y, 8 * size, u.reshape(8 * size, 128))
                                for m in range(k + 1):
                                    accs[m] = accs[m] + jnp.sum(u * v[m], axis=0)
                                accs[k + 1] = accs[k + 1] + jnp.sum(u * u, axis=0)
                            return tuple(accs)
                        accs = all_planes(body, (zero8,) * (k + 2))
                        ACC[0:k + 2] = jnp.stack(accs)
                        halo_z(RU.at[b], z_recv.at[b]).wait_recv()
                        ghost_of_z(k + 1, es, b, q, slice(56, 120))
                    else:
                        wn2 = bc(tot, 32) * sw * sw
                        drop = jnp.sum(cf * (2.0 * h - gram_times(cf)), axis=0)
                        sub = jnp.sqrt(jnp.maximum(wn2 - drop, 0.0))
                        est = givens(k - 1, nrm * SW[k - 1])
                        RES[c] = jnp.where(lane8 == k, est, RES[c])
                        est = givens(k, sub)
                        RES[c] = jnp.where(lane8 == k + 1, est, RES[c])
                        g = [GV[i] for i in range(RESTART)]
                        for i in reversed(range(RESTART)):
                            y = g[i] / RM[i, i]
                            YY[i] = y * SW[i]
                            for m in range(i):
                                g[m] = g[m] - RM[m, i] * y

        yy = [YY[i] for i in range(RESTART)]

        def update(r, row, cy):
            x = v8(XS.get(row, 64))
            for m in range(RESTART):
                x = x + yy[m] * Z[m, pl.ds(r * 8, 8)]
            x = x.reshape(64, 128)
            XS.put(row, 64, x)
            out_ref[pl.ds(pl.multiple_of(r * 64, 8), 64), :] = x
            return cy
        all_planes(update, 0)

        @pl.when(c == 0)
        def _():
            inv = MISC[1]
            whole(SB, RB.at[RESTART - 1], h_send, h_recv.at[(RESTART - 1) % 3]).wait_recv()

            g = v8(GX[...])
            for m in range(RESTART):
                g = g + yy[m] * v8(GZ[m])
            GX[...] = g.reshape(GROWS, 128)
            for t in range(3):
                g = yy[0] * v8(RB[0, t])
                for m in range(1, RESTART):
                    g = g + yy[m] * v8(RB[m, t])
                GU[0, t] = (v8(GU[0, t]) - inv * g).reshape(GROWS, 128)

    sync_all((CYCLES * RESTART) % 2).wait_send()
    rows = jnp.where(lax.broadcasted_iota(jnp.int32, (8, 128), 0) == 0, RES[0], RES[1]) * out_scale
    res_ref[...] = rows


def unpack(x_ref, r_ref, out_hbm, res_ref, out, out_sem):
    a = lax.broadcasted_iota(jnp.int32, (256, 256), 0)
    d = lax.broadcasted_iota(jnp.int32, (256, 256), 1)
    a0 = a - jnp.where(a >= 128, 128, 0)
    h = jnp.where(a0 >= 96, 3, jnp.where(a0 >= 64, 2, jnp.where(a0 >= 32, 1, 0)))
    m = jnp.where(d == 64 * h + 2 * (a0 - 32 * h) + jnp.where(a >= 128, 1, 0), 1.0, 0.0).astype(jnp.bfloat16)
    stores = []
    for i in range(0, XL, 2):
        v = jnp.concatenate([jnp.concatenate([x_ref[64 * x:64 * x + 64, :], x_ref[64 * (x + XL):64 * (x + XL) + 64, :]],
                                             axis=1) for x in (i, i + 1)], axis=0)
        o = rearrange(v, m)
        for x in range(2):
            for h in range(4):
                out[h, i + x] = o[64 * x:64 * x + 64, 64 * h:64 * h + 64]
        for h in range(4):
            stores.append(pltpu.make_async_copy(out.at[h, pl.ds(i, 2)], out_hbm.at[h, pl.ds(i, 2)], out_sem.at[i // 2, h]))
            stores[-1].start()
    res_ref[...] = r_ref[0:CYCLES, 0:RESTART + 1]
    for cp in stores:
        cp.wait()


def solution(mesh):
    grid_spec = P(('sys', 'gx'), 'gy', 'gz')
    vel_spec = P(None, ('sys', 'gx'), 'gy', 'gz')
    table_spec = P('sys', None)
    f32 = jnp.float32

    def local_solve(source, initial, velocity, damping):
        big = (SETR, 128)
        vol, flat = (NP * 8, 8, 128), (NP * 64, 128)
        v = lambda *s: pltpu.VMEM(s, f32)
        n = RESTART
        scratch = [
            v(n, *vol), v(LATE - 1, *vol), v(LATE - 1, *vol), v(LATE - 1, *vol), v(n, *vol),
            v(*big), v(*big), v(*big), v(2, *big), v(2, *big), v(*flat),
            v(*flat), v(*flat), v(*flat), v(*flat), v(*flat), v(*flat), v(128, 128), v(NP, 128), v(NP, 128),
            v(n - 1, 3, GROWS, 128), v(n - 1, GROWS, 128), v(n + 3, 3, GROWS, 128), v(2, GROWS, 128),
            v(3, GROWS, 128), v(GROWS, 128), v(n, GROWS, 128), v(GROWS, 128), v(64, 128),
            v(2, 8, 128), v(n + 1, 8, 128), v(n, n, 8, 128), v(n, n, 8, 128),
            v(n, 8, 128), v(n, 8, 128), v(n, 8, 128), v(n, 8, 128), v(n, 8, 128), v(n, 8, 128), v(n + 1, 8, 128), v(n, 8, 128), v(n, 8, 128),
            v(CYCLES, 8, 128), v(8, 8, 128), v(4, 48, 64, 64), pltpu.VMEM((256, 256), jnp.bfloat16),
            pltpu.SemaphoreType.DMA((2,)), pltpu.SemaphoreType.DMA((2,)), pltpu.SemaphoreType.DMA,
            pltpu.SemaphoreType.DMA((3,)), pltpu.SemaphoreType.DMA, pltpu.SemaphoreType.DMA((2,)),
            pltpu.SemaphoreType.DMA, pltpu.SemaphoreType.DMA((2,)), pltpu.SemaphoreType.DMA, pltpu.SemaphoreType.DMA((5, 4)),
        ]
        hbm = pl.BlockSpec(memory_space=pl.ANY)
        vm = pl.BlockSpec(memory_space=pltpu.VMEM)
        packed, rows = pl.pallas_call(
            kernel,
            out_shape=(pltpu.VMEM(flat, f32), pltpu.VMEM((8, 128), f32)),
            in_specs=[hbm, hbm, hbm, pl.BlockSpec(memory_space=pltpu.SMEM)],
            out_specs=(vm, vm),
            scratch_shapes=scratch,
            compiler_params=pltpu.CompilerParams(
                collective_id=0, has_side_effects=True, vmem_limit_bytes=60 * 2**20),
            name='fgmres',
        )(source, initial, velocity, damping)
        out, res = pl.pallas_call(
            unpack,
            out_shape=(jax.ShapeDtypeStruct((4, XL, 64, 64), f32), jax.ShapeDtypeStruct((CYCLES, n + 1), f32)),
            in_specs=[vm, vm],
            out_specs=(hbm, vm),
            scratch_shapes=[v(4, XL, 64, 64), pltpu.SemaphoreType.DMA((6, 4))],
            compiler_params=pltpu.CompilerParams(vmem_limit_bytes=16 * 2**20),
            name='unpack',
        )(packed, rows)
        return out.reshape(source.shape), res

    return jax.shard_map(local_solve, mesh=mesh, in_specs=(grid_spec, grid_spec, vel_spec, table_spec),
                         out_specs=(grid_spec, table_spec), check_vma=False)
```

```python
import math
import jax
import jax.numpy as jnp
from jax import lax
from jax.experimental import pallas as pl
from jax.experimental.pallas import tpu as pltpu
from jax.sharding import PartitionSpec as P

FLAT = pl.DeviceIdType.LOGICAL
RESTART = 10
CYCLES = 2
XL = 12
NP = 2 * XL
PZ = XL + 2
LO, HI, ROWS = 8, 72, 80
SETR = 2 * PZ * ROWS
LATE = 8
XG, YG, ZG = slice(0, 32), slice(32, 56), slice(56, 120)
GROWS = 120
DEALT = 2


def pairs(unroll, body, carry=()):
    if unroll == XL:
        for i in range(XL):
            carry = body(i, carry)
        return carry

    def trip(t, carry):
        for i in range(unroll):
            carry = body(t * unroll + i, carry)
        return carry
    return lax.fori_loop(0, XL // unroll, trip, carry)


def v8(x):
    return x.reshape(-1, 8, 128)


class Set:
    def __init__(self, ref, t=None):
        self.ref, self.t = ref, t

    def index(self, start, size):
        rows = pl.ds(start, size) if not isinstance(start, int) else slice(start, start + size)
        return (rows, slice(None)) if self.t is None else (self.t, rows, slice(None))

    def get(self, start, size):
        return self.ref[self.index(start, size)]

    def put(self, start, size, v):
        self.ref[self.index(start, size)] = v

    def view(self, start, size):
        return self.ref.at[self.index(start, size)]


def row0(p):
    r = p * ROWS + LO
    return r if isinstance(r, int) else pl.multiple_of(r, 8)


def rearrange(v, m):
    f32 = jnp.float32
    a1 = v.astype(jnp.bfloat16)
    v = v - a1.astype(f32)
    a2 = v.astype(jnp.bfloat16)
    a3 = (v - a2.astype(f32)).astype(jnp.bfloat16)
    n = v.shape[0]
    o = jnp.dot(jnp.concatenate([a1, a2, a3], axis=0), m, preferred_element_type=f32)
    return (o[2 * n:] + o[n:2 * n]) + o[:n]


def pick(j, lo, hi, fn):
    if hi - lo == 1:
        fn(lo)
    else:
        mid = (lo + hi) // 2
        lax.cond(j < mid, lambda: pick(j, lo, mid, fn), lambda: pick(j, mid, hi, fn))


def all_planes(body, carry, step=1):
    def trip(t, carry):
        for zl in range(2):
            for i in range(step):
                x = t * step + i
                carry = body(x + zl * XL, row0(x + (zl * PZ + 1)), carry)
        return carry
    return lax.fori_loop(0, XL // step, trip, carry)


def kernel(src_hbm, ini_hbm, vel_hbm, damp_ref, out_ref, res_ref,
           U, NU, N2U, MU, Z, ZC, X, W, T1, T2, MW, CO, CZP, CZM, CZA, CGX, CGY, YB,
           GU, GMU, RB, RU, SB, SU, GZ, GX, GX2, SS, ACC, GM, RM, SIG, EC, KAP, SW, CS, SN, GV, YY, NRM, RES, MISC, STG, DEAL,
           s_send, s_recv, h_send, h_recv, u_send, u_recv, z_send, z_recv, x_recv, l_sem):
    f32 = jnp.float32
    gx, gy, gz = lax.axis_index('gx'), lax.axis_index('gy'), lax.axis_index('gz')
    peers = {}
    for p in range(1, 8):
        a, b, c = p // 4, (p // 2) % 2, p % 2
        peers[p] = (1 - gx if a else gx) * 4 + (1 - gy if b else gy) * 2 + (1 - gz if c else gz)
    side = {0: 4, 1: 2, 2: 1}

    def load(q, slot, src):
        return pltpu.make_async_copy(src, STG.at[slot], l_sem.at[q])

    load(0, 0, ini_hbm).start()
    bar = pltpu.get_barrier_semaphore()
    for p in range(1, 8):
        pl.semaphore_signal(bar, inc=1, device_id=peers[p], device_id_type=FLAT)

    lane = lax.broadcasted_iota(jnp.int32, (64, 128), 1)
    lane8 = lane[0:8]
    left = lane < 64
    zh = jnp.where(left, jnp.where(lane < 32, lane, lane - 32), jnp.where(lane < 96, lane - 64, lane - 96))
    zh32 = zh[0:32]
    first_q, last_q = lane < 32, lane >= 96
    zero64 = jnp.zeros((64, 128), f32)
    zero8 = jnp.zeros((8, 128), f32)
    hi_x = (1 - gx).astype(f32)
    l0 = 31 * (1 - gz)
    o_x = 96 * (1 - gx)
    y_send = 63 * (1 - gy)
    y_pad = HI - 65 * gy
    edge_lo = zh32 == 32 * (1 - gz)
    edge_hi = zh32 == 31 + 32 * gz
    WS, ZS, XS = Set(W), Set(ZC), Set(X)

    def seams(V, ghost=None):
        for zl in range(2):
            b = zl * PZ
            a = pltpu.roll(V.get(row0(b + XL), 64), 32, 1)
            d = pltpu.roll(V.get(row0(b + 1), 64), 96, 1)
            lo = 0.0 if ghost is None else ghost[zl] * (1.0 - hi_x)
            hi = 0.0 if ghost is None else ghost[zl] * hi_x
            V.put(row0(b), 64, jnp.where(first_q, lo, a))
            V.put(row0(b + XL + 1), 64, jnp.where(last_q, hi, d))

    def neighbours(V, i, put, ghost=None):
        size = 64 if ghost is None else 32
        for y in range(0, 64, size):
            co = lambda C, r: C[r * 64 + y:r * 64 + y + size, :]
            hv = lambda d, r: CO[d, r * 64 + y:r * 64 + y + size, :]
            at = lambda q, d: V.get(row0(q) + y + d, size)
            u0, u1 = at(i + 1, 0), at(i + (PZ + 1), 0)
            below, above = pltpu.roll(u1, 1, 1), pltpu.roll(u0, 127, 1)
            if ghost is None:
                cm0, cp1 = co(CZM, i), co(CZP, i + XL)
            else:
                g = pltpu.roll(ghost[y:y + size, :], (l0 - i + 128) % 128, 1)
                below = jnp.where(edge_lo, g, below)
                above = jnp.where(edge_hi, g, above)
                cm0, cp1 = co(CZA, i), co(CZA, i + XL)
            for zl, u, n in ((0, u0, co(CZP, i) * u1 + cm0 * below), (1, u1, co(CZM, i + XL) * u0 + cp1 * above)):
                q, r = i + (zl * PZ + 1), i + zl * XL
                yp, ym = at(q, 1), at(q, -1)
                xp, xm = at(q + 1, 0), at(q - 1, 0)
                n = n + (xp + xm) - hv(1, r) * (xp - xm)
                n = n + (yp + ym) - hv(2, r) * (yp - ym)
                put(r * 8 + y // 8, row0(q) + y, size, u, n)

    def spread_x(rec):
        g = rec[XG, :]
        return [jnp.concatenate([pltpu.roll(g, (o_x - 64 * zl - 32 * yh + 128) % 128, 1) for yh in range(2)], axis=0)
                for zl in range(2)]

    def fill_ghosts(V, rec):
        seams(V, spread_x(rec))

        @pl.loop(0, 2)
        def _(zl):
            for i in range(XL):
                V.put((zl * PZ + (i + 1)) * ROWS + y_pad, 1, rec[pl.ds(zl * XL + (i + 32), 1), :])

    def add_ghosts_xy(rec):
        pd = (XL - 1) * (1 - gx)
        for zl, g in enumerate(spread_x(rec)):
            row = (pd + (zl * PZ + 1)) * ROWS + LO
            WS.put(row, 64, WS.get(row, 64) - CGX[64 * zl:64 * zl + 64, :] * g)
        YB[...] = CGY[...] * rec[YG, :]
        for r in range(NP):
            row = row0(r % XL + r // XL * PZ + 1) + y_send
            WS.put(row, 1, WS.get(row, 1) - YB[r:r + 1, :])

    def pack_xy(get, out):
        pd = (XL - 1) * (1 - gx)
        acc = zero64[0:32]
        for zl in range(2):
            for yh in range(2):
                slot = 2 * zl + yh
                r = pltpu.roll(get(zl, pd, 32 * yh, 32), (32 * slot - o_x + 128) % 128, 1)
                here = jnp.logical_and(lane[0:32] >= 32 * slot, lane[0:32] < 32 * slot + 32)
                acc = jnp.where(here, r, acc)
        out[XG, :] = acc

        for zl in range(2):
            for i in range(XL):
                r = 32 + zl * XL + i
                out[r:r + 1, :] = get(zl, i, y_send, 1)

    def pack_z(get, out):
        acc = zero64
        for i in range(XL):
            r = pltpu.roll(get(1 - gz, i, 0, 64), (i - l0 + 128) % 128, 1)
            acc = jnp.where(zh == i, r, acc)
        out[ZG, :] = acc

    def pack(get, out):
        pack_xy(get, out)
        pack_z(get, out)

    def of_set(V):
        return lambda zl, i, y, n: V.get((zl * PZ + i + 1) * ROWS + LO + y, n)

    def of_mw(zl, i, y, n):
        return MW[pl.ds((zl * XL + i) * 64 + y, n), :]

    def halo_start(src, dst, send, recv, axes=(0, 1, 2)):
        for ax in axes:
            rows = (XG, YG, ZG)[ax]
            pltpu.make_async_remote_copy(
                src_ref=src.at[rows, :], dst_ref=dst.at[rows, :], send_sem=send, recv_sem=recv,
                device_id=peers[side[ax]], device_id_type=FLAT).start()

    def whole(src, dst, send, recv):
        return pltpu.make_async_remote_copy(src_ref=src, dst_ref=dst, send_sem=send, recv_sem=recv,
                                            device_id=peers[1], device_id_type=FLAT)

    def three_at_once(b, dst, recv, recv_z=None):
        sets = (WS, Set(T1, b), Set(T2, b))
        for q, t in enumerate(sets):
            pack_xy(of_set(t), SB.at[q])
        for q in range(3):
            halo_start(SB.at[q], dst.at[q], h_send, recv, (0, 1))
        for q, t in enumerate(sets):
            pack_z(of_set(t), SB.at[q])
        for q in range(3):
            halo_start(SB.at[q], dst.at[q], h_send, recv if recv_z is None else recv_z, (2,))

    def sync_all(par):
        return pltpu.make_async_remote_copy(
            src_ref=SS.at[par, pl.ds(1, 7), :], dst_ref=SS.at[par, pl.ds(1, 7), :],
            send_sem=s_send.at[par], recv_sem=s_recv.at[par], device_id=peers[1], device_id_type=FLAT)

    def sync_start(par, items):
        row = zero8
        for idx, acc in items:
            row = jnp.where(lane8 == idx, jnp.sum(acc, axis=1, keepdims=True), row)
        row = row + pltpu.roll(row, 4, 0)
        row = row + pltpu.roll(row, 2, 0)
        row = row + pltpu.roll(row, 1, 0)
        SS[par, 0:1, :] = row[0:1]
        for p in (6, 7, 5, 3, 4, 2, 1):
            pltpu.make_async_remote_copy(
                src_ref=SS.at[par, pl.ds(0, 1), :], dst_ref=SS.at[par, pl.ds(p, 1), :],
                send_sem=s_send.at[par], recv_sem=s_recv.at[par],
                device_id=peers[p], device_id_type=FLAT).start()

    def sync_wait(par):
        sync_all(par).wait_recv()
        tot = SS[par]
        tot = tot + pltpu.roll(tot, 4, 0)
        tot = tot + pltpu.roll(tot, 2, 0)
        return tot + pltpu.roll(tot, 1, 0)

    def bc(tot, k):
        return jnp.broadcast_to(tot[:, k:k + 1], (8, 128))

    def fold(x):
        return jnp.sum(v8(x), axis=0)

    def poly(c, j):
        s = damp_ref[c, j] / 6.0
        a0, a1, a2 = 3.0 * s, 3.0 * s * s, s * s * s
        q = jnp.full((8, 128), a0 - 6.0 * a1 + 36.0 * a2, f32)
        return q, (a1 - 12.0 * a2) / q, a2 / q

    @pl.loop(0, 2 * PZ)
    def _(p):
        for V in (ZS, XS, WS, Set(T1, 0), Set(T1, 1)):
            V.put(pl.multiple_of(p * ROWS, 8), 8, zero8)
            V.put(pl.multiple_of(p * ROWS + HI, 8), 8, zero8)

    a = lax.broadcasted_iota(jnp.int32, (256, 256), 0)
    d = lax.broadcasted_iota(jnp.int32, (256, 256), 1)
    d0 = d - jnp.where(d >= 128, 128, 0)
    h = jnp.where(d0 >= 96, 3, jnp.where(d0 >= 64, 2, jnp.where(d0 >= 32, 1, 0)))
    target = 64 * h + 2 * (d0 - 32 * h) + jnp.where(d >= 128, 1, 0)
    DEAL[...] = jnp.where(a == target, 1.0, 0.0).astype(jnp.bfloat16)

    @pl.loop(0, 5)
    def _(q):
        load(q, q % 4, ini_hbm).wait()

        @pl.when(q == 0)
        def _():
            for d in range(3):
                load(1 + d, 1 + d, vel_hbm.at[d]).start()
        m = DEAL[...]
        half = jnp.where(jnp.full((8, 128), q, jnp.int32) % 4 == 0, 1.0, 0.5)
        for i in range(0, XL, DEALT):
            v = jnp.concatenate([jnp.concatenate([STG[q % 4, h * XL + x] for h in range(4)], axis=1)
                                 for x in range(i, i + DEALT)], axis=0)
            o = rearrange(v, m)
            o = v8(o[:, 0:128]), v8(o[:, 128:256])
            for zl in range(2):
                CO[q, (i + zl * XL) * 64:(i + DEALT + zl * XL) * 64, :] = (o[zl] * half).reshape(-1, 128)

        @pl.when(q == 0)
        def _():
            load(4, 0, src_hbm).start()

            pack(lambda zl, i, y, n: CO[0, pl.ds((zl * XL + i) * 64 + y, n), :], SU)
            pl.semaphore_wait(bar, 7)
            halo_start(SU, GX, u_send, x_recv)

            def take_x(r, row, c):
                XS.put(row, 64, CO[0, pl.ds(pl.multiple_of(r * 64, 8), 64), :])
                return c
            all_planes(take_x, 0)

    @pl.loop(0, XL)
    def _(i):
        low = pl.ds(pl.multiple_of(i * 64, 8), 64)
        high = pl.ds(pl.multiple_of((i + XL) * 64, 8), 64)
        h0, h1 = CO[3, low, :], CO[3, high, :]
        cm0, cp1 = 1.0 + h0, 1.0 - h1
        CZP[low, :] = 1.0 - h0
        CZM[low, :] = jnp.where(zh == 0, 0.0, cm0)
        CZA[low, :] = jnp.where(zh == 32 * gz, 0.0, cm0)
        CZM[high, :] = 1.0 + h1
        CZP[high, :] = jnp.where(zh == 31, 0.0, cp1)
        CZA[high, :] = jnp.where(zh == 63 - 32 * gz, 0.0, cp1)

    pd = (XL - 1) * (1 - gx)
    at_x = jnp.logical_and(lane >= o_x, lane < o_x + 32)
    sign_x, sign_y = (2 * gx - 1).astype(f32), (2 * gy - 1).astype(f32)
    for zl in range(2):
        hv = CO[1, pl.ds(pl.multiple_of((zl * XL + pd) * 64, 8), 64), :]
        CGX[64 * zl:64 * zl + 64, :] = jnp.where(at_x, 1.0 + sign_x * hv, 0.0)

    @pl.loop(0, NP)
    def _(r):
        CGY[pl.ds(r, 1), :] = 1.0 + sign_y * CO[2, pl.ds(r * 64 + y_send, 1), :]
    whole(SU, GX, u_send, x_recv).wait()

    def halo_xy(dst, recv):
        return whole(SU.at[pl.ds(0, 56), :], dst.at[pl.ds(0, 56), :], u_send, recv)

    def halo_z(dst, recv):
        return whole(SU.at[pl.ds(56, 64), :], dst.at[pl.ds(56, 64), :], z_send, recv)

    def ghost_of_z(k, e, b, q, rows):
        g = v8(RU[b, rows, :])
        for i in range(k):
            g = g - e[i] * v8(GMU[i, rows, :])
        GZ[k, rows, :] = (q * g).reshape(-1, 128)

    def first_ghosts(rows, scale, q, r1, r2):
        g = [v8(GU[0, t, rows, :]) for t in range(3)]
        if scale is not None:
            g = [t * scale for t in g]
            for t in range(3):
                GU[0, t, rows, :] = g[t].reshape(-1, 128)
        GZ[0, rows, :] = (q * (g[0] + r1 * g[1] + r2 * g[2])).reshape(-1, 128)

    def sweep(V, unroll, put, ghost=None):
        def one(i, c):
            neighbours(V, i, put, ghost)
            return c
        pairs(unroll, one)

    def to_n(V):
        def put(r8, row, size, u, n):
            V.put(row, size, n)
        return put

    def givens(m, sub):
        h = [RM[i, m] for i in range(m + 1)]
        for i in range(m):
            cs, sn = CS[i], SN[i]
            h[i], h[i + 1] = cs * h[i] + sn * h[i + 1], cs * h[i + 1] - sn * h[i]
        d = h[m]
        rad = jnp.sqrt(d * d + sub * sub)
        cs, sn = d / rad, sub / rad
        CS[m] = cs
        SN[m] = sn
        h[m] = cs * d + sn * sub
        RM[0:m + 1, m] = jnp.stack(h)
        g = GV[m]
        GV[m] = cs * g
        GV[m + 1] = -sn * g
        est = MISC[4] * jnp.abs(sn)
        MISC[4] = est
        return est

    out_scale = 1.0 / math.sqrt(1572864.0)
    last_halo = CYCLES * RESTART - 3

    @pl.loop(0, CYCLES)
    def _(c):
        fill_ghosts(XS, GX)

        def put_r(r8, row, size, u, n):
            WS.put(row, size, CO[4, r8 * 8:r8 * 8 + size, :] - (6.0 * u - n))
        sweep(XS, XL, put_r, GX.at[ZG, :])

        @pl.when(c == 0)
        def _():
            def one(r, row, acc):
                t = v8(WS.get(row, 64)).reshape(2, 4, 8, 128)
                return acc + jnp.sum(t * t, axis=0)
            acc = all_planes(one, jnp.zeros((4, 8, 128), f32), 2)
            sync_start(0, [(16, jnp.sum(acc, axis=0))])

        @pl.loop(0, RESTART)
        def _(j):
            step = c * RESTART + j
            par = (step + 1) % 2
            b = step % 2
            nxt = (j + 1) % RESTART
            slot = c * RESTART + (1 - c) * j + c * (j % 3)

            @pl.when(j * (j - LATE) >= 0)
            def _():
                seams(WS)
                sweep(WS, XL, to_n(Set(T1, 0)))
                seams(Set(T1, 0))

            @pl.when(j >= LATE)
            def _():
                q, r1, r2 = poly(c, j)
                q, r1, r2 = (jnp.concatenate([t] * 8, axis=0) for t in (q * KAP[j], r1, r2))

                def put_z(r8, row, size, u, n):
                    z = q * (WS.get(row, size) + r1 * u + r2 * n)
                    ZS.put(row, size, z)
                    Z[j, r8:r8 + size // 8] = v8(z)
                sweep(Set(T1, 0), XL, put_z)

            @pl.when(j == 0)
            def _():
                sweep(Set(T1, 0), XL, to_n(Set(T2, 0)))

                @pl.when(c == 0)
                def _():
                    three_at_once(0, GU.at[0], h_recv.at[1], z_recv.at[1])
                    tot = sync_wait(0)
                    sync_all(0).wait_send()
                    beta0 = jnp.sqrt(bc(tot, 16))
                    MISC[0] = beta0
                    MISC[1] = 1.0 / beta0

                inv0 = MISC[1]
                KAP[0] = jnp.ones((8, 128), f32)
                q, r1, r2 = poly(c, 0)

                def start(r, row, acc):
                    u, n, n2 = (v8(t.get(row, 64)) * inv0 for t in (WS, Set(T1, 0), Set(T2, 0)))
                    z = q * (u + r1 * n + r2 * n2)
                    acc = acc + jnp.sum((u * u).reshape(2, 4, 8, 128), axis=0)
                    at = pl.ds(r * 8, 8)
                    U[0, at] = u
                    NU[0, at] = n
                    N2U[0, at] = n2
                    Z[0, at] = z
                    ZS.put(row, 64, z.reshape(64, 128))
                    return acc
                ACC[0] = jnp.sum(all_planes(start, jnp.zeros((4, 8, 128), f32)), axis=0)

                @pl.when(c == 0)
                def _():
                    whole(SB.at[:, pl.ds(56, 64), :], GU.at[0, :, pl.ds(56, 64), :], h_send, z_recv.at[1]).wait_recv()
                    first_ghosts(slice(56, 120), inv0, q, r1, r2)

                @pl.when(c > 0)
                def _():
                    whole(SB, RB.at[RESTART - 1], h_send, h_recv.at[(RESTART - 1) % 3]).wait_recv()
                    for t in range(3):
                        g = YY[0] * v8(RB[0, t])
                        for m in range(1, RESTART):
                            g = g + YY[m] * v8(RB[m, t])
                        GU[0, t] = (v8(GU[0, t]) - inv0 * g).reshape(GROWS, 128)
                    first_ghosts(slice(0, 120), None, q, r1, r2)

            seams(ZS)
            GX2[...] = GZ[j, ZG, :]

            def put_w(r8, row, size, u, n):
                WS.put(row, size, 6.0 * u - n)
            sweep(ZS, XL, put_w, GX2)

            @pl.when(j > 0)
            def _():
                def case(k):
                    halo_xy(RU.at[1 - b], u_recv.at[1 - b]).wait_recv()
                    ghost_of_z(k, [EC[i] for i in range(k)], 1 - b, KAP[k] * poly(c, k)[0], slice(0, 56))
                pick(j, 1, RESTART, case)

            @pl.when(step == 0)
            def _():
                whole(SB.at[:, pl.ds(0, 56), :], GU.at[0, :, pl.ds(0, 56), :], h_send, h_recv.at[1]).wait_recv()
                whole(SB, GU.at[0], h_send, h_recv.at[1]).wait_send()
                first_ghosts(slice(0, 56), MISC[1], *poly(c, 0))
            add_ghosts_xy(GZ.at[j])

            def case(k):
                ends = k == 0 or k == RESTART - 1
                wd = 4 if k < 4 else 2 if k < 8 else 1
                count = k + 2 if ends else k + 1

                def dots(t, accs):
                    accs = list(accs)
                    for zl in range(2):
                        x = t * 2 + zl * XL
                        w = jnp.concatenate([v8(WS.get(row0(t * 2 + (zl * PZ + 1 + i)), 64)) for i in range(2)])
                        w = w.reshape(16 // wd, wd, 8, 128)
                        for i in range(k + 1):
                            v = U[i, pl.ds(x * 8, 16)].reshape(16 // wd, wd, 8, 128)
                            accs[i] = accs[i] + jnp.sum(v * w, axis=0)
                        if ends:
                            accs[k + 1] = accs[k + 1] + jnp.sum(w * w, axis=0)
                    return tuple(accs)
                accs = lax.fori_loop(0, XL // 2, dots, (jnp.zeros((wd, 8, 128), f32),) * count)
                accs = [jnp.sum(a, axis=0) for a in accs]
                items = [(i, accs[i]) for i in range(k + 1)] + [(16 + i, ACC[i]) for i in range(k + 1)]
                if ends:
                    items.append((32, accs[k + 1]))
                sync_start(par, items)
            pick(j, 0, RESTART, case)

            @pl.when(step > 0)
            def _():
                sync_all(1 - par).wait_send()

            @pl.when(step < CYCLES * RESTART - 1)
            def _():
                seams(WS)
                sweep(WS, XL, to_n(Set(T1, b)))

            @pl.when(CYCLES * RESTART - 1 - step > 0)
            def _():
                seams(Set(T1, b))
                r1, r2 = (jnp.concatenate([t] * 8, axis=0) for t in poly(c, nxt)[1:])

                def put(r8, row, size, u, n):
                    Set(T2, b).put(row, size, n)
                    MW[r8 * 8:r8 * 8 + size, :] = WS.get(row, size) + r1 * u + r2 * n
                sweep(Set(T1, b), XL, put)

            @pl.when(j > 0)
            def _():
                halo_xy(RU.at[b], u_recv.at[b]).wait_send()
                halo_z(RU.at[b], z_recv.at[b]).wait_send()

            @pl.when(j < RESTART - 1)
            def _():
                pack_xy(of_mw, SU)
                halo_start(SU, RU.at[b], u_send, u_recv.at[b], (0, 1))
                pack_z(of_mw, SU)
                halo_start(SU, RU.at[b], z_send, z_recv.at[b], (2,))

            @pl.when(step <= last_halo + 1)
            def _():
                @pl.when(step > 0)
                def _():
                    whole(SB, RB.at[slot], h_send, h_recv.at[0]).wait_send()

                @pl.when(step <= last_halo)
                def _():
                    three_at_once(b, RB.at[slot], h_recv.at[step % 3])

                @pl.when(j > 0)
                def _():
                    whole(SB, RB.at[slot], h_send, h_recv.at[(step + 2) % 3]).wait_recv()

            prev = c * RESTART + (1 - c) * (j - 1) + c * ((j + 2) % 3)
            def case(k):
                if k < RESTART - 1:
                    q, r1, r2 = poly(c, k + 1)
                    e = [EC[i] for i in range(k)]

                    size = 8 if k < 4 else 2

                    def body(r, row, cy):
                        for y in range(0, 8, size):
                            at = pl.ds(r * 8 + y, size)
                            if k:
                                n = v8(Set(T1, 1 - b).get(row + 8 * y, 8 * size))
                                n2 = v8(Set(T2, 1 - b).get(row + 8 * y, 8 * size))
                                if k == LATE - 2:
                                    n = r1 * n + r2 * n2
                                    for m in range(k):
                                        d = r1 * NU[m, at] + r2 * N2U[m, at]
                                        n = n - e[m] * d
                                        MU[m, at] = U[m, at] + d
                                    MU[k, at] = U[k, at] + n
                                    continue
                                for m in range(k):
                                    nm, n2m = NU[m, at], N2U[m, at]
                                    n = n - e[m] * nm
                                    n2 = n2 - e[m] * n2m
                                    MU[m, at] = U[m, at] + r1 * nm + r2 * n2m
                                NU[k, at] = n
                                N2U[k, at] = n2
                            else:
                                n, n2 = NU[0, at], N2U[0, at]
                            MU[k, at] = U[k, at] + r1 * n + r2 * n2
                        return cy
                    if k < LATE - 1:
                        all_planes(body, 0)

                    if k:
                        for t in range(3):
                            g = v8(RB[prev, t])
                            for i in range(k):
                                g = g - e[i] * v8(GU[i, t])
                            GU[k, t] = g.reshape(GROWS, 128)

                    @pl.loop(0, k + 1)
                    def _(i):
                        g = v8(GU[i, 0]) + r1 * v8(GU[i, 1]) + r2 * v8(GU[i, 2])
                        GMU[i] = g.reshape(GROWS, 128)
                if k >= 2:
                    est = givens(k - 2, NRM[k - 1] * SW[k - 2])
                    RES[c] = jnp.where(lane8 == k - 1, est, RES[c])
            pick(j, 0, RESTART, case)

            tot = sync_wait(par)

            def case(k):
                nn = bc(tot, 16 + k)
                nrm = jnp.sqrt(nn)
                sg = 1.0 / nrm
                SIG[k] = sg
                NRM[k] = nrm
                kap = KAP[k]
                sw = sg / kap
                SW[k] = sw
                sig = SIG[0:k + 1]
                h = jnp.stack([bc(tot, i) for i in range(k + 1)]) * (sig * sw)
                gcol = jnp.stack([bc(tot, 16 + i) for i in range(k + 1)]) * (sig * sg)
                GM[k, 0:k + 1] = gcol
                if k > 0:
                    GM[0:k, k] = gcol[0:k]

                def gram_times(x):
                    out = gcol * x[k]
                    for m in range(k):
                        out = out + GM[m, 0:k + 1] * x[m]
                    return out
                cf = 2.0 * h - gram_times(h)
                RM[0:k + 1, k] = cf
                if k == 0:
                    beta = MISC[0] * nrm
                    MISC[4] = beta
                    GV[0] = beta
                    RES[c] = jnp.where(lane8 == 0, beta, 0.0)
                    wn = jnp.sqrt(bc(tot, 32)) * sw
                    rho = 1.0 / wn
                    MISC[2] = rho
                else:
                    rho = MISC[2]
                if k < RESTART - 1:
                    es = cf * (sig * (kap * nrm))
                    EC[0:k + 1] = es
                    KAP[k + 1] = rho * sg
                    q = (rho * sg) * poly(c, k + 1)[0]

                    size = 8 if k < 3 else 4 if k < 5 or k >= LATE - 1 else 2

                    def body(r, row, accs):
                        accs = list(accs)
                        for y in range(0, 8, size):
                            at = pl.ds(r * 8 + y, size)
                            v = [U[m, at] for m in range(k + 1)]
                            u = v8(WS.get(row + 8 * y, 8 * size))
                            if k < LATE - 1:
                                z = v8(MW[pl.ds(pl.multiple_of(r * 64 + 8 * y, 8), 8 * size), :])
                            for m in range(k + 1):
                                u = u - es[m] * v[m]
                                if k < LATE - 1:
                                    z = z - es[m] * MU[m, at]
                            U[k + 1, at] = u
                            if k < LATE - 1:
                                z = q * z
                                Z[k + 1, at] = z
                                ZS.put(row + 8 * y, 8 * size, z.reshape(8 * size, 128))
                            else:
                                WS.put(row + 8 * y, 8 * size, u.reshape(8 * size, 128))
                            for m in range(k + 1):
                                accs[m] = accs[m] + jnp.sum(u * v[m], axis=0)
                            accs[k + 1] = accs[k + 1] + jnp.sum(u * u, axis=0)
                        return tuple(accs)
                    accs = all_planes(body, (zero8,) * (k + 2), 2 if k < 3 else 1)
                    ACC[0:k + 2] = jnp.stack(accs)
                    halo_z(RU.at[b], z_recv.at[b]).wait_recv()
                    ghost_of_z(k + 1, es, b, q, slice(56, 120))
                else:
                    wn2 = bc(tot, 32) * sw * sw
                    drop = jnp.sum(cf * (2.0 * h - gram_times(cf)), axis=0)
                    sub = jnp.sqrt(jnp.maximum(wn2 - drop, 0.0))
                    est = givens(k - 1, nrm * SW[k - 1])
                    RES[c] = jnp.where(lane8 == k, est, RES[c])
                    est = givens(k, sub)
                    RES[c] = jnp.where(lane8 == k + 1, est, RES[c])
                    g = [GV[i] for i in range(RESTART)]
                    for i in reversed(range(RESTART)):
                        y = g[i] / RM[i, i]
                        YY[i] = y * SW[i]
                        for m in range(i):
                            g[m] = g[m] - RM[m, i] * y
            pick(j, 0, RESTART, case)

        yy = [YY[i] for i in range(RESTART)]

        def update(r, row, cy):
            x = v8(XS.get(row, 64))
            for m in range(RESTART):
                x = x + yy[m] * Z[m, pl.ds(r * 8, 8)]
            x = x.reshape(64, 128)
            XS.put(row, 64, x)
            out_ref[pl.ds(pl.multiple_of(r * 64, 8), 64), :] = x
            return cy
        all_planes(update, 0)

        @pl.when(c == 0)
        def _():

            g = v8(GX[...])
            for m in range(RESTART):
                g = g + yy[m] * v8(GZ[m])
            GX[...] = g.reshape(GROWS, 128)

    sync_all((CYCLES * RESTART) % 2).wait_send()
    rows = jnp.where(lax.broadcasted_iota(jnp.int32, (8, 128), 0) == 0, RES[0], RES[1]) * out_scale
    res_ref[...] = rows


def unpack(x_ref, r_ref, out_hbm, res_ref, out, out_sem):
    a = lax.broadcasted_iota(jnp.int32, (256, 256), 0)
    d = lax.broadcasted_iota(jnp.int32, (256, 256), 1)
    a0 = a - jnp.where(a >= 128, 128, 0)
    h = jnp.where(a0 >= 96, 3, jnp.where(a0 >= 64, 2, jnp.where(a0 >= 32, 1, 0)))
    m = jnp.where(d == 64 * h + 2 * (a0 - 32 * h) + jnp.where(a >= 128, 1, 0), 1.0, 0.0).astype(jnp.bfloat16)
    stores = []
    for i in range(0, XL, 2):
        v = jnp.concatenate([jnp.concatenate([x_ref[64 * x:64 * x + 64, :], x_ref[64 * (x + XL):64 * (x + XL) + 64, :]],
                                             axis=1) for x in (i, i + 1)], axis=0)
        o = rearrange(v, m)
        for x in range(2):
            for h in range(4):
                out[h, i + x] = o[64 * x:64 * x + 64, 64 * h:64 * h + 64]
        for h in range(4):
            stores.append(pltpu.make_async_copy(out.at[h, pl.ds(i, 2)], out_hbm.at[h, pl.ds(i, 2)], out_sem.at[i // 2, h]))
            stores[-1].start()
    res_ref[...] = r_ref[0:CYCLES, 0:RESTART + 1]
    for cp in stores:
        cp.wait()


def solution(mesh):
    grid_spec = P(('sys', 'gx'), 'gy', 'gz')
    vel_spec = P(None, ('sys', 'gx'), 'gy', 'gz')
    table_spec = P('sys', None)
    f32 = jnp.float32

    def local_solve(source, initial, velocity, damping):
        big = (SETR, 128)
        vol, flat = (NP * 8, 8, 128), (NP * 64, 128)
        v = lambda *s: pltpu.VMEM(s, f32)
        n = RESTART
        scratch = [
            v(n, *vol), v(LATE - 2, *vol), v(LATE - 2, *vol), v(LATE - 1, *vol), v(n, *vol),
            v(*big), v(*big), v(*big), v(2, *big), v(2, *big), v(*flat),
            v(5, *flat), v(*flat), v(*flat), v(*flat), v(128, 128), v(NP, 128), v(NP, 128),
            v(n - 1, 3, GROWS, 128), v(n - 1, GROWS, 128), v(n + 3, 3, GROWS, 128), v(2, GROWS, 128),
            v(3, GROWS, 128), v(GROWS, 128), v(n, GROWS, 128), v(GROWS, 128), v(64, 128),
            v(2, 8, 128), v(n + 1, 8, 128), v(n, n, 8, 128), v(n, n, 8, 128),
            v(n, 8, 128), v(n, 8, 128), v(n, 8, 128), v(n, 8, 128), v(n, 8, 128), v(n, 8, 128), v(n + 1, 8, 128), v(n, 8, 128), v(n, 8, 128),
            v(CYCLES, 8, 128), v(8, 8, 128), v(4, 48, 64, 64), pltpu.VMEM((256, 256), jnp.bfloat16),
            pltpu.SemaphoreType.DMA((2,)), pltpu.SemaphoreType.DMA((2,)), pltpu.SemaphoreType.DMA,
            pltpu.SemaphoreType.DMA((3,)), pltpu.SemaphoreType.DMA, pltpu.SemaphoreType.DMA((2,)),
            pltpu.SemaphoreType.DMA, pltpu.SemaphoreType.DMA((2,)), pltpu.SemaphoreType.DMA, pltpu.SemaphoreType.DMA((5,)),
        ]
        hbm = pl.BlockSpec(memory_space=pl.ANY)
        vm = pl.BlockSpec(memory_space=pltpu.VMEM)
        packed, rows = pl.pallas_call(
            kernel,
            out_shape=(pltpu.VMEM(flat, f32), pltpu.VMEM((8, 128), f32)),
            in_specs=[hbm, hbm, hbm, pl.BlockSpec(memory_space=pltpu.SMEM)],
            out_specs=(vm, vm),
            scratch_shapes=scratch,
            compiler_params=pltpu.CompilerParams(
                collective_id=0, has_side_effects=True, vmem_limit_bytes=60 * 2**20),
            name='fgmres',
        )(source, initial, velocity, damping)
        out, res = pl.pallas_call(
            unpack,
            out_shape=(jax.ShapeDtypeStruct((4, XL, 64, 64), f32), jax.ShapeDtypeStruct((CYCLES, n + 1), f32)),
            in_specs=[vm, vm],
            out_specs=(hbm, vm),
            scratch_shapes=[v(4, XL, 64, 64), pltpu.SemaphoreType.DMA((6, 4))],
            compiler_params=pltpu.CompilerParams(vmem_limit_bytes=16 * 2**20),
            name='unpack',
        )(packed, rows)
        return out.reshape(source.shape), res

    return jax.shard_map(local_solve, mesh=mesh, in_specs=(grid_spec, grid_spec, vel_spec, table_spec),
                         out_specs=(grid_spec, table_spec), check_vma=False)
```

```python
import math
import jax
import jax.numpy as jnp
from jax import lax
from jax.experimental import pallas as pl
from jax.experimental.pallas import tpu as pltpu
from jax.sharding import PartitionSpec as P

FLAT = pl.DeviceIdType.LOGICAL
LANES, YS, QUARTER, SUB, PAIR = 128, 64, 32, 8, 256
TWO, THREE, FOUR = 2, 3, 4
RESTART = 10
CYCLES = TWO
XL = 12
NP = TWO * XL
PZ = XL + TWO
LO, HI, ROWS = SUB, 72, 80
SETR = TWO * PZ * ROWS
LATE = SUB
XG, YG, ZG = slice(0, QUARTER), slice(QUARTER, 56), slice(56, 120)
GROWS = 120
DEALT = TWO


def pairs(unroll, body, carry=()):
    if unroll == XL:
        for i in range(XL):
            carry = body(i, carry)
        return carry

    def trip(t, carry):
        for i in range(unroll):
            carry = body(t * unroll + i, carry)
        return carry
    return lax.fori_loop(0, XL // unroll, trip, carry)


def v8(x):
    return x.reshape(-1, SUB, LANES)


class Set:
    def __init__(self, ref, t=None):
        self.ref, self.t = ref, t

    def index(self, start, size):
        rows = pl.ds(start, size) if not isinstance(start, int) else slice(start, start + size)
        return (rows, slice(None)) if self.t is None else (self.t, rows, slice(None))

    def get(self, start, size):
        return self.ref[self.index(start, size)]

    def put(self, start, size, v):
        self.ref[self.index(start, size)] = v

    def view(self, start, size):
        return self.ref.at[self.index(start, size)]


def row0(p):
    r = p * ROWS + LO
    return r if isinstance(r, int) else pl.multiple_of(r, SUB)


def rearrange(v, m):
    f32 = jnp.float32
    a1 = v.astype(jnp.bfloat16)
    v = v - a1.astype(f32)
    a2 = v.astype(jnp.bfloat16)
    a3 = (v - a2.astype(f32)).astype(jnp.bfloat16)
    n = v.shape[0]
    o = jnp.dot(jnp.concatenate([a1, a2, a3], axis=0), m, preferred_element_type=f32)
    return (o[TWO * n:] + o[n:TWO * n]) + o[:n]


def pick(j, lo, hi, fn):
    if hi - lo == 1:
        fn(lo)
    else:
        mid = (lo + hi) // TWO
        lax.cond(j < mid, lambda: pick(j, lo, mid, fn), lambda: pick(j, mid, hi, fn))


def all_planes(body, carry, step=1):
    def trip(t, carry):
        for zl in range(TWO):
            for i in range(step):
                x = t * step + i
                carry = body(x + zl * XL, row0(x + (zl * PZ + 1)), carry)
        return carry
    return lax.fori_loop(0, XL // step, trip, carry)


def kernel(src_hbm, ini_hbm, vel_hbm, damp_ref, out_ref, res_ref,
           U, NU, N2U, MU, Z, ZC, X, W, T1, T2, MW, CO, CZP, CZM, CZA, CGX, CGY, YB,
           GU, GMU, RB, RU, SB, SU, GZ, GX, GX2, SS, ACC, GM, RM, SIG, EC, KAP, SW, CS, SN, GV, YY, NRM, RES, MISC, STG, DEAL,
           s_send, s_recv, h_send, h_recv, u_send, u_recv, z_send, z_recv, x_recv, l_sem):
    f32 = jnp.float32
    gx, gy, gz = lax.axis_index('gx'), lax.axis_index('gy'), lax.axis_index('gz')
    peers = {}
    for p in range(1, SUB):
        a, b, c = p // FOUR, (p // TWO) % TWO, p % TWO
        peers[p] = (1 - gx if a else gx) * FOUR + (1 - gy if b else gy) * TWO + (1 - gz if c else gz)
    side = {0: FOUR, 1: TWO, TWO: 1}

    def load(q, slot, src):
        return pltpu.make_async_copy(src, STG.at[slot], l_sem.at[q])

    load(0, 0, ini_hbm).start()
    bar = pltpu.get_barrier_semaphore()
    for p in range(1, SUB):
        pl.semaphore_signal(bar, inc=1, device_id=peers[p], device_id_type=FLAT)

    lane = lax.broadcasted_iota(jnp.int32, (YS, LANES), 1)
    lane8 = lane[0:SUB]
    left = lane < YS
    zh = jnp.where(left, jnp.where(lane < QUARTER, lane, lane - QUARTER), jnp.where(lane < 96, lane - YS, lane - 96))
    zh32 = zh[0:QUARTER]
    first_q, last_q = lane < QUARTER, lane >= 96
    zero64 = jnp.zeros((YS, LANES), f32)
    zero8 = jnp.zeros((SUB, LANES), f32)
    hi_x = (1 - gx).astype(f32)
    l0 = 31 * (1 - gz)
    o_x = 96 * (1 - gx)
    y_send = 63 * (1 - gy)
    y_pad = HI - 65 * gy
    edge_lo = zh32 == QUARTER * (1 - gz)
    edge_hi = zh32 == 31 + QUARTER * gz
    WS, ZS, XS = Set(W), Set(ZC), Set(X)

    def seams(V, ghost=None):
        for zl in range(TWO):
            b = zl * PZ
            a = pltpu.roll(V.get(row0(b + XL), YS), QUARTER, 1)
            d = pltpu.roll(V.get(row0(b + 1), YS), 96, 1)
            lo = 0.0 if ghost is None else ghost[zl] * (1.0 - hi_x)
            hi = 0.0 if ghost is None else ghost[zl] * hi_x
            V.put(row0(b), YS, jnp.where(first_q, lo, a))
            V.put(row0(b + XL + 1), YS, jnp.where(last_q, hi, d))

    def neighbours(V, i, put, ghost=None):
        size = YS if ghost is None else QUARTER
        for y in range(0, YS, size):
            co = lambda C, r: C[r * YS + y:r * YS + y + size, :]
            hv = lambda d, r: CO[d, r * YS + y:r * YS + y + size, :]
            at = lambda q, d: V.get(row0(q) + y + d, size)
            u0, u1 = at(i + 1, 0), at(i + (PZ + 1), 0)
            below, above = pltpu.roll(u1, 1, 1), pltpu.roll(u0, 127, 1)
            if ghost is None:
                cm0, cp1 = co(CZM, i), co(CZP, i + XL)
            else:
                g = pltpu.roll(ghost[y:y + size, :], (l0 - i + LANES) % LANES, 1)
                below = jnp.where(edge_lo, g, below)
                above = jnp.where(edge_hi, g, above)
                cm0, cp1 = co(CZA, i), co(CZA, i + XL)
            for zl, u, n in ((0, u0, co(CZP, i) * u1 + cm0 * below), (1, u1, co(CZM, i + XL) * u0 + cp1 * above)):
                q, r = i + (zl * PZ + 1), i + zl * XL
                yp, ym = at(q, 1), at(q, -1)
                xp, xm = at(q + 1, 0), at(q - 1, 0)
                n = n + (xp + xm) - hv(1, r) * (xp - xm)
                n = n + (yp + ym) - hv(TWO, r) * (yp - ym)
                put(r * SUB + y // SUB, row0(q) + y, size, u, n)

    def spread_x(rec):
        g = rec[XG, :]
        return [jnp.concatenate([pltpu.roll(g, (o_x - YS * zl - QUARTER * yh + LANES) % LANES, 1) for yh in range(TWO)], axis=0)
                for zl in range(TWO)]

    def fill_ghosts(V, rec):
        seams(V, spread_x(rec))

        @pl.loop(0, TWO)
        def _(zl):
            for i in range(XL):
                V.put((zl * PZ + (i + 1)) * ROWS + y_pad, 1, rec[pl.ds(zl * XL + (i + QUARTER), 1), :])

    def add_ghosts_xy(rec):
        pd = (XL - 1) * (1 - gx)
        for zl, g in enumerate(spread_x(rec)):
            row = (pd + (zl * PZ + 1)) * ROWS + LO
            WS.put(row, YS, WS.get(row, YS) - CGX[YS * zl:YS * zl + YS, :] * g)
        YB[...] = CGY[...] * rec[YG, :]
        for r in range(NP):
            row = row0(r % XL + r // XL * PZ + 1) + y_send
            WS.put(row, 1, WS.get(row, 1) - YB[r:r + 1, :])

    def pack_xy(get, out):
        pd = (XL - 1) * (1 - gx)
        acc = zero64[0:QUARTER]
        for zl in range(TWO):
            for yh in range(TWO):
                slot = TWO * zl + yh
                r = pltpu.roll(get(zl, pd, QUARTER * yh, QUARTER), (QUARTER * slot - o_x + LANES) % LANES, 1)
                here = jnp.logical_and(lane[0:QUARTER] >= QUARTER * slot, lane[0:QUARTER] < QUARTER * slot + QUARTER)
                acc = jnp.where(here, r, acc)
        out[XG, :] = acc

        for zl in range(TWO):
            for i in range(XL):
                r = QUARTER + zl * XL + i
                out[r:r + 1, :] = get(zl, i, y_send, 1)

    def pack_z(get, out):
        acc = zero64
        for i in range(XL):
            r = pltpu.roll(get(1 - gz, i, 0, YS), (i - l0 + LANES) % LANES, 1)
            acc = jnp.where(zh == i, r, acc)
        out[ZG, :] = acc

    def pack(get, out):
        pack_xy(get, out)
        pack_z(get, out)

    def of_set(V):
        return lambda zl, i, y, n: V.get((zl * PZ + i + 1) * ROWS + LO + y, n)

    def of_mw(zl, i, y, n):
        return MW[pl.ds((zl * XL + i) * YS + y, n), :]

    def halo_start(src, dst, send, recv, axes=(0, 1, TWO)):
        for ax in axes:
            rows = (XG, YG, ZG)[ax]
            pltpu.make_async_remote_copy(
                src_ref=src.at[rows, :], dst_ref=dst.at[rows, :], send_sem=send, recv_sem=recv,
                device_id=peers[side[ax]], device_id_type=FLAT).start()

    def whole(src, dst, send, recv):
        return pltpu.make_async_remote_copy(src_ref=src, dst_ref=dst, send_sem=send, recv_sem=recv,
                                            device_id=peers[1], device_id_type=FLAT)

    def three_at_once(b, dst, recv, recv_z=None):
        sets = (WS, Set(T1, b), Set(T2, b))
        for q, t in enumerate(sets):
            pack_xy(of_set(t), SB.at[q])
        for q in range(THREE):
            halo_start(SB.at[q], dst.at[q], h_send, recv, (0, 1))
        for q, t in enumerate(sets):
            pack_z(of_set(t), SB.at[q])
        for q in range(THREE):
            halo_start(SB.at[q], dst.at[q], h_send, recv if recv_z is None else recv_z, (TWO,))

    def sync_all(par):
        return pltpu.make_async_remote_copy(
            src_ref=SS.at[par, pl.ds(1, 7), :], dst_ref=SS.at[par, pl.ds(1, 7), :],
            send_sem=s_send.at[par], recv_sem=s_recv.at[par], device_id=peers[1], device_id_type=FLAT)

    def sync_start(par, items):
        row = zero8
        for idx, acc in items:
            row = jnp.where(lane8 == idx, jnp.sum(acc, axis=1, keepdims=True), row)
        row = row + pltpu.roll(row, FOUR, 0)
        row = row + pltpu.roll(row, TWO, 0)
        row = row + pltpu.roll(row, 1, 0)
        SS[par, 0:1, :] = row[0:1]
        for p in (6, 7, 5, THREE, FOUR, TWO, 1):
            pltpu.make_async_remote_copy(
                src_ref=SS.at[par, pl.ds(0, 1), :], dst_ref=SS.at[par, pl.ds(p, 1), :],
                send_sem=s_send.at[par], recv_sem=s_recv.at[par],
                device_id=peers[p], device_id_type=FLAT).start()

    def sync_wait(par):
        sync_all(par).wait_recv()
        tot = SS[par]
        tot = tot + pltpu.roll(tot, FOUR, 0)
        tot = tot + pltpu.roll(tot, TWO, 0)
        return tot + pltpu.roll(tot, 1, 0)

    def bc(tot, k):
        return jnp.broadcast_to(tot[:, k:k + 1], (SUB, LANES))

    def fold(x):
        return jnp.sum(v8(x), axis=0)

    def poly(c, j):
        s = damp_ref[c, j] / 6.0
        a0, a1, a2 = 3.0 * s, 3.0 * s * s, s * s * s
        q = jnp.full((SUB, LANES), a0 - 6.0 * a1 + 36.0 * a2, f32)
        return q, (a1 - 12.0 * a2) / q, a2 / q

    @pl.loop(0, TWO * PZ)
    def _(p):
        for V in (ZS, XS, WS, Set(T1, 0), Set(T1, 1)):
            V.put(pl.multiple_of(p * ROWS, SUB), SUB, zero8)
            V.put(pl.multiple_of(p * ROWS + HI, SUB), SUB, zero8)

    a = lax.broadcasted_iota(jnp.int32, (PAIR, PAIR), 0)
    d = lax.broadcasted_iota(jnp.int32, (PAIR, PAIR), 1)
    d0 = d - jnp.where(d >= LANES, LANES, 0)
    h = jnp.where(d0 >= 96, THREE, jnp.where(d0 >= YS, TWO, jnp.where(d0 >= QUARTER, 1, 0)))
    target = YS * h + TWO * (d0 - QUARTER * h) + jnp.where(d >= LANES, 1, 0)
    DEAL[...] = jnp.where(a == target, 1.0, 0.0).astype(jnp.bfloat16)

    @pl.loop(0, 5)
    def _(q):
        load(q, q % FOUR, ini_hbm).wait()

        @pl.when(q == 0)
        def _():
            for d in range(THREE):
                load(1 + d, 1 + d, vel_hbm.at[d]).start()
        m = DEAL[...]
        half = jnp.where(jnp.full((SUB, LANES), q, jnp.int32) % FOUR == 0, 1.0, 0.5)
        for i in range(0, XL, DEALT):
            v = jnp.concatenate([jnp.concatenate([STG[q % FOUR, h * XL + x] for h in range(FOUR)], axis=1)
                                 for x in range(i, i + DEALT)], axis=0)
            o = rearrange(v, m)
            o = v8(o[:, 0:LANES]), v8(o[:, LANES:PAIR])
            for zl in range(TWO):
                CO[q, (i + zl * XL) * YS:(i + DEALT + zl * XL) * YS, :] = (o[zl] * half).reshape(-1, LANES)

        @pl.when(q == 0)
        def _():
            load(FOUR, 0, src_hbm).start()

            pack(lambda zl, i, y, n: CO[0, pl.ds((zl * XL + i) * YS + y, n), :], SU)
            pl.semaphore_wait(bar, 7)
            halo_start(SU, GX, u_send, x_recv)

            def take_x(r, row, c):
                XS.put(row, YS, CO[0, pl.ds(pl.multiple_of(r * YS, SUB), YS), :])
                return c
            all_planes(take_x, 0)

    @pl.loop(0, XL)
    def _(i):
        low = pl.ds(pl.multiple_of(i * YS, SUB), YS)
        high = pl.ds(pl.multiple_of((i + XL) * YS, SUB), YS)
        h0, h1 = CO[THREE, low, :], CO[THREE, high, :]
        cm0, cp1 = 1.0 + h0, 1.0 - h1
        CZP[low, :] = 1.0 - h0
        CZM[low, :] = jnp.where(zh == 0, 0.0, cm0)
        CZA[low, :] = jnp.where(zh == QUARTER * gz, 0.0, cm0)
        CZM[high, :] = 1.0 + h1
        CZP[high, :] = jnp.where(zh == 31, 0.0, cp1)
        CZA[high, :] = jnp.where(zh == 63 - QUARTER * gz, 0.0, cp1)

    pd = (XL - 1) * (1 - gx)
    at_x = jnp.logical_and(lane >= o_x, lane < o_x + QUARTER)
    sign_x, sign_y = (TWO * gx - 1).astype(f32), (TWO * gy - 1).astype(f32)
    for zl in range(TWO):
        hv = CO[1, pl.ds(pl.multiple_of((zl * XL + pd) * YS, SUB), YS), :]
        CGX[YS * zl:YS * zl + YS, :] = jnp.where(at_x, 1.0 + sign_x * hv, 0.0)

    @pl.loop(0, NP)
    def _(r):
        CGY[pl.ds(r, 1), :] = 1.0 + sign_y * CO[TWO, pl.ds(r * YS + y_send, 1), :]
    whole(SU, GX, u_send, x_recv).wait()

    def halo_xy(dst, recv):
        return whole(SU.at[pl.ds(0, 56), :], dst.at[pl.ds(0, 56), :], u_send, recv)

    def halo_z(dst, recv):
        return whole(SU.at[pl.ds(56, YS), :], dst.at[pl.ds(56, YS), :], z_send, recv)

    def ghost_of_z(k, e, b, q, rows):
        g = v8(RU[b, rows, :])
        for i in range(k):
            g = g - e[i] * v8(GMU[i, rows, :])
        GZ[k, rows, :] = (q * g).reshape(-1, LANES)

    def first_ghosts(rows, scale, q, r1, r2):
        g = [v8(GU[0, t, rows, :]) for t in range(THREE)]
        if scale is not None:
            g = [t * scale for t in g]
            for t in range(THREE):
                GU[0, t, rows, :] = g[t].reshape(-1, LANES)
        GZ[0, rows, :] = (q * (g[0] + r1 * g[1] + r2 * g[TWO])).reshape(-1, LANES)

    def sweep(V, unroll, put, ghost=None):
        def one(i, c):
            neighbours(V, i, put, ghost)
            return c
        pairs(unroll, one)

    def to_n(V):
        def put(r8, row, size, u, n):
            V.put(row, size, n)
        return put

    def givens(m, sub):
        h = [RM[i, m] for i in range(m + 1)]
        for i in range(m):
            cs, sn = CS[i], SN[i]
            h[i], h[i + 1] = cs * h[i] + sn * h[i + 1], cs * h[i + 1] - sn * h[i]
        d = h[m]
        rad = jnp.sqrt(d * d + sub * sub)
        cs, sn = d / rad, sub / rad
        CS[m] = cs
        SN[m] = sn
        h[m] = cs * d + sn * sub
        RM[0:m + 1, m] = jnp.stack(h)
        g = GV[m]
        GV[m] = cs * g
        GV[m + 1] = -sn * g
        est = MISC[FOUR] * jnp.abs(sn)
        MISC[FOUR] = est
        return est

    out_scale = 1.0 / math.sqrt(1572864.0)
    last_halo = CYCLES * RESTART - THREE

    @pl.loop(0, CYCLES)
    def _(c):
        fill_ghosts(XS, GX)

        def put_r(r8, row, size, u, n):
            WS.put(row, size, CO[FOUR, r8 * SUB:r8 * SUB + size, :] - (6.0 * u - n))
        sweep(XS, XL, put_r, GX.at[ZG, :])

        @pl.when(c == 0)
        def _():
            def one(r, row, acc):
                t = v8(WS.get(row, YS)).reshape(TWO, FOUR, SUB, LANES)
                return acc + jnp.sum(t * t, axis=0)
            acc = all_planes(one, jnp.zeros((FOUR, SUB, LANES), f32), TWO)
            sync_start(0, [(16, jnp.sum(acc, axis=0))])

        @pl.loop(0, RESTART)
        def _(j):
            step = c * RESTART + j
            par = (step + 1) % TWO
            b = step % TWO
            nxt = (j + 1) % RESTART
            slot = c * RESTART + (1 - c) * j + c * (j % THREE)

            @pl.when(j * (j - LATE) >= 0)
            def _():
                seams(WS)
                sweep(WS, XL, to_n(Set(T1, 0)))
                seams(Set(T1, 0))

            @pl.when(j >= LATE)
            def _():
                q, r1, r2 = poly(c, j)
                q, r1, r2 = (jnp.concatenate([t] * SUB, axis=0) for t in (q * KAP[j], r1, r2))

                def put_z(r8, row, size, u, n):
                    z = q * (WS.get(row, size) + r1 * u + r2 * n)
                    ZS.put(row, size, z)
                    Z[j, r8:r8 + size // SUB] = v8(z)
                sweep(Set(T1, 0), XL, put_z)

            @pl.when(j == 0)
            def _():
                sweep(Set(T1, 0), XL, to_n(Set(T2, 0)))

                @pl.when(c == 0)
                def _():
                    three_at_once(0, GU.at[0], h_recv.at[1], z_recv.at[1])
                    tot = sync_wait(0)
                    sync_all(0).wait_send()
                    beta0 = jnp.sqrt(bc(tot, 16))
                    MISC[0] = beta0
                    MISC[1] = 1.0 / beta0

                inv0 = MISC[1]
                KAP[0] = jnp.ones((SUB, LANES), f32)
                q, r1, r2 = poly(c, 0)

                def start(r, row, acc):
                    u, n, n2 = (v8(t.get(row, YS)) * inv0 for t in (WS, Set(T1, 0), Set(T2, 0)))
                    z = q * (u + r1 * n + r2 * n2)
                    acc = acc + jnp.sum((u * u).reshape(TWO, FOUR, SUB, LANES), axis=0)
                    at = pl.ds(r * SUB, SUB)
                    U[0, at] = u
                    NU[0, at] = n
                    N2U[0, at] = n2
                    Z[0, at] = z
                    ZS.put(row, YS, z.reshape(YS, LANES))
                    return acc
                ACC[0] = jnp.sum(all_planes(start, jnp.zeros((FOUR, SUB, LANES), f32)), axis=0)

                @pl.when(c == 0)
                def _():
                    whole(SB.at[:, pl.ds(56, YS), :], GU.at[0, :, pl.ds(56, YS), :], h_send, z_recv.at[1]).wait_recv()
                    first_ghosts(slice(56, 120), inv0, q, r1, r2)

                @pl.when(c > 0)
                def _():
                    whole(SB, RB.at[RESTART - 1], h_send, h_recv.at[(RESTART - 1) % THREE]).wait_recv()
                    for t in range(THREE):
                        g = YY[0] * v8(RB[0, t])
                        for m in range(1, RESTART):
                            g = g + YY[m] * v8(RB[m, t])
                        GU[0, t] = (v8(GU[0, t]) - inv0 * g).reshape(GROWS, LANES)
                    first_ghosts(slice(0, 120), None, q, r1, r2)

            seams(ZS)
            GX2[...] = GZ[j, ZG, :]

            def put_w(r8, row, size, u, n):
                WS.put(row, size, 6.0 * u - n)
            sweep(ZS, XL, put_w, GX2)

            @pl.when(j > 0)
            def _():
                def case(k):
                    halo_xy(RU.at[1 - b], u_recv.at[1 - b]).wait_recv()
                    ghost_of_z(k, [EC[i] for i in range(k)], 1 - b, KAP[k] * poly(c, k)[0], slice(0, 56))
                pick(j, 1, RESTART, case)

            @pl.when(step == 0)
            def _():
                whole(SB.at[:, pl.ds(0, 56), :], GU.at[0, :, pl.ds(0, 56), :], h_send, h_recv.at[1]).wait_recv()
                whole(SB, GU.at[0], h_send, h_recv.at[1]).wait_send()
                first_ghosts(slice(0, 56), MISC[1], *poly(c, 0))
            add_ghosts_xy(GZ.at[j])

            def case(k):
                ends = k == 0 or k == RESTART - 1
                wd = FOUR if k < FOUR else TWO if k < SUB else 1
                count = k + TWO if ends else k + 1

                def dots(t, accs):
                    accs = list(accs)
                    for zl in range(TWO):
                        x = t * TWO + zl * XL
                        w = jnp.concatenate([v8(WS.get(row0(t * TWO + (zl * PZ + 1 + i)), YS)) for i in range(TWO)])
                        w = w.reshape(16 // wd, wd, SUB, LANES)
                        for i in range(k + 1):
                            v = U[i, pl.ds(x * SUB, 16)].reshape(16 // wd, wd, SUB, LANES)
                            accs[i] = accs[i] + jnp.sum(v * w, axis=0)
                        if ends:
                            accs[k + 1] = accs[k + 1] + jnp.sum(w * w, axis=0)
                    return tuple(accs)
                accs = lax.fori_loop(0, XL // TWO, dots, (jnp.zeros((wd, SUB, LANES), f32),) * count)
                accs = [jnp.sum(a, axis=0) for a in accs]
                items = [(i, accs[i]) for i in range(k + 1)] + [(16 + i, ACC[i]) for i in range(k + 1)]
                if ends:
                    items.append((QUARTER, accs[k + 1]))
                sync_start(par, items)
            pick(j, 0, RESTART, case)

            @pl.when(step > 0)
            def _():
                sync_all(1 - par).wait_send()

            @pl.when(step < CYCLES * RESTART - 1)
            def _():
                seams(WS)
                sweep(WS, XL, to_n(Set(T1, b)))

            @pl.when(CYCLES * RESTART - 1 - step > 0)
            def _():
                seams(Set(T1, b))
                r1, r2 = (jnp.concatenate([t] * SUB, axis=0) for t in poly(c, nxt)[1:])

                def put(r8, row, size, u, n):
                    Set(T2, b).put(row, size, n)
                    MW[r8 * SUB:r8 * SUB + size, :] = WS.get(row, size) + r1 * u + r2 * n
                sweep(Set(T1, b), XL, put)

            @pl.when(j > 0)
            def _():
                halo_xy(RU.at[b], u_recv.at[b]).wait_send()
                halo_z(RU.at[b], z_recv.at[b]).wait_send()

            @pl.when(j < RESTART - 1)
            def _():
                pack_xy(of_mw, SU)
                halo_start(SU, RU.at[b], u_send, u_recv.at[b], (0, 1))
                pack_z(of_mw, SU)
                halo_start(SU, RU.at[b], z_send, z_recv.at[b], (TWO,))

            @pl.when(step <= last_halo + 1)
            def _():
                @pl.when(step > 0)
                def _():
                    whole(SB, RB.at[slot], h_send, h_recv.at[0]).wait_send()

                @pl.when(step <= last_halo)
                def _():
                    three_at_once(b, RB.at[slot], h_recv.at[step % THREE])

                @pl.when(j > 0)
                def _():
                    whole(SB, RB.at[slot], h_send, h_recv.at[(step + TWO) % THREE]).wait_recv()

            prev = c * RESTART + (1 - c) * (j - 1) + c * ((j + TWO) % THREE)
            def case(k):
                if k < RESTART - 1:
                    q, r1, r2 = poly(c, k + 1)
                    e = [EC[i] for i in range(k)]

                    size = SUB if k < FOUR else TWO

                    def body(r, row, cy):
                        for y in range(0, SUB, size):
                            at = pl.ds(r * SUB + y, size)
                            if k:
                                n = v8(Set(T1, 1 - b).get(row + SUB * y, SUB * size))
                                n2 = v8(Set(T2, 1 - b).get(row + SUB * y, SUB * size))
                                if k == LATE - TWO:
                                    n = r1 * n + r2 * n2
                                    for m in range(k):
                                        d = r1 * NU[m, at] + r2 * N2U[m, at]
                                        n = n - e[m] * d
                                        MU[m, at] = U[m, at] + d
                                    MU[k, at] = U[k, at] + n
                                    continue
                                for m in range(k):
                                    nm, n2m = NU[m, at], N2U[m, at]
                                    n = n - e[m] * nm
                                    n2 = n2 - e[m] * n2m
                                    MU[m, at] = U[m, at] + r1 * nm + r2 * n2m
                                NU[k, at] = n
                                N2U[k, at] = n2
                            else:
                                n, n2 = NU[0, at], N2U[0, at]
                            MU[k, at] = U[k, at] + r1 * n + r2 * n2
                        return cy
                    if k < LATE - 1:
                        all_planes(body, 0)

                    if k:
                        for t in range(THREE):
                            g = v8(RB[prev, t])
                            for i in range(k):
                                g = g - e[i] * v8(GU[i, t])
                            GU[k, t] = g.reshape(GROWS, LANES)

                    @pl.loop(0, k + 1)
                    def _(i):
                        g = v8(GU[i, 0]) + r1 * v8(GU[i, 1]) + r2 * v8(GU[i, TWO])
                        GMU[i] = g.reshape(GROWS, LANES)
                if k >= TWO:
                    est = givens(k - TWO, NRM[k - 1] * SW[k - TWO])
                    RES[c] = jnp.where(lane8 == k - 1, est, RES[c])
            pick(j, 0, RESTART, case)

            tot = sync_wait(par)

            def case(k):
                nn = bc(tot, 16 + k)
                nrm = jnp.sqrt(nn)
                sg = 1.0 / nrm
                SIG[k] = sg
                NRM[k] = nrm
                kap = KAP[k]
                sw = sg / kap
                SW[k] = sw
                sig = SIG[0:k + 1]
                h = jnp.stack([bc(tot, i) for i in range(k + 1)]) * (sig * sw)
                gcol = jnp.stack([bc(tot, 16 + i) for i in range(k + 1)]) * (sig * sg)
                GM[k, 0:k + 1] = gcol
                if k > 0:
                    GM[0:k, k] = gcol[0:k]

                def gram_times(x):
                    out = gcol * x[k]
                    for m in range(k):
                        out = out + GM[m, 0:k + 1] * x[m]
                    return out
                cf = 2.0 * h - gram_times(h)
                RM[0:k + 1, k] = cf
                if k == 0:
                    beta = MISC[0] * nrm
                    MISC[FOUR] = beta
                    GV[0] = beta
                    RES[c] = jnp.where(lane8 == 0, beta, 0.0)
                    wn = jnp.sqrt(bc(tot, QUARTER)) * sw
                    rho = 1.0 / wn
                    MISC[TWO] = rho
                else:
                    rho = MISC[TWO]
                if k < RESTART - 1:
                    es = cf * (sig * (kap * nrm))
                    EC[0:k + 1] = es
                    KAP[k + 1] = rho * sg
                    q = (rho * sg) * poly(c, k + 1)[0]

                    size = SUB if k < THREE else FOUR if k < 5 or k >= LATE - 1 else TWO

                    def body(r, row, accs):
                        accs = list(accs)
                        for y in range(0, SUB, size):
                            at = pl.ds(r * SUB + y, size)
                            v = [U[m, at] for m in range(k + 1)]
                            u = v8(WS.get(row + SUB * y, SUB * size))
                            if k < LATE - 1:
                                z = v8(MW[pl.ds(pl.multiple_of(r * YS + SUB * y, SUB), SUB * size), :])
                            for m in range(k + 1):
                                u = u - es[m] * v[m]
                                if k < LATE - 1:
                                    z = z - es[m] * MU[m, at]
                            U[k + 1, at] = u
                            if k < LATE - 1:
                                z = q * z
                                Z[k + 1, at] = z
                                ZS.put(row + SUB * y, SUB * size, z.reshape(SUB * size, LANES))
                            else:
                                WS.put(row + SUB * y, SUB * size, u.reshape(SUB * size, LANES))
                            for m in range(k + 1):
                                accs[m] = accs[m] + jnp.sum(u * v[m], axis=0)
                            accs[k + 1] = accs[k + 1] + jnp.sum(u * u, axis=0)
                        return tuple(accs)
                    accs = all_planes(body, (zero8,) * (k + TWO), TWO if k < 5 else 1)
                    ACC[0:k + TWO] = jnp.stack(accs)
                    halo_z(RU.at[b], z_recv.at[b]).wait_recv()
                    ghost_of_z(k + 1, es, b, q, slice(56, 120))
                else:
                    wn2 = bc(tot, QUARTER) * sw * sw
                    drop = jnp.sum(cf * (2.0 * h - gram_times(cf)), axis=0)
                    sub = jnp.sqrt(jnp.maximum(wn2 - drop, 0.0))
                    est = givens(k - 1, nrm * SW[k - 1])
                    RES[c] = jnp.where(lane8 == k, est, RES[c])
                    est = givens(k, sub)
                    RES[c] = jnp.where(lane8 == k + 1, est, RES[c])
                    g = [GV[i] for i in range(RESTART)]
                    for i in reversed(range(RESTART)):
                        y = g[i] / RM[i, i]
                        YY[i] = y * SW[i]
                        for m in range(i):
                            g[m] = g[m] - RM[m, i] * y
            pick(j, 0, RESTART, case)

        yy = [YY[i] for i in range(RESTART)]

        def update(r, row, cy):
            x = v8(XS.get(row, YS))
            for m in range(RESTART):
                x = x + yy[m] * Z[m, pl.ds(r * SUB, SUB)]
            x = x.reshape(YS, LANES)
            XS.put(row, YS, x)
            out_ref[pl.ds(pl.multiple_of(r * YS, SUB), YS), :] = x
            return cy
        all_planes(update, 0)

        @pl.when(c == 0)
        def _():

            g = v8(GX[...])
            for m in range(RESTART):
                g = g + yy[m] * v8(GZ[m])
            GX[...] = g.reshape(GROWS, LANES)

    sync_all((CYCLES * RESTART) % TWO).wait_send()
    rows = jnp.where(lax.broadcasted_iota(jnp.int32, (SUB, LANES), 0) == 0, RES[0], RES[1]) * out_scale
    res_ref[...] = rows


def unpack(x_ref, r_ref, out_hbm, res_ref, out, out_sem):
    a = lax.broadcasted_iota(jnp.int32, (PAIR, PAIR), 0)
    d = lax.broadcasted_iota(jnp.int32, (PAIR, PAIR), 1)
    a0 = a - jnp.where(a >= LANES, LANES, 0)
    h = jnp.where(a0 >= 96, THREE, jnp.where(a0 >= YS, TWO, jnp.where(a0 >= QUARTER, 1, 0)))
    m = jnp.where(d == YS * h + TWO * (a0 - QUARTER * h) + jnp.where(a >= LANES, 1, 0), 1.0, 0.0).astype(jnp.bfloat16)
    stores = []
    for i in range(0, XL, TWO):
        v = jnp.concatenate([jnp.concatenate([x_ref[YS * x:YS * x + YS, :], x_ref[YS * (x + XL):YS * (x + XL) + YS, :]],
                                             axis=1) for x in (i, i + 1)], axis=0)
        o = rearrange(v, m)
        for x in range(TWO):
            for h in range(FOUR):
                out[h, i + x] = o[YS * x:YS * x + YS, YS * h:YS * h + YS]
        for h in range(FOUR):
            stores.append(pltpu.make_async_copy(out.at[h, pl.ds(i, TWO)], out_hbm.at[h, pl.ds(i, TWO)], out_sem.at[i // TWO, h]))
            stores[-1].start()
    res_ref[...] = r_ref[0:CYCLES, 0:RESTART + 1]
    for cp in stores:
        cp.wait()


def solution(mesh):
    grid_spec = P(('sys', 'gx'), 'gy', 'gz')
    vel_spec = P(None, ('sys', 'gx'), 'gy', 'gz')
    table_spec = P('sys', None)
    f32 = jnp.float32

    def local_solve(source, initial, velocity, damping):
        big = (SETR, LANES)
        vol, flat = (NP * SUB, SUB, LANES), (NP * YS, LANES)
        v = lambda *s: pltpu.VMEM(s, f32)
        n = RESTART
        scratch = [
            v(n, *vol), v(LATE - TWO, *vol), v(LATE - TWO, *vol), v(LATE - 1, *vol), v(n, *vol),
            v(*big), v(*big), v(*big), v(TWO, *big), v(TWO, *big), v(*flat),
            v(5, *flat), v(*flat), v(*flat), v(*flat), v(LANES, LANES), v(NP, LANES), v(NP, LANES),
            v(n - 1, THREE, GROWS, LANES), v(n - 1, GROWS, LANES), v(n + THREE, THREE, GROWS, LANES), v(TWO, GROWS, LANES),
            v(THREE, GROWS, LANES), v(GROWS, LANES), v(n, GROWS, LANES), v(GROWS, LANES), v(YS, LANES),
            v(TWO, SUB, LANES), v(n + 1, SUB, LANES), v(n, n, SUB, LANES), v(n, n, SUB, LANES),
            v(n, SUB, LANES), v(n, SUB, LANES), v(n, SUB, LANES), v(n, SUB, LANES), v(n, SUB, LANES), v(n, SUB, LANES), v(n + 1, SUB, LANES), v(n, SUB, LANES), v(n, SUB, LANES),
            v(CYCLES, SUB, LANES), v(SUB, SUB, LANES), v(FOUR, 48, YS, YS), pltpu.VMEM((PAIR, PAIR), jnp.bfloat16),
            pltpu.SemaphoreType.DMA((TWO,)), pltpu.SemaphoreType.DMA((TWO,)), pltpu.SemaphoreType.DMA,
            pltpu.SemaphoreType.DMA((THREE,)), pltpu.SemaphoreType.DMA, pltpu.SemaphoreType.DMA((TWO,)),
            pltpu.SemaphoreType.DMA, pltpu.SemaphoreType.DMA((TWO,)), pltpu.SemaphoreType.DMA, pltpu.SemaphoreType.DMA((5,)),
        ]
        hbm = pl.BlockSpec(memory_space=pl.ANY)
        vm = pl.BlockSpec(memory_space=pltpu.VMEM)
        packed, rows = pl.pallas_call(
            kernel,
            out_shape=(pltpu.VMEM(flat, f32), pltpu.VMEM((SUB, LANES), f32)),
            in_specs=[hbm, hbm, hbm, pl.BlockSpec(memory_space=pltpu.SMEM)],
            out_specs=(vm, vm),
            scratch_shapes=scratch,
            compiler_params=pltpu.CompilerParams(
                collective_id=0, has_side_effects=True, vmem_limit_bytes=60 * TWO**20),
            name='fgmres',
        )(source, initial, velocity, damping)
        out, res = pl.pallas_call(
            unpack,
            out_shape=(jax.ShapeDtypeStruct((FOUR, XL, YS, YS), f32), jax.ShapeDtypeStruct((CYCLES, n + 1), f32)),
            in_specs=[vm, vm],
            out_specs=(hbm, vm),
            scratch_shapes=[v(FOUR, XL, YS, YS), pltpu.SemaphoreType.DMA((6, FOUR))],
            compiler_params=pltpu.CompilerParams(vmem_limit_bytes=16 * TWO**20),
            name='unpack',
        )(packed, rows)
        return out.reshape(source.shape), res

    return jax.shard_map(local_solve, mesh=mesh, in_specs=(grid_spec, grid_spec, vel_spec, table_spec),
                         out_specs=(grid_spec, table_spec), check_vma=False)
```
